128 devices in a mesh: gx: 16 (over x, z), gy: 8 (over y, core).
Axes of the slice: x: 4, y: 4, z: 4, core: 2. Of those that a mesh axis runs over, the one named last changes fastest.
Arguments:
- pressure: float32 [512, 256, 128], P('gx', 'gy'), may hold values from -6 to 6
- depth: float32 [512, 256, 128], P('gx', 'gy'), may hold values from -6 to 6
- saturation: float32 [2, 512, 256, 128], P(None, 'gx', 'gy'), may hold values from 0.05 to 0.45
- permeability: float32 [3, 512, 256, 128], P(None, 'gx', 'gy'), may hold values from 0.1 to 10
- pore_volume: float32 [512, 256, 128], P('gx', 'gy'), may hold values from 0.5 to 2
- fault_pairs: int32 [4096, 3], P(('gx', 'gy')), may hold values from 0 to 1023, as said below
- fault_kind: int32 [4096], P(('gx', 'gy')), may hold values from 0 to 15
- fault_count: int32 [128], P(('gx', 'gy')), may hold values from 8 to 32, as said below
- fault_table: float32 [16, 128], replicated, may hold values from 0.2 to 2
Outputs:
- saturation_next: float32 [3, 512, 256, 128], P(None, 'gx', 'gy')
The draws below stay inside these ranges and needn't reach their ends.
Inputs may be any that keep to these rules, and one draw needn't show every extreme that they name: `fault_pairs`: each device holds 32 rows. Column 0 and column 2 are areal column numbers a * 32 + b of the source and target device. Column 1 is the target device i2 * 8 + j2, which lies within one index of the source device along gx and along gy, counted cyclically. Among one device's 32 rows at most 4 name the same target device, and on every device some target device is named by exactly 4 rows. Rows 0 to fault_count - 1 of a device are live; some device has 32 live rows.
All inputs are finite; a program needn't handle non-finite values.
Results may differ from the reference program's by a relative error of at most 0.0003.
Values sent between devices are 32-bit elements; how exact they have to be, the bound alone decides.
A program may use at most 64 MiB of HBM per device.

```python
import math
import jax
import jax.numpy as jnp
from jax import lax

CX = 32
CY = 32
NZ = 128
FB = 32
CAP = 4
NTAB = 16
NX = 512
NY = 256
N_GX = 16
N_GY = 8


def draw_fault_pairs(key, part):
    devices = N_GX * N_GY

    def one_device(device_key, device):
        order = jax.random.permutation(jax.random.fold_in(device_key, 1), 9 * CAP)[:FB].astype(jnp.int32)
        near = order // CAP
        step_x = near // 3 - 1
        step_y = near % 3 - 1
        home_x = device // N_GY
        home_y = device % N_GY
        target = (home_x + step_x) % N_GX * N_GY + (home_y + step_y) % N_GY
        source = jax.random.randint(jax.random.fold_in(device_key, 2), (FB,), 0, CX * CY, dtype=jnp.int32)
        landing = jax.random.randint(jax.random.fold_in(device_key, 3), (FB,), 0, CX * CY, dtype=jnp.int32)
        return jnp.stack([source, target.astype(jnp.int32), landing], axis=1)
    keys = jax.random.split(jax.random.fold_in(key, 11), devices)
    device_ids = jnp.arange(devices, dtype=jnp.int32)
    return jax.vmap(one_device)(keys, device_ids).reshape(devices * FB, 3)


def draw_fault_count(key, part):
    devices = N_GX * N_GY
    levels = jax.random.randint(jax.random.fold_in(key, 21), (devices,), 0, 3, dtype=jnp.int32)
    counts = jnp.where(levels == 0, FB, jnp.where(levels == 1, FB // 2, FB // 4)).astype(jnp.int32)
    busiest = jax.random.randint(jax.random.fold_in(key, 22), (), 0, devices, dtype=jnp.int32)
    return jnp.where(jnp.arange(devices, dtype=jnp.int32) == busiest, FB, counts).astype(jnp.int32)


def set_ends(entries, own_key, low, largest):
    index_at = [jax.random.randint(jax.random.fold_in(own_key, axis), (), 0, length) for axis, length in enumerate(entries.shape)]
    widest = entries.shape.index(max(entries.shape))
    beside = index_at[:widest] + [(index_at[widest] + 1) % entries.shape[widest]] + index_at[widest + 1:]
    return entries.at[tuple(index_at)].set(low).at[tuple(beside)].set(largest)


def shard_levels(key, dims, cuts, smallest, top_value):
    loudness, own = 1.0, jax.random.fold_in(key, 6)
    for dim, parts in cuts:
        draws = jnp.exp(jax.random.uniform(jax.random.fold_in(own, dim), (parts,), jnp.float32, smallest / len(cuts), top_value / len(cuts)))
        loudness = loudness * jnp.repeat(draws, dims[dim] // parts).reshape([-1 if axis == dim else 1 for axis in range(len(dims))])
    return loudness


def normal_values(own_key, dims, spread, reach, cuts=(), held_as=jnp.bfloat16):
    factor_of = shard_levels(own_key, dims, cuts, -0.22, 0.18) if cuts else 1.0
    values = jax.random.normal(own_key, dims, jnp.float32) * spread * factor_of
    return jnp.minimum(jnp.maximum(values, -reach), reach).astype(held_as)


def setup_inputs(seed: int = 0) -> dict:
    streams_of = jax.random.split(jax.random.key(seed), 10)
    pressure = normal_values(streams_of[0], (NX, NY, NZ), 1.0, 6.0, ((0, 16), (1, 8)), jnp.float32)
    depth = normal_values(streams_of[1], (NX, NY, NZ), 1.0, 6.0, ((0, 16), (1, 8)), jnp.float32)
    saturation = jnp.clip(0.05 + 0.39999999 * jax.random.uniform(streams_of[2], (2, NX, NY, NZ), jnp.float32) ** shard_levels(streams_of[2], (2, NX, NY, NZ), ((1, 16), (2, 8)), -0.2, 0.2), 0.05, 0.45)
    permeability = jnp.clip(jnp.exp(math.log(10.0) - 4.6051702 * jax.random.uniform(streams_of[3], (3, NX, NY, NZ), jnp.float32) ** shard_levels(streams_of[3], (3, NX, NY, NZ), ((1, 16), (2, 8)), -0.2, 0.2)), 0.1, 10.0)
    pore_volume = jnp.clip(jnp.exp(math.log(2.0) - 1.3862944 * jax.random.uniform(streams_of[4], (NX, NY, NZ), jnp.float32) ** shard_levels(streams_of[4], (NX, NY, NZ), ((0, 16), (1, 8)), -0.2, 0.2)), 0.5, 2.0)
    fault_pairs = draw_fault_pairs(jax.random.fold_in(streams_of[9], 71), 0)
    fault_kind = set_ends(jax.random.randint(streams_of[6], (N_GX * N_GY * FB,), 0, NTAB), jax.random.fold_in(streams_of[6], 1), 0, NTAB - 1).astype(jnp.int32)
    fault_count = draw_fault_count(jax.random.fold_in(streams_of[9], 71), 0)
    fault_table = jnp.clip(jnp.exp(jax.random.uniform(streams_of[8], (NTAB, NZ), jnp.float32, math.log(0.2), math.log(2.0))), 0.2, 2.0)
    return dict(pressure=pressure, depth=depth, saturation=saturation, permeability=permeability, pore_volume=pore_volume, fault_pairs=fault_pairs, fault_kind=fault_kind, fault_count=fault_count, fault_table=fault_table)


VISCOSITY = (0.5, 1.0, 0.25)
DENSITY = (1.0, 0.8, 0.25)
step_length = 0.2


def mobility(sat_water, sat_oil):
    sat_gas = 1.0 - sat_water - sat_oil
    return (sat_water * sat_water / VISCOSITY[0], sat_oil * sat_oil / VISCOSITY[1], sat_gas * sat_gas / VISCOSITY[2])


def harmonic(first, second):
    return 2.0 * first * second / (first + second)


def phase_flux(press_low, depth_low, mobile_low, press_high, depth_high, mobile_high, trans):
    flows = []
    for phase in range(3):
        drive = (press_low - press_high) - DENSITY[phase] * (depth_low - depth_high)
        upwind = jnp.where(drive > 0.0, mobile_low[phase], mobile_high[phase])
        flows.append(trans * upwind * drive)
    return jnp.stack(flows, axis=-2)


def consecutive(array, axis, start):
    return lax.slice_in_dim(array, start, array.shape[axis] - 1 + start, axis=axis)


def face_flows(press, height, mobile, perm, axis):
    def lower(array):
        return consecutive(array, axis, 0)

    def upper(array):
        return consecutive(array, axis, 1)

    return phase_flux(lower(press), lower(height), tuple(lower(m) for m in mobile),
                      upper(press), upper(height), tuple(upper(m) for m in mobile),
                      harmonic(lower(perm), upper(perm)))


def reference(pressure, depth, saturation, permeability, pore_volume, fault_pairs, fault_kind, fault_count, fault_table):
    sat_water = saturation[0]
    sat_oil = saturation[1]
    mobile = mobility(sat_water, sat_oil)
    flow_x = jnp.pad(face_flows(pressure, depth, mobile, permeability[0], 0), ((1, 1), (0, 0), (0, 0), (0, 0)))
    flow_y = jnp.pad(face_flows(pressure, depth, mobile, permeability[1], 1), ((0, 0), (1, 1), (0, 0), (0, 0)))
    flow_z = jnp.pad(face_flows(pressure, depth, mobile, permeability[2], 2), ((0, 0), (0, 0), (0, 0), (1, 1)))
    net = (flow_x[1:] - flow_x[:-1]) + (flow_y[:, 1:] - flow_y[:, :-1]) + (flow_z[..., 1:] - flow_z[..., :-1])
    devices = N_GX * N_GY
    pairs = fault_pairs.reshape(devices, FB, 3)
    device = jnp.arange(devices, dtype=jnp.int32)[:, None]
    home_x = device // N_GY
    home_y = device % N_GY
    source = ((home_x * CX + pairs[..., 0] // CY) * NY + home_y * CY + pairs[..., 0] % CY).reshape(-1)
    target = pairs[..., 1]
    dest = (((target // N_GY) * CX + pairs[..., 2] // CY) * NY + (target % N_GY) * CY + pairs[..., 2] % CY).reshape(-1)
    live = (jnp.arange(FB, dtype=jnp.int32)[None, :] < fault_count[:, None]).reshape(-1)
    trans = fault_table[fault_kind] * live[:, None].astype(jnp.float32)
    press_flat = pressure.reshape(NX * NY, NZ)
    depth_flat = depth.reshape(NX * NY, NZ)
    mobile_flat = tuple(m.reshape(NX * NY, NZ) for m in mobile)
    fault_flow = phase_flux(press_flat[source], depth_flat[source], tuple(m[source] for m in mobile_flat),
                            press_flat[dest], depth_flat[dest], tuple(m[dest] for m in mobile_flat), trans)
    net_flat = net.reshape(NX * NY, 3, NZ).at[source].add(fault_flow).at[dest].add(-fault_flow)
    net = net_flat.reshape(NX, NY, 3, NZ)
    sat_gas = 1.0 - sat_water - sat_oil
    return jnp.stack([current - step_length * net[:, :, phase, :] / pore_volume
                      for phase, current in enumerate((sat_water, sat_oil, sat_gas))], axis=0)
```

```python
import jax
import jax.numpy as jnp
from jax import lax
from jax.experimental import pallas as pl
from jax.experimental.pallas import tpu as pltpu
from jax.sharding import PartitionSpec as P

CAP = 4
CODES = 9
HERE = 4
SLOTS = 40
RHO = (1.0, 0.8, 0.25)
STEP = 0.2
NX = 32
NY = 32
NZ = 128
COLS = NX * NY
TILE = 8
BLOCK = 2
MESH = pl.DeviceIdType.MESH


def mobility(sw, so):
    sg = 1.0 - sw - so
    return (sw * sw * 2.0, so * so, sg * sg * 4.0)


def harmonic(a, b):
    return 2.0 * a * b / (a + b)


def fluxes(pa, da, ma, pb, db, mb, trans):
    dp = pa - pb
    dd = da - db
    out = []
    for f in range(3):
        drive = dp - (dd if RHO[f] == 1.0 else RHO[f] * dd)
        out.append(trans * jnp.where(drive > 0.0, ma[f], mb[f]) * drive)
    return out


def grid_kernel(
    press, depth, sat, perm, pore, pairs, kind, count, table,
    acc, wgt, hot, rows,
    P_, D_, W_, O_, KX, KY, KZ, PV, TAB, PR, KD, CT,
    sreq, sidx, rreq, ridx, loc, sresp, rresp,
    ysend, hx, hy, fxs, fys,
    lsem, ssem, rsem, hsend, hrecv,
):
    ix = lax.axis_index("gx")
    iy = lax.axis_index("gy")
    nx = lax.axis_size("gx")
    ny = lax.axis_size("gy")

    def device(dx, dy):
        return (lax.rem(ix + (dx + nx), nx), lax.rem(iy + (dy + ny), ny))

    loads = []
    for n, (src, dst) in enumerate((
        (pairs, PR), (kind, KD), (count, CT),
        (press, P_.at[pl.ds(0, COLS)]), (depth, D_.at[pl.ds(0, COLS)]),
        (sat.at[0], W_.at[pl.ds(0, COLS)]), (sat.at[1], O_.at[pl.ds(0, COLS)]),
        (table, TAB),
        (perm.at[0], KX), (perm.at[1], KY.at[pl.ds(0, COLS)]),
        (perm.at[2], KZ), (pore, PV),
    )):
        copy = pltpu.make_async_copy(src, dst, lsem.at[n])
        copy.start()
        loads.append(copy)

    offsets = [(dx, dy) for dx in (-1, 0, 1) for dy in (-1, 0, 1)]
    barrier = pltpu.get_barrier_semaphore()
    for dx, dy in offsets:
        if (dx, dy) != (0, 0):
            pl.semaphore_signal(barrier, inc=1, device_id=device(dx, dy), device_id_type=MESH)

    zero = jnp.zeros((TILE, NZ), jnp.float32)
    for ref in (P_, D_, W_, O_, KY):
        ref[pl.ds(COLS, TILE), :] = zero
    for f in range(3):
        for t in range(4):
            fxs[f, pl.ds(TILE * t, TILE), :] = zero
        for k in range(BLOCK):
            fys[k, f, pl.ds(0, TILE), :] = zero
        rows[f, pl.ds(32, TILE), :] = zero
        rows[f, pl.ds(SLOTS + 32, TILE), :] = zero

    for n in range(3):
        loads[n].wait()
    live = CT[0]
    log_y = ny.bit_length() - 1
    used = jnp.int32(0)
    words = [jnp.int32(0)] * CODES
    for r in range(32):
        target = PR[1, r]
        cx = ((target >> log_y) - ix + 1) & (nx - 1)
        cy = ((target & (ny - 1)) - iy + 1) & (ny - 1)
        code = cx * 3 + cy
        rank = (used >> (code * 3)) & 7
        on = jnp.where(r < live, 1, 0)
        used = used + (on << (code * 3))
        entry = ((r + 32) * on) << (rank * 6)
        for c in range(CODES):
            words[c] = words[c] + jnp.where(code == c, entry, 0)

    for n in range(3, 8):
        loads[n].wait()
    lane = lax.broadcasted_iota(jnp.int32, (1, NZ), 1)
    idx0 = jnp.full((1, NZ), -1, jnp.int32)
    idx1 = jnp.full((1, NZ), -1, jnp.int32)

    def place(idx0, idx1, k, value):
        for copy in range(3):
            at = 2 * SLOTS * copy + k
            if at < NZ:
                idx0 = jnp.where(lane == at, value, idx0)
            else:
                idx1 = jnp.where(lane == at - NZ, value, idx1)
        return idx0, idx1

    for c in range(CODES):
        for s in range(CAP):
            entry = words[c] >> (6 * s)
            r = entry & 31
            full = jnp.where((entry & 32) > 0, 1.0, 0.0)
            src = PR[0, r]
            land = PR[2, r]
            kd = KD[r]
            for q, ref in enumerate((P_, D_, W_, O_)):
                sreq[c, pl.ds(4 * q + s, 1), :] = ref[pl.ds(src, 1), :]
            sreq[c, pl.ds(16 + s, 1), :] = TAB[pl.ds(kd, 1), :] * full
            sidx[c, pl.ds(s, 1), :] = jnp.full((1, NZ), land, jnp.int32)
            idx0, idx1 = place(idx0, idx1, c * CAP + s, src)

    for side, y in ((0, NY - 1), (1, 0)):
        for q, ref in enumerate((P_, D_, W_, O_)):
            ysend[side, q] = ref[pl.ds(y, NX, NY), :]
    for n in range(8, 12):
        loads[n].wait()
    for side, y in ((0, NY - 1), (1, 0)):
        ysend[side, 4] = KY[pl.ds(y, NX, NY), :]

    pl.semaphore_wait(barrier, 8)

    requests = []
    for c in sorted(range(CODES), key=lambda c: -abs(offsets[c][0]) - abs(offsets[c][1])):
        if c == HERE:
            continue
        for part, (src, dst) in enumerate(((sreq, rreq), (sidx, ridx))):
            copy = pltpu.make_async_remote_copy(
                src_ref=src.at[c], dst_ref=dst.at[c],
                send_sem=ssem.at[part, c], recv_sem=rsem.at[part, c],
                device_id=device(*offsets[c]), device_id_type=MESH,
            )
            copy.start()
            requests.append(copy)
    halos = []
    for side, (dx, x) in enumerate(((1, NX - 1), (-1, 0))):
        for q, ref in enumerate((P_, D_, W_, O_, KX)):
            copy = pltpu.make_async_remote_copy(
                src_ref=ref.at[pl.ds(x * NY, NY)], dst_ref=hx.at[side, q],
                send_sem=hsend.at[side, q], recv_sem=hrecv.at[side, q],
                device_id=device(dx, 0), device_id_type=MESH,
            )
            copy.start()
            halos.append(copy)
    for side, dy in enumerate((1, -1)):
        copy = pltpu.make_async_remote_copy(
            src_ref=ysend.at[side], dst_ref=hy.at[side],
            send_sem=hsend.at[2 + side, 0], recv_sem=hrecv.at[2 + side, 0],
            device_id=device(0, dy), device_id_type=MESH,
        )
        copy.start()
        halos.append(copy)

    lanes = lax.broadcasted_iota(jnp.int32, (TILE, NZ), 1)
    sublanes = lax.broadcasted_iota(jnp.int32, (TILE, NZ), 0)
    last_lane = lanes == NZ - 1
    last_sub = sublanes == TILE - 1

    def block(b, carry):
        for t in range(4):
            base = b * (BLOCK * NY) + TILE * t
            at = pl.ds(pl.multiple_of(base, TILE), TILE)
            p, d, w, o, kx = P_[at, :], D_[at, :], W_[at, :], O_[at, :], KX[at, :]
            m = mobility(w, o)
            fx = [fxs[f, pl.ds(TILE * t, TILE), :] for f in range(3)]
            for k in range(BLOCK):
                row = b * BLOCK + k
                at = pl.ds(pl.multiple_of(base + k * NY, TILE), TILE)
                nrow = jnp.minimum(row + 1, NX - 1)
                nat = pl.ds(pl.multiple_of(nrow * NY + TILE * t, TILE), TILE)
                pn, dn, wn, on, kn = P_[nat, :], D_[nat, :], W_[nat, :], O_[nat, :], KX[nat, :]
                mn = mobility(wn, on)
                inside = jnp.where(row < NX - 1, 2.0, 0.0)
                gx = fluxes(p, d, m, pn, dn, mn, inside * kx * kn / (kx + kn))
                net = [gx[f] - fx[f] for f in range(3)]
                uat = pl.ds(base + k * NY + 1, TILE)
                ky, ku = KY[at, :], KY[uat, :]
                gy = fluxes(p, d, m, P_[uat, :], D_[uat, :], mobility(W_[uat, :], O_[uat, :]), harmonic(ky, ku))
                for f in range(3):
                    g = jnp.where(last_sub, 0.0, gy[f]) if t == 3 else gy[f]
                    fys[k, f, pl.ds(TILE + TILE * t, TILE), :] = g
                    net[f] = net[f] + (g - fys[k, f, pl.ds(TILE + TILE * t - 1, TILE), :])
                kz = KZ[at, :]
                up = lambda v: pltpu.roll(v, NZ - 1, 1)
                tz = jnp.where(last_lane, 0.0, harmonic(kz, up(kz)))
                gz = fluxes(p, d, m, up(p), up(d), [up(v) for v in m], tz)
                wt = STEP / PV[at, :]
                wgt[at, :] = wt
                sats = (w, o, 1.0 - w - o)
                for f in range(3):
                    total = net[f] + (gz[f] - pltpu.roll(gz[f], 1, 1))
                    acc[f, at, :] = sats[f] - wt * total
                p, d, w, o, kx, m, fx = pn, dn, wn, on, kn, mn, gx
            for f in range(3):
                fxs[f, pl.ds(TILE * t, TILE), :] = fx[f]
        return carry

    half = NX // BLOCK // 2
    lax.fori_loop(0, half, block, 0)

    for copy in requests:
        copy.wait_recv()
    lands = {}
    for c in range(CODES):
        ref = sidx if c == HERE else ridx
        for s in range(CAP):
            lands[c, s] = ref[c, pl.ds(s, 1), :][0, 0]
    for c in range(CODES):
        for s in range(CAP):
            for q, ref in enumerate((P_, D_, W_, O_)):
                loc[c, pl.ds(4 * q + s, 1), :] = ref[pl.ds(lands[c, s], 1), :]
    answers = []
    for c in sorted(range(CODES), key=lambda c: -abs(offsets[c][0]) - abs(offsets[c][1])):
        ref = sreq if c == HERE else rreq
        a = [ref[c, pl.ds(4 * q, 4), :] for q in range(5)]
        b = [loc[c, pl.ds(4 * q, 4), :] for q in range(4)]
        flow = fluxes(a[0], a[1], mobility(a[2], a[3]), b[0], b[1], mobility(b[2], b[3]), a[4])
        for f in range(3):
            sresp[c, pl.ds(4 * f, 4), :] = flow[f]
            rows[f, pl.ds(SLOTS + 4 * c, 4), :] = -flow[f]
            if c == HERE:
                rows[f, pl.ds(4 * c, 4), :] = flow[f]
        sresp[c, pl.ds(12, 4), :] = jnp.zeros((4, NZ), jnp.float32)
        if c == HERE:
            continue
        dx, dy = offsets[c]
        copy = pltpu.make_async_remote_copy(
            src_ref=sresp.at[c], dst_ref=rresp.at[c],
            send_sem=ssem.at[2, c], recv_sem=rsem.at[2, c],
            device_id=device(-dx, -dy), device_id_type=MESH,
        )
        copy.start()
        answers.append((c, copy))

    for c in range(CODES):
        for s in range(CAP):
            idx0, idx1 = place(idx0, idx1, SLOTS + c * CAP + s, lands[c, s])

    lax.fori_loop(half, 2 * half, block, 0)

    for copy in halos:
        copy.wait_recv()
    for axis, sides, local in (
        ("x", hx, lambda ref, side: ref[pl.ds((NX - 1) * NY if side else 0, NY), :]),
        ("y", hy, lambda ref, side: ref[pl.ds((NY - 1) if side else 0, NX, NY), :]),
    ):
        place_, count_ = (ix, nx) if axis == "x" else (iy, ny)
        for side in range(2):
            far = [sides[side, q] for q in range(5)]
            near = [local(r, side) for r in (P_, D_, W_, O_, KX if axis == "x" else KY)]
            inside = jnp.where(place_ == (count_ - 1 if side else 0), 0.0, 1.0)
            lo, hi = (near, far) if side else (far, near)
            flow = fluxes(
                lo[0], lo[1], mobility(lo[2], lo[3]), hi[0], hi[1], mobility(hi[2], hi[3]),
                inside * harmonic(lo[4], hi[4]),
            )
            wt = local(wgt, side)
            for f in range(3):
                step = wt * flow[f]
                if axis == "x":
                    at = pl.ds((NX - 1) * NY if side else 0, NY)
                else:
                    at = pl.ds((NY - 1) if side else 0, NX, NY)
                if side:
                    acc[f, at, :] = acc[f, at, :] - step
                else:
                    acc[f, at, :] = acc[f, at, :] + step

    idx = jnp.concatenate([idx0, idx1], axis=1)
    cell = lax.broadcasted_iota(jnp.int32, (32, 2 * NZ), 0)

    def mark(b, carry):
        start = pl.multiple_of(b * 32, 32)
        hot[pl.ds(start, 32), :] = jnp.where(cell + start == idx, 1.0, 0.0).astype(jnp.bfloat16)
        return carry

    lax.fori_loop(0, COLS // 32, mark, 0)

    for c, copy in answers:
        copy.wait_recv()
        for f in range(3):
            rows[f, pl.ds(4 * c, 4), :] = rresp[c, pl.ds(4 * f, 4), :]
    for copy in requests + halos:
        copy.wait_send()
    for _, copy in answers:
        copy.wait_send()


def add_kernel(acc, wgt, hot, rows, out, parts, held, sem):
    for f in range(3):
        value = rows[f]
        for k in range(3):
            part = value.astype(jnp.bfloat16)
            parts[pl.ds(2 * SLOTS * k, 2 * SLOTS), pl.ds(NZ * f, NZ)] = part
            value = value - part.astype(jnp.float32)
        parts[pl.ds(240, 16), pl.ds(NZ * f, NZ)] = jnp.zeros((16, NZ), jnp.bfloat16)
    size = COLS // 8
    copies = []
    for n in range(8):
        at = pl.ds(n * size, size)
        delta = jnp.dot(hot[at, :], parts[...], preferred_element_type=jnp.float32)
        wt = wgt[at, :]
        for f in range(3):
            held[f, at, :] = acc[f, at, :] - wt * delta[:, NZ * f:NZ * (f + 1)]
            copy = pltpu.make_async_copy(held.at[f, at], out.at[f, at], sem.at[n, f])
            copy.start()
            copies.append(copy)
    for copy in copies:
        copy.wait()


def body(pressure, depth, saturation, permeability, pore_volume, fault_pairs, fault_kind, fault_count, fault_table):
    f32, i32 = jnp.float32, jnp.int32
    hbm = pl.BlockSpec(memory_space=pltpu.HBM)
    vmem = pl.BlockSpec(memory_space=pltpu.VMEM)
    V = pltpu.VMEM
    acc, wgt, hot, rows = pl.pallas_call(
        grid_kernel,
        out_shape=(
            V((3, COLS, NZ), f32), V((COLS, NZ), f32), V((COLS, 2 * NZ), jnp.bfloat16), V((3, 2 * SLOTS, NZ), f32),
        ),
        in_specs=[hbm] * 9,
        out_specs=(vmem,) * 4,
        scratch_shapes=[
            V((COLS + TILE, NZ), f32), V((COLS + TILE, NZ), f32), V((COLS + TILE, NZ), f32), V((COLS + TILE, NZ), f32),
            V((COLS, NZ), f32), V((COLS + TILE, NZ), f32), V((COLS, NZ), f32), V((COLS, NZ), f32),
            V((16, NZ), f32),
            pltpu.SMEM((3, 32), i32), pltpu.SMEM((32,), i32), pltpu.SMEM((1,), i32),
            V((CODES, 24, NZ), f32), V((CODES, 8, NZ), i32), V((CODES, 24, NZ), f32), V((CODES, 8, NZ), i32),
            V((CODES, 16, NZ), f32), V((CODES, 16, NZ), f32), V((CODES, 16, NZ), f32),
            V((2, 5, NX, NZ), f32), V((2, 5, NY, NZ), f32), V((2, 5, NX, NZ), f32),
            V((3, NY, NZ), f32), V((BLOCK, 3, TILE + NY, NZ), f32),
            pltpu.SemaphoreType.DMA((12,)),
            pltpu.SemaphoreType.DMA((3, CODES)), pltpu.SemaphoreType.DMA((3, CODES)),
            pltpu.SemaphoreType.DMA((4, 5)), pltpu.SemaphoreType.DMA((4, 5)),
        ],
        compiler_params=pltpu.CompilerParams(collective_id=0, has_side_effects=True, vmem_limit_bytes=24 * 2**20),
        name="grid",
    )(
        pressure.reshape(COLS, NZ), depth.reshape(COLS, NZ), saturation.reshape(2, COLS, NZ),
        permeability.reshape(3, COLS, NZ), pore_volume.reshape(COLS, NZ),
        fault_pairs.T, fault_kind, fault_count, fault_table,
    )
    out = pl.pallas_call(
        add_kernel,
        out_shape=jax.ShapeDtypeStruct((3, COLS, NZ), f32),
        in_specs=[vmem] * 4,
        out_specs=hbm,
        scratch_shapes=[V((2 * NZ, 3 * NZ), jnp.bfloat16), V((3, COLS, NZ), f32), pltpu.SemaphoreType.DMA((8, 3))],
        compiler_params=pltpu.CompilerParams(vmem_limit_bytes=16 * 2**20),
        name="add",
    )(acc, wgt, hot, rows)
    return out.reshape(3, NX, NY, NZ)


def solution(mesh):
    in_specs = (
        P("gx", "gy", None),
        P("gx", "gy", None),
        P(None, "gx", "gy", None),
        P(None, "gx", "gy", None),
        P("gx", "gy", None),
        P(("gx", "gy"), None),
        P(("gx", "gy")),
        P(("gx", "gy")),
        P(),
    )
    out_specs = P(None, "gx", "gy", None)
    return jax.shard_map(body, mesh=mesh, in_specs=in_specs, out_specs=out_specs, check_vma=False)
```

```python
import jax
import jax.numpy as jnp
from jax import lax
from jax.experimental import pallas as pl
from jax.experimental.pallas import tpu as pltpu
from jax.sharding import PartitionSpec as P

CAP = 4
CODES = 9
HERE = 4
SLOTS = 40
RHO = (1.0, 0.8, 0.25)
STEP = 0.2
NX = 32
NY = 32
NZ = 128
COLS = NX * NY
TILE = 8
BLOCK = 2
MESH = pl.DeviceIdType.MESH


def mobility(sw, so):
    sg = 1.0 - sw - so
    return (sw * sw * 2.0, so * so, sg * sg * 4.0)


def harmonic(a, b):
    return 2.0 * a * b / (a + b)


def fluxes(pa, da, ma, pb, db, mb, trans):
    dp = pa - pb
    dd = da - db
    out = []
    for f in range(3):
        drive = dp - (dd if RHO[f] == 1.0 else RHO[f] * dd)
        out.append(trans * jnp.where(drive > 0.0, ma[f], mb[f]) * drive)
    return out


def grid_kernel(
    press, depth, sat, perm, pore, pairs, kind, table, CT,
    acc, wgt, hot, rows,
    P_, D_, W_, O_, KX, KY, KZ, PV, TAB, PR, KD,
    sreq, sidx, rreq, ridx, loc, sresp, rresp,
    ysend, hx, hy, fxs, fys,
    lsem, ssem, rsem, hsend, hrecv,
):
    ix = lax.axis_index("gx")
    iy = lax.axis_index("gy")
    nx = lax.axis_size("gx")
    ny = lax.axis_size("gy")

    def device(dx, dy):
        return (lax.rem(ix + (dx + nx), nx), lax.rem(iy + (dy + ny), ny))

    loads = []
    for n, (src, dst) in enumerate((
        (pairs, PR), (kind, KD),
        (press, P_.at[pl.ds(0, COLS)]), (depth, D_.at[pl.ds(0, COLS)]),
        (sat.at[0], W_.at[pl.ds(0, COLS)]), (sat.at[1], O_.at[pl.ds(0, COLS)]),
        (table, TAB),
        (perm.at[0], KX), (perm.at[1], KY.at[pl.ds(0, COLS)]),
        (perm.at[2], KZ), (pore, PV),
    )):
        copy = pltpu.make_async_copy(src, dst, lsem.at[n])
        copy.start()
        loads.append(copy)

    offsets = [(dx, dy) for dx in (-1, 0, 1) for dy in (-1, 0, 1)]
    barrier = pltpu.get_barrier_semaphore()
    for dx, dy in offsets:
        if (dx, dy) != (0, 0):
            pl.semaphore_signal(barrier, inc=1, device_id=device(dx, dy), device_id_type=MESH)

    zero = jnp.zeros((TILE, NZ), jnp.float32)
    for ref in (P_, D_, W_, O_, KY):
        ref[pl.ds(COLS, TILE), :] = zero
    for f in range(3):
        for t in range(4):
            fxs[f, pl.ds(TILE * t, TILE), :] = zero
        for k in range(BLOCK):
            fys[k, f, pl.ds(0, TILE), :] = zero
        rows[f, pl.ds(32, TILE), :] = zero
        rows[f, pl.ds(SLOTS + 32, TILE), :] = zero

    for n in range(2):
        loads[n].wait()
    live = CT[0]
    log_y = ny.bit_length() - 1
    used = jnp.int32(0)
    words = [jnp.int32(0)] * CODES
    for r in range(32):
        target = PR[1, r]
        cx = ((target >> log_y) - ix + 1) & (nx - 1)
        cy = ((target & (ny - 1)) - iy + 1) & (ny - 1)
        code = cx * 3 + cy
        rank = (used >> (code * 3)) & 7
        on = jnp.where(r < live, 1, 0)
        used = used + (on << (code * 3))
        entry = ((r + 32) * on) << (rank * 6)
        for c in range(CODES):
            words[c] = words[c] + jnp.where(code == c, entry, 0)

    for n in range(2, 7):
        loads[n].wait()
    lane = lax.broadcasted_iota(jnp.int32, (1, NZ), 1)
    idx0 = jnp.full((1, NZ), -1, jnp.int32)
    idx1 = jnp.full((1, NZ), -1, jnp.int32)

    def place(idx0, idx1, k, value):
        for copy in range(3):
            at = 2 * SLOTS * copy + k
            if at < NZ:
                idx0 = jnp.where(lane == at, value, idx0)
            else:
                idx1 = jnp.where(lane == at - NZ, value, idx1)
        return idx0, idx1

    for c in range(CODES):
        for s in range(CAP):
            entry = words[c] >> (6 * s)
            r = entry & 31
            full = jnp.where((entry & 32) > 0, 1.0, 0.0)
            src = PR[0, r]
            land = PR[2, r]
            kd = KD[r]
            for q, ref in enumerate((P_, D_, W_, O_)):
                sreq[c, pl.ds(4 * q + s, 1), :] = ref[pl.ds(src, 1), :]
            sreq[c, pl.ds(16 + s, 1), :] = TAB[pl.ds(kd, 1), :] * full
            sidx[c, pl.ds(s, 1), :] = jnp.full((1, NZ), land, jnp.int32)
            idx0, idx1 = place(idx0, idx1, c * CAP + s, src)

    for side, y in ((0, NY - 1), (1, 0)):
        for q, ref in enumerate((P_, D_, W_, O_)):
            ysend[side, q] = ref[pl.ds(y, NX, NY), :]
    for n in range(7, 11):
        loads[n].wait()
    for side, y in ((0, NY - 1), (1, 0)):
        ysend[side, 4] = KY[pl.ds(y, NX, NY), :]

    pl.semaphore_wait(barrier, 8)

    requests = []
    for c in sorted(range(CODES), key=lambda c: -abs(offsets[c][0]) - abs(offsets[c][1])):
        if c == HERE:
            continue
        for part, (src, dst) in enumerate(((sreq, rreq), (sidx, ridx))):
            copy = pltpu.make_async_remote_copy(
                src_ref=src.at[c], dst_ref=dst.at[c],
                send_sem=ssem.at[part, c], recv_sem=rsem.at[part, c],
                device_id=device(*offsets[c]), device_id_type=MESH,
            )
            copy.start()
            requests.append(copy)
    halos = []
    for side, (dx, x) in enumerate(((1, NX - 1), (-1, 0))):
        for q, ref in enumerate((P_, D_, W_, O_, KX)):
            copy = pltpu.make_async_remote_copy(
                src_ref=ref.at[pl.ds(x * NY, NY)], dst_ref=hx.at[side, q],
                send_sem=hsend.at[side, q], recv_sem=hrecv.at[side, q],
                device_id=device(dx, 0), device_id_type=MESH,
            )
            copy.start()
            halos.append(copy)
    for side, dy in enumerate((1, -1)):
        copy = pltpu.make_async_remote_copy(
            src_ref=ysend.at[side], dst_ref=hy.at[side],
            send_sem=hsend.at[2 + side, 0], recv_sem=hrecv.at[2 + side, 0],
            device_id=device(0, dy), device_id_type=MESH,
        )
        copy.start()
        halos.append(copy)

    lanes = lax.broadcasted_iota(jnp.int32, (TILE, NZ), 1)
    sublanes = lax.broadcasted_iota(jnp.int32, (TILE, NZ), 0)
    last_lane = lanes == NZ - 1
    last_sub = sublanes == TILE - 1

    def block(b, carry):
        for t in range(4):
            base = b * (BLOCK * NY) + TILE * t
            at = pl.ds(pl.multiple_of(base, TILE), TILE)
            p, d, w, o, kx = P_[at, :], D_[at, :], W_[at, :], O_[at, :], KX[at, :]
            m = mobility(w, o)
            fx = [fxs[f, pl.ds(TILE * t, TILE), :] for f in range(3)]
            for k in range(BLOCK):
                row = b * BLOCK + k
                at = pl.ds(pl.multiple_of(base + k * NY, TILE), TILE)
                nrow = jnp.minimum(row + 1, NX - 1)
                nat = pl.ds(pl.multiple_of(nrow * NY + TILE * t, TILE), TILE)
                pn, dn, wn, on, kn = P_[nat, :], D_[nat, :], W_[nat, :], O_[nat, :], KX[nat, :]
                mn = mobility(wn, on)
                inside = jnp.where(row < NX - 1, 2.0, 0.0)
                gx = fluxes(p, d, m, pn, dn, mn, inside * kx * kn / (kx + kn))
                net = [gx[f] - fx[f] for f in range(3)]
                uat = pl.ds(base + k * NY + 1, TILE)
                ky, ku = KY[at, :], KY[uat, :]
                gy = fluxes(p, d, m, P_[uat, :], D_[uat, :], mobility(W_[uat, :], O_[uat, :]), harmonic(ky, ku))
                for f in range(3):
                    g = jnp.where(last_sub, 0.0, gy[f]) if t == 3 else gy[f]
                    fys[k, f, pl.ds(TILE + TILE * t, TILE), :] = g
                    net[f] = net[f] + (g - fys[k, f, pl.ds(TILE + TILE * t - 1, TILE), :])
                kz = KZ[at, :]
                up = lambda v: pltpu.roll(v, NZ - 1, 1)
                tz = jnp.where(last_lane, 0.0, harmonic(kz, up(kz)))
                gz = fluxes(p, d, m, up(p), up(d), [up(v) for v in m], tz)
                wt = STEP / PV[at, :]
                wgt[at, :] = wt
                sats = (w, o, 1.0 - w - o)
                for f in range(3):
                    total = net[f] + (gz[f] - pltpu.roll(gz[f], 1, 1))
                    acc[f, at, :] = sats[f] - wt * total
                p, d, w, o, kx, m, fx = pn, dn, wn, on, kn, mn, gx
            for f in range(3):
                fxs[f, pl.ds(TILE * t, TILE), :] = fx[f]
        return carry

    half = NX // BLOCK // 2
    lax.fori_loop(0, half, block, 0)

    for copy in requests:
        copy.wait_recv()
    lands = {}
    for c in range(CODES):
        ref = sidx if c == HERE else ridx
        for s in range(CAP):
            lands[c, s] = ref[c, pl.ds(s, 1), :][0, 0]
    for c in range(CODES):
        for s in range(CAP):
            for q, ref in enumerate((P_, D_, W_, O_)):
                loc[c, pl.ds(4 * q + s, 1), :] = ref[pl.ds(lands[c, s], 1), :]
    answers = []
    for c in sorted(range(CODES), key=lambda c: -abs(offsets[c][0]) - abs(offsets[c][1])):
        ref = sreq if c == HERE else rreq
        a = [ref[c, pl.ds(4 * q, 4), :] for q in range(5)]
        b = [loc[c, pl.ds(4 * q, 4), :] for q in range(4)]
        flow = fluxes(a[0], a[1], mobility(a[2], a[3]), b[0], b[1], mobility(b[2], b[3]), a[4])
        for f in range(3):
            sresp[c, pl.ds(4 * f, 4), :] = flow[f]
            rows[f, pl.ds(SLOTS + 4 * c, 4), :] = -flow[f]
            if c == HERE:
                rows[f, pl.ds(4 * c, 4), :] = flow[f]
        sresp[c, pl.ds(12, 4), :] = jnp.zeros((4, NZ), jnp.float32)
        if c == HERE:
            continue
        dx, dy = offsets[c]
        copy = pltpu.make_async_remote_copy(
            src_ref=sresp.at[c], dst_ref=rresp.at[c],
            send_sem=ssem.at[2, c], recv_sem=rsem.at[2, c],
            device_id=device(-dx, -dy), device_id_type=MESH,
        )
        copy.start()
        answers.append((c, copy))

    for c in range(CODES):
        for s in range(CAP):
            idx0, idx1 = place(idx0, idx1, SLOTS + c * CAP + s, lands[c, s])

    lax.fori_loop(half, 2 * half, block, 0)

    for copy in halos:
        copy.wait_recv()
    for axis, sides, local in (
        ("x", hx, lambda ref, side: ref[pl.ds((NX - 1) * NY if side else 0, NY), :]),
        ("y", hy, lambda ref, side: ref[pl.ds((NY - 1) if side else 0, NX, NY), :]),
    ):
        place_, count_ = (ix, nx) if axis == "x" else (iy, ny)
        for side in range(2):
            far = [sides[side, q] for q in range(5)]
            near = [local(r, side) for r in (P_, D_, W_, O_, KX if axis == "x" else KY)]
            inside = jnp.where(place_ == (count_ - 1 if side else 0), 0.0, 1.0)
            lo, hi = (near, far) if side else (far, near)
            flow = fluxes(
                lo[0], lo[1], mobility(lo[2], lo[3]), hi[0], hi[1], mobility(hi[2], hi[3]),
                inside * harmonic(lo[4], hi[4]),
            )
            wt = local(wgt, side)
            for f in range(3):
                step = wt * flow[f]
                if axis == "x":
                    at = pl.ds((NX - 1) * NY if side else 0, NY)
                else:
                    at = pl.ds((NY - 1) if side else 0, NX, NY)
                if side:
                    acc[f, at, :] = acc[f, at, :] - step
                else:
                    acc[f, at, :] = acc[f, at, :] + step

    idx = jnp.concatenate([idx0, idx1], axis=1)
    cell = lax.broadcasted_iota(jnp.int32, (32, 2 * NZ), 0)

    def mark(b, carry):
        start = pl.multiple_of(b * 32, 32)
        hot[pl.ds(start, 32), :] = jnp.where(cell + start == idx, 1.0, 0.0).astype(jnp.bfloat16)
        return carry

    lax.fori_loop(0, COLS // 32, mark, 0)

    for c, copy in answers:
        copy.wait_recv()
        for f in range(3):
            rows[f, pl.ds(4 * c, 4), :] = rresp[c, pl.ds(4 * f, 4), :]
    for copy in requests + halos:
        copy.wait_send()
    for _, copy in answers:
        copy.wait_send()


def add_kernel(acc, wgt, hot, rows, out, parts, held, sem):
    for f in range(3):
        value = rows[f]
        for k in range(3):
            part = value.astype(jnp.bfloat16)
            parts[pl.ds(2 * SLOTS * k, 2 * SLOTS), pl.ds(NZ * f, NZ)] = part
            value = value - part.astype(jnp.float32)
        parts[pl.ds(240, 16), pl.ds(NZ * f, NZ)] = jnp.zeros((16, NZ), jnp.bfloat16)
    size = COLS // 8
    copies = []
    for n in range(8):
        at = pl.ds(n * size, size)
        delta = jnp.dot(hot[at, :], parts[...], preferred_element_type=jnp.float32)
        wt = wgt[at, :]
        for f in range(3):
            held[f, at, :] = acc[f, at, :] - wt * delta[:, NZ * f:NZ * (f + 1)]
            copy = pltpu.make_async_copy(held.at[f, at], out.at[f, at], sem.at[n, f])
            copy.start()
            copies.append(copy)
    for copy in copies:
        copy.wait()


def body(pressure, depth, saturation, permeability, pore_volume, fault_pairs, fault_kind, fault_count, fault_table):
    f32, i32 = jnp.float32, jnp.int32
    hbm = pl.BlockSpec(memory_space=pltpu.HBM)
    vmem = pl.BlockSpec(memory_space=pltpu.VMEM)
    V = pltpu.VMEM
    acc, wgt, hot, rows = pl.pallas_call(
        grid_kernel,
        out_shape=(
            V((3, COLS, NZ), f32), V((COLS, NZ), f32), V((COLS, 2 * NZ), jnp.bfloat16), V((3, 2 * SLOTS, NZ), f32),
        ),
        in_specs=[hbm] * 8 + [pl.BlockSpec(memory_space=pltpu.SMEM)],
        out_specs=(vmem,) * 4,
        scratch_shapes=[
            V((COLS + TILE, NZ), f32), V((COLS + TILE, NZ), f32), V((COLS + TILE, NZ), f32), V((COLS + TILE, NZ), f32),
            V((COLS, NZ), f32), V((COLS + TILE, NZ), f32), V((COLS, NZ), f32), V((COLS, NZ), f32),
            V((16, NZ), f32),
            pltpu.SMEM((3, 32), i32), pltpu.SMEM((32,), i32),
            V((CODES, 24, NZ), f32), V((CODES, 8, NZ), i32), V((CODES, 24, NZ), f32), V((CODES, 8, NZ), i32),
            V((CODES, 16, NZ), f32), V((CODES, 16, NZ), f32), V((CODES, 16, NZ), f32),
            V((2, 5, NX, NZ), f32), V((2, 5, NY, NZ), f32), V((2, 5, NX, NZ), f32),
            V((3, NY, NZ), f32), V((BLOCK, 3, TILE + NY, NZ), f32),
            pltpu.SemaphoreType.DMA((11,)),
            pltpu.SemaphoreType.DMA((3, CODES)), pltpu.SemaphoreType.DMA((3, CODES)),
            pltpu.SemaphoreType.DMA((4, 5)), pltpu.SemaphoreType.DMA((4, 5)),
        ],
        compiler_params=pltpu.CompilerParams(collective_id=0, has_side_effects=True, vmem_limit_bytes=24 * 2**20),
        name="grid",
    )(
        *(
            pltpu.with_memory_space_constraint(x, pltpu.HBM)
            for x in (
                pressure.reshape(COLS, NZ), depth.reshape(COLS, NZ), saturation.reshape(2, COLS, NZ),
                permeability.reshape(3, COLS, NZ), pore_volume.reshape(COLS, NZ),
                fault_pairs.T, fault_kind, fault_table,
            )
        ),
        fault_count,
    )
    out = pl.pallas_call(
        add_kernel,
        out_shape=jax.ShapeDtypeStruct((3, COLS, NZ), f32),
        in_specs=[vmem] * 4,
        out_specs=hbm,
        scratch_shapes=[V((2 * NZ, 3 * NZ), jnp.bfloat16), V((3, COLS, NZ), f32), pltpu.SemaphoreType.DMA((8, 3))],
        compiler_params=pltpu.CompilerParams(vmem_limit_bytes=16 * 2**20),
        name="add",
    )(acc, wgt, hot, rows)
    return out.reshape(3, NX, NY, NZ)


def solution(mesh):
    in_specs = (
        P("gx", "gy", None),
        P("gx", "gy", None),
        P(None, "gx", "gy", None),
        P(None, "gx", "gy", None),
        P("gx", "gy", None),
        P(("gx", "gy"), None),
        P(("gx", "gy")),
        P(("gx", "gy")),
        P(),
    )
    out_specs = P(None, "gx", "gy", None)
    return jax.shard_map(body, mesh=mesh, in_specs=in_specs, out_specs=out_specs, check_vma=False)
```

```python
import jax
import jax.numpy as jnp
from jax import lax
from jax.experimental import pallas as pl
from jax.experimental.pallas import tpu as pltpu
from jax.sharding import PartitionSpec as P

CAP = 4
CODES = 9
HERE = 4
SLOTS = 40
RHO = (1.0, 0.8, 0.25)
STEP = 0.2
NX = 32
NY = 32
NZ = 128
COLS = NX * NY
TILE = 8
LINE = 4
BLOCK = 2
MESH = pl.DeviceIdType.MESH


def mobility(sw, so):
    sg = 1.0 - sw - so
    return (sw * sw * 2.0, so * so, sg * sg * 4.0)


def harmonic(a, b):
    return 2.0 * a * b / (a + b)


def fluxes(pa, da, ma, pb, db, mb, trans):
    dp = pa - pb
    dd = da - db
    out = []
    for f in range(3):
        drive = dp - (dd if RHO[f] == 1.0 else RHO[f] * dd)
        out.append(trans * jnp.where(drive > 0.0, ma[f], mb[f]) * drive)
    return out


def grid_kernel(
    press, depth, sat, perm, pore, pairs, kind, table, CT,
    acc, wgt, hot, rows,
    X, K, PV, TAB, PR, KD,
    sreq, rreq, lreq, loc, sresp, rresp,
    ysend, hx, hy, fxs, fys,
    lsem, ssem, rsem, qsem, psem, hsend, hrecv,
):
    P_, D_, W_, O_ = (X.at[q] for q in range(4))
    KX, KY, KZ = (K.at[q] for q in range(3))
    cols = pl.ds(0, COLS)
    ix = lax.axis_index("gx")
    iy = lax.axis_index("gy")
    nx = lax.axis_size("gx")
    ny = lax.axis_size("gy")

    def device(dx, dy):
        return (lax.rem(ix + (dx + nx), nx), lax.rem(iy + (dy + ny), ny))

    offsets = [(dx, dy) for dx in (-1, 0, 1) for dy in (-1, 0, 1)]
    barrier = pltpu.get_barrier_semaphore()
    iz = lax.rem(ix, LINE)
    first = iz == 0
    last = iz == LINE - 1

    odd = lax.rem(iy, 2) == 1

    def greet(dx, dy):
        pl.semaphore_signal(barrier, inc=1, device_id=device(dx, dy), device_id_type=MESH)

    for dx, dy in offsets:
        if dx != 1 and (dx, dy) != (0, 0):
            greet(dx, dy)

    @pl.when(jnp.logical_not(last))
    def _():
        for dy in (-1, 0, 1):
            greet(1, dy)

    @pl.when(jnp.logical_and(first, odd))
    def _():
        for dy in (-2, -1, 0, 1):
            greet(LINE, dy)

    @pl.when(jnp.logical_and(last, odd))
    def _():
        greet(1 - LINE, 0)

    @pl.when(jnp.logical_and(last, jnp.logical_not(odd)))
    def _():
        greet(1 - LINE, 1)

    loads = [
        pltpu.make_async_copy(src, dst, lsem.at[n])
        for n, src, dst in (
            (0, pairs, PR), (1, kind, KD),
            (2, press, X.at[0, cols]), (2, depth, X.at[1, cols]), (2, sat, X.at[pl.ds(2, 2), cols]),
            (3, table, TAB), (4, perm, K.at[:, cols]), (5, pore, PV),
        )
    ]
    for copy in loads:
        copy.start()
    state = pltpu.make_async_copy(X.at[:, cols], X.at[:, cols], lsem.at[2])

    zero = jnp.zeros((TILE, NZ), jnp.float32)
    for q in range(4):
        X[q, pl.ds(COLS, TILE), :] = zero
    K[1, pl.ds(COLS, TILE), :] = zero
    for f in range(3):
        for t in range(4):
            fxs[f, pl.ds(TILE * t, TILE), :] = zero
        for k in range(BLOCK):
            fys[k, f, pl.ds(0, TILE), :] = zero
        rows[f, pl.ds(32, TILE), :] = zero
        rows[f, pl.ds(SLOTS + 32, TILE), :] = zero

    for n in range(2):
        loads[n].wait()
    live = CT[0]
    log_y = ny.bit_length() - 1
    used = jnp.int32(0)
    words = [jnp.int32(0)] * CODES
    for r in range(32):
        target = PR[1, r]
        cx = ((target >> log_y) - ix + 1) & (nx - 1)
        cy = ((target & (ny - 1)) - iy + 1) & (ny - 1)
        code = cx * 3 + cy
        rank = (used >> (code * 3)) & 7
        on = jnp.where(r < live, 1, 0)
        used = used + (on << (code * 3))
        entry = ((r + 32) * on) << (rank * 6)
        for c in range(CODES):
            words[c] = words[c] + jnp.where(code == c, entry, 0)

    state.wait()
    loads[5].wait()
    lane = lax.broadcasted_iota(jnp.int32, (1, NZ), 1)
    idx0 = jnp.full((1, NZ), -1, jnp.int32)
    idx1 = jnp.full((1, NZ), -1, jnp.int32)

    def place(idx0, idx1, k, value):
        for copy in range(3):
            at = 2 * SLOTS * copy + k
            if at < NZ:
                idx0 = jnp.where(lane == at, value, idx0)
            else:
                idx1 = jnp.where(lane == at - NZ, value, idx1)
        return idx0, idx1

    for c in range(CODES):
        for s in range(CAP):
            entry = words[c] >> (6 * s)
            r = entry & 31
            full = jnp.where((entry & 32) > 0, 1.0, 0.0)
            src = PR[0, r]
            land = PR[2, r]
            kd = KD[r]
            for q, ref in enumerate((P_, D_, W_, O_)):
                sreq[c, pl.ds(4 * q + s, 1), :] = ref[pl.ds(src, 1), :]
            sreq[c, pl.ds(16 + s, 1), :] = TAB[pl.ds(kd, 1), :] * full
            sreq[c, pl.ds(20 + s, 1), :] = jnp.full((1, NZ), land, jnp.int32).astype(jnp.float32)
            idx0, idx1 = place(idx0, idx1, c * CAP + s, src)

    pl.semaphore_wait(barrier, jnp.where(first, jnp.where(odd, 9, 7), 8))

    def request(c, target):
        return pltpu.make_async_remote_copy(
            src_ref=sreq.at[c], dst_ref=rreq.at[c], send_sem=ssem.at[0], recv_sem=rsem.at[0],
            device_id=target, device_id_type=MESH,
        )

    def to_relay(c, to_odd):
        dx, dy = offsets[c]
        k = c if to_odd else 3 + c
        return pltpu.make_async_remote_copy(
            src_ref=sreq.at[c], dst_ref=lreq.at[k], send_sem=ssem.at[0], recv_sem=qsem.at[k],
            device_id=device(-LINE, dy if to_odd else dy + 1), device_id_type=MESH,
        )

    for own_odd in (False, True):
        @pl.when(jnp.logical_and(first, odd if own_odd else jnp.logical_not(odd)))
        def _(own_odd=own_odd):
            for c in (0, 2, 1):
                to_relay(c, own_odd == (c == 1)).start()

    @pl.when(jnp.logical_not(first))
    def _():
        for c in (0, 2, 1):
            request(c, device(*offsets[c])).start()

    for c in (6, 8, 3, 5, 7):
        request(c, device(*offsets[c])).start()
    eight = pl.ds(0, 8)
    requests = pltpu.make_async_remote_copy(
        src_ref=sreq.at[eight], dst_ref=rreq.at[eight], send_sem=ssem.at[0], recv_sem=rsem.at[0],
        device_id=device(0, 1), device_id_type=MESH,
    )

    for side, y in ((0, NY - 1), (1, 0)):
        for q, ref in enumerate((P_, D_, W_, O_)):
            ysend[side, q] = ref[pl.ds(y, NX, NY), :]
    for n in range(6, 8):
        loads[n].wait()
    for side, y in ((0, NY - 1), (1, 0)):
        ysend[side, 4] = KY[pl.ds(y, NX, NY), :]

    def halo(src, dst, n, dx, dy):
        return pltpu.make_async_remote_copy(
            src_ref=src, dst_ref=dst, send_sem=hsend.at[n], recv_sem=hrecv.at[n],
            device_id=device(dx, dy), device_id_type=MESH,
        )

    halos_x = []
    for side, (dx, x) in enumerate(((1, NX - 1), (-1, 0))):
        row = pl.ds(x * NY, NY)
        halos_x.append([
            halo(X.at[:, row], hx.at[side, pl.ds(0, 4)], side, dx, 0),
            halo(K.at[0, row], hx.at[side, 4], side, dx, 0),
        ])
    whole_x = [halo(hx.at[side], hx.at[side], side, dx, 0) for side, dx in enumerate((1, -1))]
    halos_y = [halo(ysend.at[side], hy.at[side], 2 + side, 0, dy) for side, dy in enumerate((1, -1))]
    goes = (ix < nx - 1, ix > 0, iy < ny - 1, iy > 0)
    comes = (goes[1], goes[0], goes[3], goes[2])

    @pl.when(goes[0])
    def _():
        for copy in halos_x[0]:
            copy.start()

    @pl.when(jnp.logical_not(first))
    def _():
        for copy in halos_x[1]:
            copy.start()

    for side in range(2):
        @pl.when(goes[2 + side])
        def _(side=side):
            halos_y[side].start()

    lanes = lax.broadcasted_iota(jnp.int32, (TILE, NZ), 1)
    sublanes = lax.broadcasted_iota(jnp.int32, (TILE, NZ), 0)
    last_lane = lanes == NZ - 1
    last_sub = sublanes == TILE - 1

    def block(b, carry):
        for t in range(4):
            base = b * (BLOCK * NY) + TILE * t
            at = pl.ds(pl.multiple_of(base, TILE), TILE)
            p, d, w, o, kx = P_[at, :], D_[at, :], W_[at, :], O_[at, :], KX[at, :]
            m = mobility(w, o)
            fx = [fxs[f, pl.ds(TILE * t, TILE), :] for f in range(3)]
            for k in range(BLOCK):
                row = b * BLOCK + k
                at = pl.ds(pl.multiple_of(base + k * NY, TILE), TILE)
                nrow = jnp.minimum(row + 1, NX - 1)
                nat = pl.ds(pl.multiple_of(nrow * NY + TILE * t, TILE), TILE)
                pn, dn, wn, on, kn = P_[nat, :], D_[nat, :], W_[nat, :], O_[nat, :], KX[nat, :]
                mn = mobility(wn, on)
                inside = jnp.where(row < NX - 1, 2.0, 0.0)
                gx = fluxes(p, d, m, pn, dn, mn, inside * kx * kn / (kx + kn))
                net = [gx[f] - fx[f] for f in range(3)]
                uat = pl.ds(base + k * NY + 1, TILE)
                ky, ku = KY[at, :], KY[uat, :]
                gy = fluxes(p, d, m, P_[uat, :], D_[uat, :], mobility(W_[uat, :], O_[uat, :]), harmonic(ky, ku))
                for f in range(3):
                    g = jnp.where(last_sub, 0.0, gy[f]) if t == 3 else gy[f]
                    fys[k, f, pl.ds(TILE + TILE * t, TILE), :] = g
                    net[f] = net[f] + (g - fys[k, f, pl.ds(TILE + TILE * t - 1, TILE), :])
                kz = KZ[at, :]
                up = lambda v: pltpu.roll(v, NZ - 1, 1)
                tz = jnp.where(last_lane, 0.0, harmonic(kz, up(kz)))
                gz = fluxes(p, d, m, up(p), up(d), [up(v) for v in m], tz)
                wt = STEP / PV[at, :]
                wgt[at, :] = wt
                sats = (w, o, 1.0 - w - o)
                for f in range(3):
                    total = net[f] + (gz[f] - pltpu.roll(gz[f], 1, 1))
                    acc[f, at, :] = sats[f] - wt * total
                p, d, w, o, kx, m, fx = pn, dn, wn, on, kn, mn, gx
            for f in range(3):
                fxs[f, pl.ds(TILE * t, TILE), :] = fx[f]
        return carry

    half = NX // BLOCK // 2
    lax.fori_loop(0, half, block, 0)

    relays = pltpu.make_async_remote_copy(
        src_ref=lreq, dst_ref=rreq.at[pl.ds(0, 6)], send_sem=psem.at[0], recv_sem=rsem.at[0],
        device_id=device(LINE - 1, 0), device_id_type=MESH,
    )

    @pl.when(jnp.logical_and(first, odd))
    def _():
        for k in (1, 4, 0, 2, 3, 5):
            c = k % 3
            to_relay(c, k < 3).wait_recv()
            pltpu.make_async_remote_copy(
                src_ref=lreq.at[k], dst_ref=rreq.at[c], send_sem=psem.at[0], recv_sem=rsem.at[0],
                device_id=device(LINE - 1, 0 if k < 3 else -1), device_id_type=MESH,
            ).start()

    requests.wait_recv()
    lands = {}
    for c in range(CODES):
        ref = sreq if c == HERE else rreq
        for s in range(CAP):
            lands[c, s] = jnp.clip(ref[c, pl.ds(20 + s, 1), :].astype(jnp.int32), 0, COLS - 1)[0, 0]
    for c in range(CODES):
        for s in range(CAP):
            for q, ref in enumerate((P_, D_, W_, O_)):
                loc[c, pl.ds(4 * q + s, 1), :] = ref[pl.ds(lands[c, s], 1), :]
    for c in sorted(range(CODES), key=lambda c: -abs(offsets[c][0]) - abs(offsets[c][1])):
        ref = sreq if c == HERE else rreq
        a = [ref[c, pl.ds(4 * q, 4), :] for q in range(5)]
        b = [loc[c, pl.ds(4 * q, 4), :] for q in range(4)]
        flow = fluxes(a[0], a[1], mobility(a[2], a[3]), b[0], b[1], mobility(b[2], b[3]), a[4])
        for f in range(3):
            sresp[c, pl.ds(4 * f, 4), :] = flow[f]
            rows[f, pl.ds(SLOTS + 4 * c, 4), :] = -flow[f]
            if c == HERE:
                rows[f, pl.ds(4 * c, 4), :] = flow[f]
        sresp[c, pl.ds(12, 4), :] = jnp.zeros((4, NZ), jnp.float32)
        if c == HERE:
            continue
        dx, dy = offsets[c]
        copy = pltpu.make_async_remote_copy(
            src_ref=sresp.at[c], dst_ref=rresp.at[c],
            send_sem=ssem.at[1], recv_sem=rsem.at[1],
            device_id=device(-dx, -dy), device_id_type=MESH,
        )
        copy.start()
    answers = pltpu.make_async_remote_copy(
        src_ref=sresp.at[eight], dst_ref=rresp.at[eight], send_sem=ssem.at[1], recv_sem=rsem.at[1],
        device_id=device(0, 1), device_id_type=MESH,
    )

    @pl.when(jnp.logical_and(first, goes[1]))
    def _():
        for copy in halos_x[1]:
            copy.start()

    for c in range(CODES):
        for s in range(CAP):
            idx0, idx1 = place(idx0, idx1, SLOTS + c * CAP + s, lands[c, s])

    lax.fori_loop(half, 2 * half, block, 0)

    def face(axis, side):
        far = [(hy if axis else hx)[side, q] for q in range(5)]
        if axis:
            at = pl.ds((NY - 1) if side else 0, NX, NY)
        else:
            at = pl.ds((NX - 1) * NY if side else 0, NY)
        near = [ref[at, :] for ref in (P_, D_, W_, O_, KY if axis else KX)]
        lo, hi = (near, far) if side else (far, near)
        flow = fluxes(
            lo[0], lo[1], mobility(lo[2], lo[3]), hi[0], hi[1], mobility(hi[2], hi[3]), harmonic(lo[4], hi[4])
        )
        wt = wgt[at, :]
        for f in range(3):
            step = wt * flow[f]
            acc[f, at, :] = acc[f, at, :] + (-step if side else step)

    for axis in range(2):
        for side in range(2):
            @pl.when(comes[2 * axis + side])
            def _(axis=axis, side=side):
                if axis:
                    halos_y[side].wait_recv()
                else:
                    whole_x[side].wait_recv()
                face(axis, side)

    idx = jnp.concatenate([idx0, idx1], axis=1)
    cell = lax.broadcasted_iota(jnp.int32, (32, 2 * NZ), 0)

    def mark(b, carry):
        start = pl.multiple_of(b * 32, 32)
        hot[pl.ds(start, 32), :] = jnp.where(cell + start == idx, 1.0, 0.0).astype(jnp.bfloat16)
        return carry

    lax.fori_loop(0, COLS // 32, mark, 0)

    answers.wait_recv()
    for c in range(CODES):
        if c != HERE:
            for f in range(3):
                rows[f, pl.ds(4 * c, 4), :] = rresp[c, pl.ds(4 * f, 4), :]
    requests.wait_send()
    answers.wait_send()
    for side in range(2):
        @pl.when(goes[side])
        def _(side=side):
            whole_x[side].wait_send()

        @pl.when(goes[2 + side])
        def _(side=side):
            halos_y[side].wait_send()

    @pl.when(jnp.logical_and(first, odd))
    def _():
        relays.wait_send()


def add_kernel(acc, wgt, hot, rows, out, parts, held, sem):
    for f in range(3):
        value = rows[f]
        for k in range(3):
            part = value.astype(jnp.bfloat16)
            parts[pl.ds(2 * SLOTS * k, 2 * SLOTS), pl.ds(NZ * f, NZ)] = part
            value = value - part.astype(jnp.float32)
        parts[pl.ds(240, 16), pl.ds(NZ * f, NZ)] = jnp.zeros((16, NZ), jnp.bfloat16)
    size = COLS // 8
    for n in range(8):
        at = pl.ds(n * size, size)
        delta = jnp.dot(hot[at, :], parts[...], preferred_element_type=jnp.float32)
        wt = wgt[at, :]
        for f in range(3):
            held[f, at, :] = acc[f, at, :] - wt * delta[:, NZ * f:NZ * (f + 1)]
            pltpu.make_async_copy(held.at[f, at], out.at[f, at], sem).start()
    pltpu.make_async_copy(held, out, sem).wait()


def body(pressure, depth, saturation, permeability, pore_volume, fault_pairs, fault_kind, fault_count, fault_table):
    f32, i32 = jnp.float32, jnp.int32
    hbm = pl.BlockSpec(memory_space=pltpu.HBM)
    vmem = pl.BlockSpec(memory_space=pltpu.VMEM)
    V = pltpu.VMEM
    acc, wgt, hot, rows = pl.pallas_call(
        grid_kernel,
        out_shape=(
            V((3, COLS, NZ), f32), V((COLS, NZ), f32), V((COLS, 2 * NZ), jnp.bfloat16), V((3, 2 * SLOTS, NZ), f32),
        ),
        in_specs=[hbm] * 8 + [pl.BlockSpec(memory_space=pltpu.SMEM)],
        out_specs=(vmem,) * 4,
        scratch_shapes=[
            V((4, COLS + TILE, NZ), f32), V((3, COLS + TILE, NZ), f32), V((COLS, NZ), f32), V((16, NZ), f32),
            pltpu.SMEM((3, 32), i32), pltpu.SMEM((32,), i32),
            V((CODES, 24, NZ), f32), V((CODES, 24, NZ), f32), V((6, 24, NZ), f32), V((CODES, 24, NZ), f32),
            V((CODES, 16, NZ), f32), V((CODES, 16, NZ), f32),
            V((2, 5, NX, NZ), f32), V((2, 5, NY, NZ), f32), V((2, 5, NX, NZ), f32),
            V((3, NY, NZ), f32), V((BLOCK, 3, TILE + NY, NZ), f32),
            pltpu.SemaphoreType.DMA((6,)), pltpu.SemaphoreType.DMA((2,)), pltpu.SemaphoreType.DMA((2,)),
            pltpu.SemaphoreType.DMA((6,)), pltpu.SemaphoreType.DMA((1,)),
            pltpu.SemaphoreType.DMA((4,)), pltpu.SemaphoreType.DMA((4,)),
        ],
        compiler_params=pltpu.CompilerParams(collective_id=0, has_side_effects=True, vmem_limit_bytes=24 * 2**20),
        name="grid",
    )(
        *(
            pltpu.with_memory_space_constraint(x, pltpu.HBM)
            for x in (
                pressure.reshape(COLS, NZ), depth.reshape(COLS, NZ), saturation.reshape(2, COLS, NZ),
                permeability.reshape(3, COLS, NZ), pore_volume.reshape(COLS, NZ),
                fault_pairs.T, fault_kind, fault_table,
            )
        ),
        fault_count,
    )
    out = pl.pallas_call(
        add_kernel,
        out_shape=jax.ShapeDtypeStruct((3, COLS, NZ), f32),
        in_specs=[vmem] * 4,
        out_specs=hbm,
        scratch_shapes=[V((2 * NZ, 3 * NZ), jnp.bfloat16), V((3, COLS, NZ), f32), pltpu.SemaphoreType.DMA],
        compiler_params=pltpu.CompilerParams(vmem_limit_bytes=16 * 2**20),
        name="add",
    )(acc, wgt, hot, rows)
    return out.reshape(3, NX, NY, NZ)


def solution(mesh):
    in_specs = (
        P("gx", "gy", None),
        P("gx", "gy", None),
        P(None, "gx", "gy", None),
        P(None, "gx", "gy", None),
        P("gx", "gy", None),
        P(("gx", "gy"), None),
        P(("gx", "gy")),
        P(("gx", "gy")),
        P(),
    )
    out_specs = P(None, "gx", "gy", None)
    return jax.shard_map(body, mesh=mesh, in_specs=in_specs, out_specs=out_specs, check_vma=False)
```

```python
import jax
import jax.numpy as jnp
from jax import lax
from jax.experimental import pallas as pl
from jax.experimental.pallas import tpu as pltpu
from jax.sharding import PartitionSpec as P

CAP = 4
CODES = 9
HERE = 4
SLOTS = 40
RHO = (1.0, 0.8, 0.25)
STEP = 0.2
NX = 32
NY = 32
NZ = 128
COLS = NX * NY
TILE = 8
LINE = 4
BLOCK = 2
RELAY_AT = 6
MESH = pl.DeviceIdType.MESH


def mobility(sw, so):
    sg = 1.0 - sw - so
    return (sw * sw * 2.0, so * so, sg * sg * 4.0)


def harmonic(a, b):
    return 2.0 * a * b / (a + b)


def fluxes(pa, da, ma, pb, db, mb, trans):
    dp = pa - pb
    dd = da - db
    out = []
    for f in range(3):
        drive = dp - (dd if RHO[f] == 1.0 else RHO[f] * dd)
        out.append(trans * jnp.where(drive > 0.0, ma[f], mb[f]) * drive)
    return out


def grid_kernel(
    press, depth, sat, perm, pore, pairs, kind, table, CT,
    acc, wgt, hot, rows,
    X, K, PV, TAB, PR, KD,
    sreq, rreq, lreq, loc, sresp, rresp,
    ysend, hx, hy, fxs, fys,
    lsem, ssem, rsem, qsem, psem, hsend, hrecv, open_,
):
    P_, D_, W_, O_ = (X.at[q] for q in range(4))
    KX, KY, KZ = (K.at[q] for q in range(3))
    cols = pl.ds(0, COLS)
    ix = lax.axis_index("gx")
    iy = lax.axis_index("gy")
    nx = lax.axis_size("gx")
    ny = lax.axis_size("gy")

    def device(dx, dy):
        return (lax.rem(ix + (dx + nx), nx), lax.rem(iy + (dy + ny), ny))

    offsets = [(dx, dy) for dx in (-1, 0, 1) for dy in (-1, 0, 1)]
    barrier = pltpu.get_barrier_semaphore()
    iz = lax.rem(ix, LINE)
    first = iz == 0
    last = iz == LINE - 1

    odd = lax.rem(iy, 2) == 1

    def greet(dx, dy):
        pl.semaphore_signal(barrier, inc=1, device_id=device(dx, dy), device_id_type=MESH)

    for dx, dy in offsets:
        if dx != 1 and (dx, dy) != (0, 0):
            greet(dx, dy)

    @pl.when(jnp.logical_not(last))
    def _():
        for dy in (-1, 0, 1):
            greet(1, dy)

    @pl.when(jnp.logical_and(first, odd))
    def _():
        for dy in (-2, -1, 0, 1):
            greet(LINE, dy)

    @pl.when(jnp.logical_and(first, odd))
    def _():
        for dy in (-1, 0):
            greet(LINE - 1, dy)

    loads = [
        pltpu.make_async_copy(src, dst, lsem.at[n])
        for n, src, dst in (
            (0, pairs, PR), (1, kind, KD),
            (2, press, X.at[0, cols]), (2, depth, X.at[1, cols]), (2, sat, X.at[pl.ds(2, 2), cols]),
            (3, table, TAB), (4, perm, K.at[:, cols]), (5, pore, PV),
        )
    ]
    for copy in loads:
        copy.start()
    state = pltpu.make_async_copy(X.at[:, cols], X.at[:, cols], lsem.at[2])

    zero = jnp.zeros((TILE, NZ), jnp.float32)
    for q in range(4):
        X[q, pl.ds(COLS, TILE), :] = zero
    K[1, pl.ds(COLS, TILE), :] = zero
    for f in range(3):
        for t in range(4):
            fxs[f, pl.ds(TILE * t, TILE), :] = zero
        for k in range(BLOCK):
            fys[k, f, pl.ds(0, TILE), :] = zero
        rows[f, pl.ds(32, TILE), :] = zero
        rows[f, pl.ds(SLOTS + 32, TILE), :] = zero

    for n in range(2):
        loads[n].wait()
    live = CT[0]
    log_y = ny.bit_length() - 1
    used = jnp.int32(0)
    words = [jnp.int32(0)] * CODES
    for r in range(32):
        target = PR[1, r]
        cx = ((target >> log_y) - ix + 1) & (nx - 1)
        cy = ((target & (ny - 1)) - iy + 1) & (ny - 1)
        code = cx * 3 + cy
        rank = (used >> (code * 3)) & 7
        on = jnp.where(r < live, 1, 0)
        used = used + (on << (code * 3))
        entry = ((r + 32) * on) << (rank * 6)
        for c in range(CODES):
            words[c] = words[c] + jnp.where(code == c, entry, 0)

    @pl.when(last)
    def _():
        pl.semaphore_wait(barrier, 9)

    for own_odd in (False, True):
        @pl.when(jnp.logical_and(last, odd if own_odd else jnp.logical_not(odd)))
        def _(own_odd=own_odd):
            pl.semaphore_signal(
                open_.at[0 if own_odd else 1], inc=1, device_id=device(1 - LINE, 0 if own_odd else 1),
                device_id_type=MESH,
            )

    state.wait()
    loads[5].wait()
    lane = lax.broadcasted_iota(jnp.int32, (1, NZ), 1)
    idx0 = jnp.full((1, NZ), -1, jnp.int32)
    idx1 = jnp.full((1, NZ), -1, jnp.int32)

    def place(idx0, idx1, k, value):
        for copy in range(3):
            at = 2 * SLOTS * copy + k
            if at < NZ:
                idx0 = jnp.where(lane == at, value, idx0)
            else:
                idx1 = jnp.where(lane == at - NZ, value, idx1)
        return idx0, idx1

    for c in range(CODES):
        for s in range(CAP):
            entry = words[c] >> (6 * s)
            r = entry & 31
            full = jnp.where((entry & 32) > 0, 1.0, 0.0)
            src = PR[0, r]
            land = PR[2, r]
            kd = KD[r]
            for q, ref in enumerate((P_, D_, W_, O_)):
                sreq[c, pl.ds(4 * q + s, 1), :] = ref[pl.ds(src, 1), :]
            sreq[c, pl.ds(16 + s, 1), :] = TAB[pl.ds(kd, 1), :] * full
            sreq[c, pl.ds(20 + s, 1), :] = jnp.full((1, NZ), land, jnp.int32).astype(jnp.float32)
            idx0, idx1 = place(idx0, idx1, c * CAP + s, src)

    @pl.when(jnp.logical_not(last))
    def _():
        pl.semaphore_wait(barrier, jnp.where(first, 7, 8))


    def request(c, target):
        return pltpu.make_async_remote_copy(
            src_ref=sreq.at[c], dst_ref=rreq.at[c], send_sem=ssem.at[0], recv_sem=rsem.at[0],
            device_id=target, device_id_type=MESH,
        )

    def to_relay(c, to_odd):
        dx, dy = offsets[c]
        k = c if to_odd else 3 + c
        return pltpu.make_async_remote_copy(
            src_ref=sreq.at[c], dst_ref=lreq.at[k], send_sem=ssem.at[0], recv_sem=qsem.at[k],
            device_id=device(-LINE, dy if to_odd else dy + 1), device_id_type=MESH,
        )

    for own_odd in (False, True):
        @pl.when(jnp.logical_and(first, odd if own_odd else jnp.logical_not(odd)))
        def _(own_odd=own_odd):
            for c in (0, 2, 1):
                to_relay(c, own_odd == (c == 1)).start()

    @pl.when(jnp.logical_not(first))
    def _():
        for c in (0, 2, 1):
            request(c, device(*offsets[c])).start()

    for c in (6, 8, 3, 5, 7):
        request(c, device(*offsets[c])).start()
    eight = pl.ds(0, 8)
    requests = pltpu.make_async_remote_copy(
        src_ref=sreq.at[eight], dst_ref=rreq.at[eight], send_sem=ssem.at[0], recv_sem=rsem.at[0],
        device_id=device(0, 1), device_id_type=MESH,
    )

    for side, y in ((0, NY - 1), (1, 0)):
        for q, ref in enumerate((P_, D_, W_, O_)):
            ysend[side, q] = ref[pl.ds(y, NX, NY), :]
    for n in range(6, 8):
        loads[n].wait()
    for side, y in ((0, NY - 1), (1, 0)):
        ysend[side, 4] = KY[pl.ds(y, NX, NY), :]

    def halo(src, dst, n, dx, dy):
        return pltpu.make_async_remote_copy(
            src_ref=src, dst_ref=dst, send_sem=hsend.at[n], recv_sem=hrecv.at[n],
            device_id=device(dx, dy), device_id_type=MESH,
        )

    halos_x = []
    for side, (dx, x) in enumerate(((1, NX - 1), (-1, 0))):
        row = pl.ds(x * NY, NY)
        halos_x.append([
            halo(X.at[:, row], hx.at[side, pl.ds(0, 4)], side, dx, 0),
            halo(K.at[0, row], hx.at[side, 4], side, dx, 0),
        ])
    whole_x = [halo(hx.at[side], hx.at[side], side, dx, 0) for side, dx in enumerate((1, -1))]
    halos_y = [halo(ysend.at[side], hy.at[side], 2 + side, 0, dy) for side, dy in enumerate((1, -1))]
    goes = (ix < nx - 1, ix > 0, iy < ny - 1, iy > 0)
    comes = (goes[1], goes[0], goes[3], goes[2])

    @pl.when(goes[0])
    def _():
        for copy in halos_x[0]:
            copy.start()

    @pl.when(jnp.logical_not(first))
    def _():
        for copy in halos_x[1]:
            copy.start()

    for side in range(2):
        @pl.when(goes[2 + side])
        def _(side=side):
            halos_y[side].start()

    lanes = lax.broadcasted_iota(jnp.int32, (TILE, NZ), 1)
    sublanes = lax.broadcasted_iota(jnp.int32, (TILE, NZ), 0)
    last_lane = lanes == NZ - 1
    last_sub = sublanes == TILE - 1

    def block(b, carry):
        for t in range(4):
            base = b * (BLOCK * NY) + TILE * t
            at = pl.ds(pl.multiple_of(base, TILE), TILE)
            p, d, w, o, kx = P_[at, :], D_[at, :], W_[at, :], O_[at, :], KX[at, :]
            m = mobility(w, o)
            fx = [fxs[f, pl.ds(TILE * t, TILE), :] for f in range(3)]
            for k in range(BLOCK):
                row = b * BLOCK + k
                at = pl.ds(pl.multiple_of(base + k * NY, TILE), TILE)
                nrow = jnp.minimum(row + 1, NX - 1)
                nat = pl.ds(pl.multiple_of(nrow * NY + TILE * t, TILE), TILE)
                pn, dn, wn, on, kn = P_[nat, :], D_[nat, :], W_[nat, :], O_[nat, :], KX[nat, :]
                mn = mobility(wn, on)
                inside = jnp.where(row < NX - 1, 2.0, 0.0)
                gx = fluxes(p, d, m, pn, dn, mn, inside * kx * kn / (kx + kn))
                net = [gx[f] - fx[f] for f in range(3)]
                uat = pl.ds(base + k * NY + 1, TILE)
                ky, ku = KY[at, :], KY[uat, :]
                gy = fluxes(p, d, m, P_[uat, :], D_[uat, :], mobility(W_[uat, :], O_[uat, :]), harmonic(ky, ku))
                for f in range(3):
                    g = jnp.where(last_sub, 0.0, gy[f]) if t == 3 else gy[f]
                    fys[k, f, pl.ds(TILE + TILE * t, TILE), :] = g
                    net[f] = net[f] + (g - fys[k, f, pl.ds(TILE + TILE * t - 1, TILE), :])
                kz = KZ[at, :]
                up = lambda v: pltpu.roll(v, NZ - 1, 1)
                tz = jnp.where(last_lane, 0.0, harmonic(kz, up(kz)))
                gz = fluxes(p, d, m, up(p), up(d), [up(v) for v in m], tz)
                wt = STEP / PV[at, :]
                wgt[at, :] = wt
                sats = (w, o, 1.0 - w - o)
                for f in range(3):
                    total = net[f] + (gz[f] - pltpu.roll(gz[f], 1, 1))
                    acc[f, at, :] = sats[f] - wt * total
                p, d, w, o, kx, m, fx = pn, dn, wn, on, kn, mn, gx
            for f in range(3):
                fxs[f, pl.ds(TILE * t, TILE), :] = fx[f]
        return carry

    blocks = NX // BLOCK
    early = jnp.where(first, jnp.where(odd, RELAY_AT, blocks), jnp.where(last, blocks // 2 - 2, blocks // 2))
    lax.fori_loop(0, early, block, 0)

    relays = pltpu.make_async_remote_copy(
        src_ref=lreq, dst_ref=rreq.at[pl.ds(0, 6)], send_sem=psem.at[0], recv_sem=rsem.at[0],
        device_id=device(LINE - 1, 0), device_id_type=MESH,
    )

    @pl.when(jnp.logical_and(first, odd))
    def _():
        for k in (3, 5, 4, 1, 2, 0):
            c = k % 3
            if k in (3, 1):
                pl.semaphore_wait(open_.at[k // 3], 1)
            to_relay(c, k < 3).wait_recv()
            pltpu.make_async_remote_copy(
                src_ref=lreq.at[k], dst_ref=rreq.at[c], send_sem=psem.at[0], recv_sem=rsem.at[0],
                device_id=device(LINE - 1, 0 if k < 3 else -1), device_id_type=MESH,
            ).start()

    middle = jnp.where(first, blocks, early)
    lax.fori_loop(early, middle, block, 0)

    requests.wait_recv()
    lands = {}
    for c in range(CODES):
        ref = sreq if c == HERE else rreq
        for s in range(CAP):
            lands[c, s] = jnp.clip(ref[c, pl.ds(20 + s, 1), :].astype(jnp.int32), 0, COLS - 1)[0, 0]
    for c in range(CODES):
        for s in range(CAP):
            for q, ref in enumerate((P_, D_, W_, O_)):
                loc[c, pl.ds(4 * q + s, 1), :] = ref[pl.ds(lands[c, s], 1), :]
    for c in sorted(range(CODES), key=lambda c: -abs(offsets[c][0]) - abs(offsets[c][1])):
        ref = sreq if c == HERE else rreq
        a = [ref[c, pl.ds(4 * q, 4), :] for q in range(5)]
        b = [loc[c, pl.ds(4 * q, 4), :] for q in range(4)]
        flow = fluxes(a[0], a[1], mobility(a[2], a[3]), b[0], b[1], mobility(b[2], b[3]), a[4])
        for f in range(3):
            sresp[c, pl.ds(4 * f, 4), :] = flow[f]
            rows[f, pl.ds(SLOTS + 4 * c, 4), :] = -flow[f]
            if c == HERE:
                rows[f, pl.ds(4 * c, 4), :] = flow[f]
        sresp[c, pl.ds(12, 4), :] = jnp.zeros((4, NZ), jnp.float32)
        if c == HERE:
            continue
        dx, dy = offsets[c]
        copy = pltpu.make_async_remote_copy(
            src_ref=sresp.at[c], dst_ref=rresp.at[c],
            send_sem=ssem.at[1], recv_sem=rsem.at[1],
            device_id=device(-dx, -dy), device_id_type=MESH,
        )
        copy.start()
    answers = pltpu.make_async_remote_copy(
        src_ref=sresp.at[eight], dst_ref=rresp.at[eight], send_sem=ssem.at[1], recv_sem=rsem.at[1],
        device_id=device(0, 1), device_id_type=MESH,
    )

    @pl.when(jnp.logical_and(first, goes[1]))
    def _():
        for copy in halos_x[1]:
            copy.start()

    for c in range(CODES):
        for s in range(CAP):
            idx0, idx1 = place(idx0, idx1, SLOTS + c * CAP + s, lands[c, s])

    lax.fori_loop(middle, blocks, block, 0)

    def face(axis, side):
        far = [(hy if axis else hx)[side, q] for q in range(5)]
        if axis:
            at = pl.ds((NY - 1) if side else 0, NX, NY)
        else:
            at = pl.ds((NX - 1) * NY if side else 0, NY)
        near = [ref[at, :] for ref in (P_, D_, W_, O_, KY if axis else KX)]
        lo, hi = (near, far) if side else (far, near)
        flow = fluxes(
            lo[0], lo[1], mobility(lo[2], lo[3]), hi[0], hi[1], mobility(hi[2], hi[3]), harmonic(lo[4], hi[4])
        )
        wt = wgt[at, :]
        for f in range(3):
            step = wt * flow[f]
            acc[f, at, :] = acc[f, at, :] + (-step if side else step)

    for axis in range(2):
        for side in range(2):
            @pl.when(comes[2 * axis + side])
            def _(axis=axis, side=side):
                if axis:
                    halos_y[side].wait_recv()
                else:
                    whole_x[side].wait_recv()
                face(axis, side)

    idx = jnp.concatenate([idx0, idx1], axis=1)
    cell = lax.broadcasted_iota(jnp.int32, (32, 2 * NZ), 0)

    def mark(b, carry):
        start = pl.multiple_of(b * 32, 32)
        hot[pl.ds(start, 32), :] = jnp.where(cell + start == idx, 1.0, 0.0).astype(jnp.bfloat16)
        return carry

    lax.fori_loop(0, COLS // 32, mark, 0)

    answers.wait_recv()
    for c in range(CODES):
        if c != HERE:
            for f in range(3):
                rows[f, pl.ds(4 * c, 4), :] = rresp[c, pl.ds(4 * f, 4), :]
    requests.wait_send()
    answers.wait_send()
    for side in range(2):
        @pl.when(goes[side])
        def _(side=side):
            whole_x[side].wait_send()

        @pl.when(goes[2 + side])
        def _(side=side):
            halos_y[side].wait_send()

    @pl.when(jnp.logical_and(first, odd))
    def _():
        relays.wait_send()


def add_kernel(acc, wgt, hot, rows, out, parts, held, sem):
    for f in range(3):
        value = rows[f]
        for k in range(3):
            part = value.astype(jnp.bfloat16)
            parts[pl.ds(2 * SLOTS * k, 2 * SLOTS), pl.ds(NZ * f, NZ)] = part
            value = value - part.astype(jnp.float32)
        parts[pl.ds(240, 16), pl.ds(NZ * f, NZ)] = jnp.zeros((16, NZ), jnp.bfloat16)
    size = COLS // 8
    for n in range(8):
        at = pl.ds(n * size, size)
        delta = jnp.dot(hot[at, :], parts[...], preferred_element_type=jnp.float32)
        wt = wgt[at, :]
        for f in range(3):
            held[f, at, :] = acc[f, at, :] - wt * delta[:, NZ * f:NZ * (f + 1)]
            pltpu.make_async_copy(held.at[f, at], out.at[f, at], sem).start()
    pltpu.make_async_copy(held, out, sem).wait()


def body(pressure, depth, saturation, permeability, pore_volume, fault_pairs, fault_kind, fault_count, fault_table):
    f32, i32 = jnp.float32, jnp.int32
    hbm = pl.BlockSpec(memory_space=pltpu.HBM)
    vmem = pl.BlockSpec(memory_space=pltpu.VMEM)
    V = pltpu.VMEM
    acc, wgt, hot, rows = pl.pallas_call(
        grid_kernel,
        out_shape=(
            V((3, COLS, NZ), f32), V((COLS, NZ), f32), V((COLS, 2 * NZ), jnp.bfloat16), V((3, 2 * SLOTS, NZ), f32),
        ),
        in_specs=[hbm] * 8 + [pl.BlockSpec(memory_space=pltpu.SMEM)],
        out_specs=(vmem,) * 4,
        scratch_shapes=[
            V((4, COLS + TILE, NZ), f32), V((3, COLS + TILE, NZ), f32), V((COLS, NZ), f32), V((16, NZ), f32),
            pltpu.SMEM((3, 32), i32), pltpu.SMEM((32,), i32),
            V((CODES, 24, NZ), f32), V((CODES, 24, NZ), f32), V((6, 24, NZ), f32), V((CODES, 24, NZ), f32),
            V((CODES, 16, NZ), f32), V((CODES, 16, NZ), f32),
            V((2, 5, NX, NZ), f32), V((2, 5, NY, NZ), f32), V((2, 5, NX, NZ), f32),
            V((3, NY, NZ), f32), V((BLOCK, 3, TILE + NY, NZ), f32),
            pltpu.SemaphoreType.DMA((6,)), pltpu.SemaphoreType.DMA((2,)), pltpu.SemaphoreType.DMA((2,)),
            pltpu.SemaphoreType.DMA((6,)), pltpu.SemaphoreType.DMA((1,)),
            pltpu.SemaphoreType.DMA((4,)), pltpu.SemaphoreType.DMA((4,)), pltpu.SemaphoreType.REGULAR((2,)),
        ],
        compiler_params=pltpu.CompilerParams(collective_id=0, has_side_effects=True, vmem_limit_bytes=24 * 2**20),
        name="grid",
    )(
        *(
            pltpu.with_memory_space_constraint(x, pltpu.HBM)
            for x in (
                pressure.reshape(COLS, NZ), depth.reshape(COLS, NZ), saturation.reshape(2, COLS, NZ),
                permeability.reshape(3, COLS, NZ), pore_volume.reshape(COLS, NZ),
                fault_pairs.T, fault_kind, fault_table,
            )
        ),
        fault_count,
    )
    out = pl.pallas_call(
        add_kernel,
        out_shape=jax.ShapeDtypeStruct((3, COLS, NZ), f32),
        in_specs=[vmem] * 4,
        out_specs=hbm,
        scratch_shapes=[V((2 * NZ, 3 * NZ), jnp.bfloat16), V((3, COLS, NZ), f32), pltpu.SemaphoreType.DMA],
        compiler_params=pltpu.CompilerParams(vmem_limit_bytes=16 * 2**20),
        name="add",
    )(acc, wgt, hot, rows)
    return out.reshape(3, NX, NY, NZ)


def solution(mesh):
    in_specs = (
        P("gx", "gy", None),
        P("gx", "gy", None),
        P(None, "gx", "gy", None),
        P(None, "gx", "gy", None),
        P("gx", "gy", None),
        P(("gx", "gy"), None),
        P(("gx", "gy")),
        P(("gx", "gy")),
        P(),
    )
    out_specs = P(None, "gx", "gy", None)
    return jax.shard_map(body, mesh=mesh, in_specs=in_specs, out_specs=out_specs, check_vma=False)
```

```python
import jax
import jax.numpy as jnp
from jax import lax
from jax.experimental import pallas as pl
from jax.experimental.pallas import tpu as pltpu
from jax.sharding import PartitionSpec as P

CAP = 4
CODES = 9
HERE = 4
SLOTS = 40
RHO = (1.0, 0.8, 0.25)
STEP = 0.2
NX = 32
NY = 32
NZ = 128
COLS = NX * NY
TILE = 8
LINE = 4
BLOCK = 2
RELAY_AT = 6
MESH = pl.DeviceIdType.MESH


def mobility(sw, so):
    sg = 1.0 - sw - so
    return (sw * sw * 2.0, so * so, sg * sg * 4.0)


def harmonic(a, b):
    return 2.0 * a * b / (a + b)


def fluxes(pa, da, ma, pb, db, mb, trans):
    dp = pa - pb
    dd = da - db
    out = []
    for f in range(3):
        drive = dp - (dd if RHO[f] == 1.0 else RHO[f] * dd)
        out.append(trans * jnp.where(drive > 0.0, ma[f], mb[f]) * drive)
    return out


def grid_kernel(
    press, depth, sat, perm, pore, pairs, kind, table, CT,
    acc, wgt, hot, rows,
    X, K, PV, TAB, PR, KD,
    sreq, rreq, lreq, loc, sresp, rresp,
    ysend, hx, hy, fxs, fys,
    lsem, ssem, rsem, qsem, psem, hsend, hrecv, open_,
):
    P_, D_, W_, O_ = (X.at[q] for q in range(4))
    KX, KY, KZ = (K.at[q] for q in range(3))
    cols = pl.ds(0, COLS)
    ix = lax.axis_index("gx")
    iy = lax.axis_index("gy")
    nx = lax.axis_size("gx")
    ny = lax.axis_size("gy")

    def device(dx, dy):
        return (lax.rem(ix + (dx + nx), nx), lax.rem(iy + (dy + ny), ny))

    offsets = [(dx, dy) for dx in (-1, 0, 1) for dy in (-1, 0, 1)]
    barrier = pltpu.get_barrier_semaphore()
    iz = lax.rem(ix, LINE)
    first = iz == 0
    second = iz == 1
    last = iz == LINE - 1

    odd = lax.rem(iy, 2) == 1

    def greet(dx, dy):
        pl.semaphore_signal(barrier, inc=1, device_id=device(dx, dy), device_id_type=MESH)

    for dy in (-1, 1):
        greet(0, dy)

    @pl.when(jnp.logical_not(second))
    def _():
        for dy in (-1, 0, 1):
            greet(-1, dy)

    @pl.when(jnp.logical_not(last))
    def _():
        for dy in (-1, 0, 1):
            greet(1, dy)

    @pl.when(jnp.logical_and(first, odd))
    def _():
        for dy in (-2, -1, 0):
            greet(LINE, dy)

    @pl.when(jnp.logical_and(jnp.logical_and(first, odd), iy < ny - 1))
    def _():
        greet(LINE, 1)

    @pl.when(jnp.logical_and(first, odd))
    def _():
        for dy in (-1, 0):
            greet(LINE - 1, dy)

    loads = [
        pltpu.make_async_copy(src, dst, lsem.at[n])
        for n, src, dst in (
            (0, pairs, PR), (1, kind, KD),
            (2, press, X.at[0, cols]), (2, depth, X.at[1, cols]), (2, sat, X.at[pl.ds(2, 2), cols]),
            (3, table, TAB), (4, perm, K.at[:, cols]), (5, pore, PV),
        )
    ]
    for copy in loads:
        copy.start()
    state = pltpu.make_async_copy(X.at[:, cols], X.at[:, cols], lsem.at[2])

    zero = jnp.zeros((TILE, NZ), jnp.float32)
    for q in range(4):
        X[q, pl.ds(COLS, TILE), :] = zero
    K[1, pl.ds(COLS, TILE), :] = zero
    for f in range(3):
        for t in range(4):
            fxs[f, pl.ds(TILE * t, TILE), :] = zero
        for k in range(BLOCK):
            fys[k, f, pl.ds(0, TILE), :] = zero
        rows[f, pl.ds(32, TILE), :] = zero
        rows[f, pl.ds(SLOTS + 32, TILE), :] = zero

    @pl.when(last)
    def _():
        pl.semaphore_wait(barrier, 9)

    for own_odd in (False, True):
        @pl.when(jnp.logical_and(last, odd if own_odd else jnp.logical_not(odd)))
        def _(own_odd=own_odd):
            pl.semaphore_signal(
                open_.at[0 if own_odd else 1], inc=1, device_id=device(1 - LINE, 0 if own_odd else 1),
                device_id_type=MESH,
            )

    for n in range(2):
        loads[n].wait()
    live = CT[0]
    log_y = ny.bit_length() - 1
    used = jnp.int32(0)
    words = [jnp.int32(0)] * CODES
    for r in range(32):
        target = PR[1, r]
        cx = ((target >> log_y) - ix + 1) & (nx - 1)
        cy = ((target & (ny - 1)) - iy + 1) & (ny - 1)
        code = cx * 3 + cy
        rank = (used >> (code * 3)) & 7
        on = jnp.where(r < live, 1, 0)
        used = used + (on << (code * 3))
        entry = ((r + 32) * on) << (rank * 6)
        for c in range(CODES):
            words[c] = words[c] + jnp.where(code == c, entry, 0)

    state.wait()
    loads[5].wait()
    lane = lax.broadcasted_iota(jnp.int32, (1, NZ), 1)
    idx0 = jnp.full((1, NZ), -1, jnp.int32)
    idx1 = jnp.full((1, NZ), -1, jnp.int32)

    def place(idx0, idx1, k, value):
        for copy in range(3):
            at = 2 * SLOTS * copy + k
            if at < NZ:
                idx0 = jnp.where(lane == at, value, idx0)
            else:
                idx1 = jnp.where(lane == at - NZ, value, idx1)
        return idx0, idx1

    for c in range(CODES):
        for s in range(CAP):
            entry = words[c] >> (6 * s)
            r = entry & 31
            full = jnp.where((entry & 32) > 0, 1.0, 0.0)
            src = PR[0, r]
            land = PR[2, r]
            kd = KD[r]
            for q, ref in enumerate((P_, D_, W_, O_)):
                sreq[c, pl.ds(4 * q + s, 1), :] = ref[pl.ds(src, 1), :]
            sreq[c, pl.ds(16 + s, 1), :] = TAB[pl.ds(kd, 1), :] * full
            sreq[c, pl.ds(20 + s, 1), :] = jnp.full((1, NZ), land, jnp.int32).astype(jnp.float32)
            idx0, idx1 = place(idx0, idx1, c * CAP + s, src)

    @pl.when(jnp.logical_not(last))
    def _():
        pl.semaphore_wait(barrier, jnp.where(first, jnp.where(iy == 0, 3, 4), 8))


    def request(c, target):
        return pltpu.make_async_remote_copy(
            src_ref=sreq.at[c], dst_ref=rreq.at[c], send_sem=ssem.at[0], recv_sem=rsem.at[0],
            device_id=target, device_id_type=MESH,
        )

    def to_relay(c, to_odd):
        dx, dy = offsets[c]
        k = c if to_odd else 3 + c
        return pltpu.make_async_remote_copy(
            src_ref=sreq.at[c], dst_ref=lreq.at[k], send_sem=ssem.at[0], recv_sem=qsem.at[k],
            device_id=device(-LINE, dy if to_odd else dy + 1), device_id_type=MESH,
        )

    to_side = pltpu.make_async_remote_copy(
        src_ref=sreq.at[0], dst_ref=lreq.at[6], send_sem=ssem.at[0], recv_sem=qsem.at[6],
        device_id=device(0, -1), device_id_type=MESH,
    )
    from_side = pltpu.make_async_remote_copy(
        src_ref=lreq.at[6], dst_ref=lreq.at[0], send_sem=psem.at[1], recv_sem=qsem.at[0],
        device_id=device(-LINE, 0), device_id_type=MESH,
    )

    for own_odd in (False, True):
        @pl.when(jnp.logical_and(first, odd if own_odd else jnp.logical_not(odd)))
        def _(own_odd=own_odd):
            for c in (0, 2, 1):
                if c == 0 and not own_odd:
                    @pl.when(iy > 0)
                    def _():
                        to_relay(0, True).start()

                    @pl.when(iy == 0)
                    def _():
                        to_side.start()
                else:
                    to_relay(c, own_odd == (c == 1)).start()

    @pl.when(jnp.logical_not(first))
    def _():
        for c in (0, 2, 1):
            request(c, device(*offsets[c])).start()

    for c in (3, 5):
        request(c, device(*offsets[c])).start()

    @pl.when(jnp.logical_not(first))
    def _():
        for c in (6, 8, 7):
            request(c, device(*offsets[c])).start()

    @pl.when(second)
    def _():
        for dy in (-1, 0, 1):
            pl.semaphore_signal(open_.at[3 - dy], inc=1, device_id=device(-1, dy), device_id_type=MESH)

    eight = pl.ds(0, 8)
    requests = pltpu.make_async_remote_copy(
        src_ref=sreq.at[eight], dst_ref=rreq.at[eight], send_sem=ssem.at[0], recv_sem=rsem.at[0],
        device_id=device(0, 1), device_id_type=MESH,
    )

    for side, y in ((0, NY - 1), (1, 0)):
        for q, ref in enumerate((P_, D_, W_, O_)):
            ysend[side, q] = ref[pl.ds(y, NX, NY), :]
    for n in range(6, 8):
        loads[n].wait()
    for side, y in ((0, NY - 1), (1, 0)):
        ysend[side, 4] = KY[pl.ds(y, NX, NY), :]

    def halo(src, dst, n, dx, dy):
        return pltpu.make_async_remote_copy(
            src_ref=src, dst_ref=dst, send_sem=hsend.at[n], recv_sem=hrecv.at[n],
            device_id=device(dx, dy), device_id_type=MESH,
        )

    halos_x = []
    for side, (dx, x) in enumerate(((1, NX - 1), (-1, 0))):
        row = pl.ds(x * NY, NY)
        halos_x.append([
            halo(X.at[:, row], hx.at[side, pl.ds(0, 4)], side, dx, 0),
            halo(K.at[0, row], hx.at[side, 4], side, dx, 0),
        ])
    whole_x = [halo(hx.at[side], hx.at[side], side, dx, 0) for side, dx in enumerate((1, -1))]
    halos_y = [halo(ysend.at[side], hy.at[side], 2 + side, 0, dy) for side, dy in enumerate((1, -1))]
    goes = (ix < nx - 1, ix > 0, iy < ny - 1, iy > 0)
    comes = (goes[1], goes[0], goes[3], goes[2])

    @pl.when(jnp.logical_and(goes[0], jnp.logical_not(first)))
    def _():
        for copy in halos_x[0]:
            copy.start()

    @pl.when(jnp.logical_not(first))
    def _():
        for copy in halos_x[1]:
            copy.start()

    for side in range(2):
        @pl.when(goes[2 + side])
        def _(side=side):
            halos_y[side].start()

    lanes = lax.broadcasted_iota(jnp.int32, (TILE, NZ), 1)
    sublanes = lax.broadcasted_iota(jnp.int32, (TILE, NZ), 0)
    last_lane = lanes == NZ - 1
    last_sub = sublanes == TILE - 1

    def block(b, carry):
        for t in range(4):
            base = b * (BLOCK * NY) + TILE * t
            at = pl.ds(pl.multiple_of(base, TILE), TILE)
            p, d, w, o, kx = P_[at, :], D_[at, :], W_[at, :], O_[at, :], KX[at, :]
            m = mobility(w, o)
            fx = [fxs[f, pl.ds(TILE * t, TILE), :] for f in range(3)]
            for k in range(BLOCK):
                row = b * BLOCK + k
                at = pl.ds(pl.multiple_of(base + k * NY, TILE), TILE)
                nrow = jnp.minimum(row + 1, NX - 1)
                nat = pl.ds(pl.multiple_of(nrow * NY + TILE * t, TILE), TILE)
                pn, dn, wn, on, kn = P_[nat, :], D_[nat, :], W_[nat, :], O_[nat, :], KX[nat, :]
                mn = mobility(wn, on)
                inside = jnp.where(row < NX - 1, 2.0, 0.0)
                gx = fluxes(p, d, m, pn, dn, mn, inside * kx * kn / (kx + kn))
                net = [gx[f] - fx[f] for f in range(3)]
                uat = pl.ds(base + k * NY + 1, TILE)
                ky, ku = KY[at, :], KY[uat, :]
                gy = fluxes(p, d, m, P_[uat, :], D_[uat, :], mobility(W_[uat, :], O_[uat, :]), harmonic(ky, ku))
                for f in range(3):
                    g = jnp.where(last_sub, 0.0, gy[f]) if t == 3 else gy[f]
                    fys[k, f, pl.ds(TILE + TILE * t, TILE), :] = g
                    net[f] = net[f] + (g - fys[k, f, pl.ds(TILE + TILE * t - 1, TILE), :])
                kz = KZ[at, :]
                up = lambda v: pltpu.roll(v, NZ - 1, 1)
                tz = jnp.where(last_lane, 0.0, harmonic(kz, up(kz)))
                gz = fluxes(p, d, m, up(p), up(d), [up(v) for v in m], tz)
                wt = STEP / PV[at, :]
                wgt[at, :] = wt
                sats = (w, o, 1.0 - w - o)
                for f in range(3):
                    total = net[f] + (gz[f] - pltpu.roll(gz[f], 1, 1))
                    acc[f, at, :] = sats[f] - wt * total
                p, d, w, o, kx, m, fx = pn, dn, wn, on, kn, mn, gx
            for f in range(3):
                fxs[f, pl.ds(TILE * t, TILE), :] = fx[f]
        return carry

    blocks = NX // BLOCK
    early = jnp.where(first, jnp.where(odd, RELAY_AT, blocks), jnp.where(last, blocks // 2 - 2, blocks // 2))
    lax.fori_loop(0, early, block, 0)

    relays = pltpu.make_async_remote_copy(
        src_ref=lreq.at[pl.ds(0, 6)], dst_ref=rreq.at[pl.ds(0, 6)], send_sem=psem.at[0], recv_sem=rsem.at[0],
        device_id=device(LINE - 1, 0), device_id_type=MESH,
    )

    beside = jnp.logical_and(first, iy == ny - 1)

    @pl.when(beside)
    def _():
        to_side.wait_recv()
        from_side.start()

    @pl.when(jnp.logical_and(first, odd))
    def _():
        for k in (3, 5, 4, 1, 2, 0):
            c = k % 3
            if k in (3, 1):
                pl.semaphore_wait(open_.at[k // 3], 1)
            to_relay(c, k < 3).wait_recv()
            pltpu.make_async_remote_copy(
                src_ref=lreq.at[k], dst_ref=rreq.at[c], send_sem=psem.at[0], recv_sem=rsem.at[0],
                device_id=device(LINE - 1, 0 if k < 3 else -1), device_id_type=MESH,
            ).start()

    @pl.when(first)
    def _():
        for c in (6, 8, 7):
            pl.semaphore_wait(open_.at[c - 4], 1)
            request(c, device(*offsets[c])).start()
        for copy in halos_x[0]:
            copy.start()

    middle = jnp.where(first, blocks, early)
    lax.fori_loop(early, middle, block, 0)

    requests.wait_recv()
    lands = {}
    for c in range(CODES):
        ref = sreq if c == HERE else rreq
        for s in range(CAP):
            lands[c, s] = jnp.clip(ref[c, pl.ds(20 + s, 1), :].astype(jnp.int32), 0, COLS - 1)[0, 0]
    for c in range(CODES):
        for s in range(CAP):
            for q, ref in enumerate((P_, D_, W_, O_)):
                loc[c, pl.ds(4 * q + s, 1), :] = ref[pl.ds(lands[c, s], 1), :]
    for c in sorted(range(CODES), key=lambda c: -abs(offsets[c][0]) - abs(offsets[c][1])):
        ref = sreq if c == HERE else rreq
        a = [ref[c, pl.ds(4 * q, 4), :] for q in range(5)]
        b = [loc[c, pl.ds(4 * q, 4), :] for q in range(4)]
        flow = fluxes(a[0], a[1], mobility(a[2], a[3]), b[0], b[1], mobility(b[2], b[3]), a[4])
        for f in range(3):
            sresp[c, pl.ds(4 * f, 4), :] = flow[f]
            rows[f, pl.ds(SLOTS + 4 * c, 4), :] = -flow[f]
            if c == HERE:
                rows[f, pl.ds(4 * c, 4), :] = flow[f]
        sresp[c, pl.ds(12, 4), :] = jnp.zeros((4, NZ), jnp.float32)
        if c == HERE:
            continue
        dx, dy = offsets[c]
        copy = pltpu.make_async_remote_copy(
            src_ref=sresp.at[c], dst_ref=rresp.at[c],
            send_sem=ssem.at[1], recv_sem=rsem.at[1],
            device_id=device(-dx, -dy), device_id_type=MESH,
        )
        copy.start()
    answers = pltpu.make_async_remote_copy(
        src_ref=sresp.at[eight], dst_ref=rresp.at[eight], send_sem=ssem.at[1], recv_sem=rsem.at[1],
        device_id=device(0, 1), device_id_type=MESH,
    )

    @pl.when(jnp.logical_and(first, goes[1]))
    def _():
        for copy in halos_x[1]:
            copy.start()

    for c in range(CODES):
        for s in range(CAP):
            idx0, idx1 = place(idx0, idx1, SLOTS + c * CAP + s, lands[c, s])

    lax.fori_loop(middle, blocks, block, 0)

    def face(axis, side):
        far = [(hy if axis else hx)[side, q] for q in range(5)]
        if axis:
            at = pl.ds((NY - 1) if side else 0, NX, NY)
        else:
            at = pl.ds((NX - 1) * NY if side else 0, NY)
        near = [ref[at, :] for ref in (P_, D_, W_, O_, KY if axis else KX)]
        lo, hi = (near, far) if side else (far, near)
        flow = fluxes(
            lo[0], lo[1], mobility(lo[2], lo[3]), hi[0], hi[1], mobility(hi[2], hi[3]), harmonic(lo[4], hi[4])
        )
        wt = wgt[at, :]
        for f in range(3):
            step = wt * flow[f]
            acc[f, at, :] = acc[f, at, :] + (-step if side else step)

    for axis in range(2):
        for side in range(2):
            @pl.when(comes[2 * axis + side])
            def _(axis=axis, side=side):
                if axis:
                    halos_y[side].wait_recv()
                else:
                    whole_x[side].wait_recv()
                face(axis, side)

    idx = jnp.concatenate([idx0, idx1], axis=1)
    cell = lax.broadcasted_iota(jnp.int32, (32, 2 * NZ), 0)

    def mark(b, carry):
        start = pl.multiple_of(b * 32, 32)
        hot[pl.ds(start, 32), :] = jnp.where(cell + start == idx, 1.0, 0.0).astype(jnp.bfloat16)
        return carry

    lax.fori_loop(0, COLS // 32, mark, 0)

    answers.wait_recv()
    for c in range(CODES):
        if c != HERE:
            for f in range(3):
                rows[f, pl.ds(4 * c, 4), :] = rresp[c, pl.ds(4 * f, 4), :]
    requests.wait_send()
    answers.wait_send()
    for side in range(2):
        @pl.when(goes[side])
        def _(side=side):
            whole_x[side].wait_send()

        @pl.when(goes[2 + side])
        def _(side=side):
            halos_y[side].wait_send()

    @pl.when(jnp.logical_and(first, odd))
    def _():
        relays.wait_send()

    @pl.when(beside)
    def _():
        from_side.wait_send()


def add_kernel(acc, wgt, hot, rows, out, parts, held, sem):
    for f in range(3):
        value = rows[f]
        for k in range(3):
            part = value.astype(jnp.bfloat16)
            parts[pl.ds(2 * SLOTS * k, 2 * SLOTS), pl.ds(NZ * f, NZ)] = part
            value = value - part.astype(jnp.float32)
        parts[pl.ds(240, 16), pl.ds(NZ * f, NZ)] = jnp.zeros((16, NZ), jnp.bfloat16)
    size = COLS // 8
    for n in range(8):
        at = pl.ds(n * size, size)
        delta = jnp.dot(hot[at, :], parts[...], preferred_element_type=jnp.float32)
        wt = wgt[at, :]
        for f in range(3):
            held[f, at, :] = acc[f, at, :] - wt * delta[:, NZ * f:NZ * (f + 1)]
            pltpu.make_async_copy(held.at[f, at], out.at[f, at], sem).start()
    pltpu.make_async_copy(held, out, sem).wait()


def body(pressure, depth, saturation, permeability, pore_volume, fault_pairs, fault_kind, fault_count, fault_table):
    f32, i32 = jnp.float32, jnp.int32
    hbm = pl.BlockSpec(memory_space=pltpu.HBM)
    vmem = pl.BlockSpec(memory_space=pltpu.VMEM)
    V = pltpu.VMEM
    acc, wgt, hot, rows = pl.pallas_call(
        grid_kernel,
        out_shape=(
            V((3, COLS, NZ), f32), V((COLS, NZ), f32), V((COLS, 2 * NZ), jnp.bfloat16), V((3, 2 * SLOTS, NZ), f32),
        ),
        in_specs=[hbm] * 8 + [pl.BlockSpec(memory_space=pltpu.SMEM)],
        out_specs=(vmem,) * 4,
        scratch_shapes=[
            V((4, COLS + TILE, NZ), f32), V((3, COLS + TILE, NZ), f32), V((COLS, NZ), f32), V((16, NZ), f32),
            pltpu.SMEM((3, 32), i32), pltpu.SMEM((32,), i32),
            V((CODES, 24, NZ), f32), V((CODES, 24, NZ), f32), V((7, 24, NZ), f32), V((CODES, 24, NZ), f32),
            V((CODES, 16, NZ), f32), V((CODES, 16, NZ), f32),
            V((2, 5, NX, NZ), f32), V((2, 5, NY, NZ), f32), V((2, 5, NX, NZ), f32),
            V((3, NY, NZ), f32), V((BLOCK, 3, TILE + NY, NZ), f32),
            pltpu.SemaphoreType.DMA((6,)), pltpu.SemaphoreType.DMA((2,)), pltpu.SemaphoreType.DMA((2,)),
            pltpu.SemaphoreType.DMA((7,)), pltpu.SemaphoreType.DMA((2,)),
            pltpu.SemaphoreType.DMA((4,)), pltpu.SemaphoreType.DMA((4,)), pltpu.SemaphoreType.REGULAR((5,)),
        ],
        compiler_params=pltpu.CompilerParams(collective_id=0, has_side_effects=True, vmem_limit_bytes=24 * 2**20),
        name="grid",
    )(
        *(
            pltpu.with_memory_space_constraint(x, pltpu.HBM)
            for x in (
                pressure.reshape(COLS, NZ), depth.reshape(COLS, NZ), saturation.reshape(2, COLS, NZ),
                permeability.reshape(3, COLS, NZ), pore_volume.reshape(COLS, NZ),
                fault_pairs.T, fault_kind, fault_table,
            )
        ),
        fault_count,
    )
    out = pl.pallas_call(
        add_kernel,
        out_shape=jax.ShapeDtypeStruct((3, COLS, NZ), f32),
        in_specs=[vmem] * 4,
        out_specs=hbm,
        scratch_shapes=[V((2 * NZ, 3 * NZ), jnp.bfloat16), V((3, COLS, NZ), f32), pltpu.SemaphoreType.DMA],
        compiler_params=pltpu.CompilerParams(vmem_limit_bytes=16 * 2**20),
        name="add",
    )(acc, wgt, hot, rows)
    return out.reshape(3, NX, NY, NZ)


def solution(mesh):
    in_specs = (
        P("gx", "gy", None),
        P("gx", "gy", None),
        P(None, "gx", "gy", None),
        P(None, "gx", "gy", None),
        P("gx", "gy", None),
        P(("gx", "gy"), None),
        P(("gx", "gy")),
        P(("gx", "gy")),
        P(),
    )
    out_specs = P(None, "gx", "gy", None)
    return jax.shard_map(body, mesh=mesh, in_specs=in_specs, out_specs=out_specs, check_vma=False)
```

```python
import jax
import jax.numpy as jnp
from jax import lax
from jax.experimental import pallas as pl
from jax.experimental.pallas import tpu as pltpu
from jax.sharding import PartitionSpec as P

CAP = 4
CODES = 9
HERE = 4
SLOTS = 40
RHO = (1.0, 0.8, 0.25)
STEP = 0.2
NX = 32
NY = 32
NZ = 128
COLS = NX * NY
TILE = 8
LINE = 4
BLOCK = 2
RELAY_AT = 6
MESH = pl.DeviceIdType.MESH


def mobility(sw, so):
    sg = 1.0 - sw - so
    return (sw * sw * 2.0, so * so, sg * sg * 4.0)


def harmonic(a, b):
    return 2.0 * a * b / (a + b)


def fluxes(pa, da, ma, pb, db, mb, trans):
    dp = pa - pb
    dd = da - db
    out = []
    for f in range(3):
        drive = dp - (dd if RHO[f] == 1.0 else RHO[f] * dd)
        out.append(trans * jnp.where(drive > 0.0, ma[f], mb[f]) * drive)
    return out


def grid_kernel(
    press, depth, sat, perm, pore, pairs, kind, table, CT,
    acc, wgt, hot, rows,
    X, K, PV, TAB, PR, KD,
    sreq, rreq, lreq, loc, sresp, rresp,
    ysend, hx, hy, fxs, fys,
    lsem, ssem, rsem, qsem, psem, hsend, hrecv, open_,
):
    P_, D_, W_, O_ = (X.at[q] for q in range(4))
    KX, KY, KZ = (K.at[q] for q in range(3))
    cols = pl.ds(0, COLS)
    ix = lax.axis_index("gx")
    iy = lax.axis_index("gy")
    nx = lax.axis_size("gx")
    ny = lax.axis_size("gy")

    def device(dx, dy):
        return (lax.rem(ix + (dx + nx), nx), lax.rem(iy + (dy + ny), ny))

    offsets = [(dx, dy) for dx in (-1, 0, 1) for dy in (-1, 0, 1)]
    barrier = pltpu.get_barrier_semaphore()
    iz = lax.rem(ix, LINE)
    first = iz == 0
    second = iz == 1
    last = iz == LINE - 1

    odd = lax.rem(iy, 2) == 1

    def greet(dx, dy):
        pl.semaphore_signal(barrier, inc=1, device_id=device(dx, dy), device_id_type=MESH)

    top = iy == ny - 1
    bottom = iy == 0
    for dx in (-1, 0, 1):
        ahead = (second, first, last)[dx + 1]
        for dy in (-1, 0, 1):
            if (dx, dy) == (0, 0):
                continue
            if dx:
                meets = jnp.logical_not(ahead)
                if dy == 1:
                    meets = jnp.logical_and(meets, jnp.logical_or(first, jnp.logical_not(top)))
            elif dy == 1:
                meets = jnp.logical_or(ahead, jnp.logical_not(top))
            else:
                meets = None
            if meets is None:
                greet(dx, dy)
            else:
                @pl.when(meets)
                def _(dx=dx, dy=dy):
                    greet(dx, dy)

    @pl.when(jnp.logical_and(first, odd))
    def _():
        for dy in (-2, -1, 0):
            greet(LINE, dy)

    @pl.when(jnp.logical_and(jnp.logical_and(first, odd), iy < ny - 1))
    def _():
        greet(LINE, 1)

    @pl.when(jnp.logical_and(first, odd))
    def _():
        for dy in (-1, 0):
            greet(LINE - 1, dy)

    loads = [
        pltpu.make_async_copy(src, dst, lsem.at[n])
        for n, src, dst in (
            (0, pairs, PR), (1, kind, KD),
            (2, press, X.at[0, cols]), (2, depth, X.at[1, cols]), (2, sat, X.at[pl.ds(2, 2), cols]),
            (3, table, TAB), (4, perm, K.at[:, cols]), (5, pore, PV),
        )
    ]
    for copy in loads:
        copy.start()
    state = pltpu.make_async_copy(X.at[:, cols], X.at[:, cols], lsem.at[2])

    zero = jnp.zeros((TILE, NZ), jnp.float32)
    for q in range(4):
        X[q, pl.ds(COLS, TILE), :] = zero
    K[1, pl.ds(COLS, TILE), :] = zero
    for f in range(3):
        for t in range(4):
            fxs[f, pl.ds(TILE * t, TILE), :] = zero
        for k in range(BLOCK):
            fys[k, f, pl.ds(0, TILE), :] = zero
        rows[f, pl.ds(32, TILE), :] = zero
        rows[f, pl.ds(SLOTS + 32, TILE), :] = zero

    @pl.when(last)
    def _():
        pl.semaphore_wait(barrier, jnp.where(bottom, 7, 9))

    for own_odd in (False, True):
        @pl.when(jnp.logical_and(last, odd if own_odd else jnp.logical_not(odd)))
        def _(own_odd=own_odd):
            pl.semaphore_signal(
                open_.at[0 if own_odd else 1], inc=1, device_id=device(1 - LINE, 0 if own_odd else 1),
                device_id_type=MESH,
            )

    for n in range(2):
        loads[n].wait()
    live = CT[0]
    log_y = ny.bit_length() - 1
    used = jnp.int32(0)
    words = [jnp.int32(0)] * CODES
    for r in range(32):
        target = PR[1, r]
        cx = ((target >> log_y) - ix + 1) & (nx - 1)
        cy = ((target & (ny - 1)) - iy + 1) & (ny - 1)
        code = cx * 3 + cy
        rank = (used >> (code * 3)) & 7
        on = jnp.where(r < live, 1, 0)
        used = used + (on << (code * 3))
        entry = ((r + 32) * on) << (rank * 6)
        for c in range(CODES):
            words[c] = words[c] + jnp.where(code == c, entry, 0)

    state.wait()
    loads[5].wait()
    lane = lax.broadcasted_iota(jnp.int32, (1, NZ), 1)
    idx0 = jnp.full((1, NZ), -1, jnp.int32)
    idx1 = jnp.full((1, NZ), -1, jnp.int32)

    def place(idx0, idx1, k, value):
        for copy in range(3):
            at = 2 * SLOTS * copy + k
            if at < NZ:
                idx0 = jnp.where(lane == at, value, idx0)
            else:
                idx1 = jnp.where(lane == at - NZ, value, idx1)
        return idx0, idx1

    for c in range(CODES):
        for s in range(CAP):
            entry = words[c] >> (6 * s)
            r = entry & 31
            full = jnp.where((entry & 32) > 0, 1.0, 0.0)
            src = PR[0, r]
            land = PR[2, r]
            kd = KD[r]
            for q, ref in enumerate((P_, D_, W_, O_)):
                sreq[c, pl.ds(4 * q + s, 1), :] = ref[pl.ds(src, 1), :]
            sreq[c, pl.ds(16 + s, 1), :] = TAB[pl.ds(kd, 1), :] * full
            sreq[c, pl.ds(20 + s, 1), :] = jnp.full((1, NZ), land, jnp.int32).astype(jnp.float32)
            idx0, idx1 = place(idx0, idx1, c * CAP + s, src)

    @pl.when(jnp.logical_not(last))
    def _():
        pl.semaphore_wait(barrier, jnp.where(first, jnp.where(bottom, 3, 4), jnp.where(bottom, jnp.where(second, 6, 5), 8)))

    def request(c, target):
        return pltpu.make_async_remote_copy(
            src_ref=sreq.at[c], dst_ref=rreq.at[c], send_sem=ssem.at[0], recv_sem=rsem.at[0 if c < 3 else 2],
            device_id=target, device_id_type=MESH,
        )

    def to_relay(c, to_odd):
        dx, dy = offsets[c]
        k = c if to_odd else 3 + c
        return pltpu.make_async_remote_copy(
            src_ref=sreq.at[c], dst_ref=lreq.at[k], send_sem=ssem.at[0], recv_sem=qsem.at[k],
            device_id=device(-LINE, dy if to_odd else dy + 1), device_id_type=MESH,
        )

    to_side = pltpu.make_async_remote_copy(
        src_ref=sreq.at[0], dst_ref=lreq.at[6], send_sem=ssem.at[0], recv_sem=qsem.at[6],
        device_id=device(0, -1), device_id_type=MESH,
    )
    from_side = pltpu.make_async_remote_copy(
        src_ref=lreq.at[6], dst_ref=lreq.at[0], send_sem=psem.at[1], recv_sem=qsem.at[0],
        device_id=device(-LINE, 0), device_id_type=MESH,
    )

    for own_odd in (False, True):
        @pl.when(jnp.logical_and(first, odd if own_odd else jnp.logical_not(odd)))
        def _(own_odd=own_odd):
            for c in (0, 2, 1):
                if c == 0 and not own_odd:
                    @pl.when(iy > 0)
                    def _():
                        to_relay(0, True).start()

                    @pl.when(iy == 0)
                    def _():
                        to_side.start()
                else:
                    to_relay(c, own_odd == (c == 1)).start()

    @pl.when(first)
    def _():
        for c in (3, 5):
            request(c, device(*offsets[c])).start()

    @pl.when(jnp.logical_and(jnp.logical_not(first), jnp.logical_not(bottom)))
    def _():
        for c in (6, 8, 0, 2, 3, 5, 7, 1):
            request(c, device(*offsets[c])).start()

    wraps = jnp.logical_and(jnp.logical_not(first), bottom)

    @pl.when(wraps)
    def _():
        for c in (8, 2, 5, 7, 1):
            request(c, device(*offsets[c])).start()

    for c, known in ((0, second), (6, last)):
        @pl.when(jnp.logical_and(bottom, known))
        def _(c=c):
            request(c, device(*offsets[c])).start()

    @pl.when(second)
    def _():
        for dy in (-1, 0, 1):
            pl.semaphore_signal(open_.at[3 - dy], inc=1, device_id=device(-1, dy), device_id_type=MESH)

    for dx in (-1, 0, 1):
        @pl.when(jnp.logical_and(jnp.logical_and(top, jnp.logical_not(first)), jnp.logical_not((second, first, last)[dx + 1])))
        def _(dx=dx):
            pl.semaphore_signal(open_.at[6 - dx], inc=1, device_id=device(dx, 1), device_id_type=MESH)

    eight = pl.ds(0, 8)
    requests = pltpu.make_async_remote_copy(
        src_ref=sreq.at[eight], dst_ref=rreq.at[eight], send_sem=ssem.at[0], recv_sem=rsem.at[0],
        device_id=device(0, 1), device_id_type=MESH,
    )

    for side, y in ((0, NY - 1), (1, 0)):
        for q, ref in enumerate((P_, D_, W_, O_)):
            ysend[side, q] = ref[pl.ds(y, NX, NY), :]
    for n in range(6, 8):
        loads[n].wait()
    for side, y in ((0, NY - 1), (1, 0)):
        ysend[side, 4] = KY[pl.ds(y, NX, NY), :]

    def halo(src, dst, n, dx, dy):
        return pltpu.make_async_remote_copy(
            src_ref=src, dst_ref=dst, send_sem=hsend.at[n], recv_sem=hrecv.at[n],
            device_id=device(dx, dy), device_id_type=MESH,
        )

    halos_x = []
    for side, (dx, x) in enumerate(((1, NX - 1), (-1, 0))):
        row = pl.ds(x * NY, NY)
        halos_x.append([
            halo(X.at[:, row], hx.at[side, pl.ds(0, 4)], side, dx, 0),
            halo(K.at[0, row], hx.at[side, 4], side, dx, 0),
        ])
    whole_x = [halo(hx.at[side], hx.at[side], side, dx, 0) for side, dx in enumerate((1, -1))]
    halos_y = [halo(ysend.at[side], hy.at[side], 2 + side, 0, dy) for side, dy in enumerate((1, -1))]
    goes = (ix < nx - 1, ix > 0, iy < ny - 1, iy > 0)
    comes = (goes[1], goes[0], goes[3], goes[2])

    @pl.when(jnp.logical_and(goes[0], jnp.logical_not(first)))
    def _():
        for copy in halos_x[0]:
            copy.start()

    @pl.when(jnp.logical_not(first))
    def _():
        for copy in halos_x[1]:
            copy.start()

    for side in range(2):
        @pl.when(goes[2 + side])
        def _(side=side):
            halos_y[side].start()

    lanes = lax.broadcasted_iota(jnp.int32, (TILE, NZ), 1)
    sublanes = lax.broadcasted_iota(jnp.int32, (TILE, NZ), 0)
    last_lane = lanes == NZ - 1
    last_sub = sublanes == TILE - 1

    def block(b, carry):
        for t in range(4):
            base = b * (BLOCK * NY) + TILE * t
            at = pl.ds(pl.multiple_of(base, TILE), TILE)
            p, d, w, o, kx = P_[at, :], D_[at, :], W_[at, :], O_[at, :], KX[at, :]
            m = mobility(w, o)
            fx = [fxs[f, pl.ds(TILE * t, TILE), :] for f in range(3)]
            for k in range(BLOCK):
                row = b * BLOCK + k
                at = pl.ds(pl.multiple_of(base + k * NY, TILE), TILE)
                nrow = jnp.minimum(row + 1, NX - 1)
                nat = pl.ds(pl.multiple_of(nrow * NY + TILE * t, TILE), TILE)
                pn, dn, wn, on, kn = P_[nat, :], D_[nat, :], W_[nat, :], O_[nat, :], KX[nat, :]
                mn = mobility(wn, on)
                inside = jnp.where(row < NX - 1, 2.0, 0.0)
                gx = fluxes(p, d, m, pn, dn, mn, inside * kx * kn / (kx + kn))
                net = [gx[f] - fx[f] for f in range(3)]
                uat = pl.ds(base + k * NY + 1, TILE)
                ky, ku = KY[at, :], KY[uat, :]
                gy = fluxes(p, d, m, P_[uat, :], D_[uat, :], mobility(W_[uat, :], O_[uat, :]), harmonic(ky, ku))
                for f in range(3):
                    g = jnp.where(last_sub, 0.0, gy[f]) if t == 3 else gy[f]
                    fys[k, f, pl.ds(TILE + TILE * t, TILE), :] = g
                    net[f] = net[f] + (g - fys[k, f, pl.ds(TILE + TILE * t - 1, TILE), :])
                kz = KZ[at, :]
                up = lambda v: pltpu.roll(v, NZ - 1, 1)
                tz = jnp.where(last_lane, 0.0, harmonic(kz, up(kz)))
                gz = fluxes(p, d, m, up(p), up(d), [up(v) for v in m], tz)
                wt = STEP / PV[at, :]
                wgt[at, :] = wt
                sats = (w, o, 1.0 - w - o)
                for f in range(3):
                    total = net[f] + (gz[f] - pltpu.roll(gz[f], 1, 1))
                    acc[f, at, :] = sats[f] - wt * total
                p, d, w, o, kx, m, fx = pn, dn, wn, on, kn, mn, gx
            for f in range(3):
                fxs[f, pl.ds(TILE * t, TILE), :] = fx[f]
        return carry

    blocks = NX // BLOCK
    early = jnp.where(first, jnp.where(odd, RELAY_AT, blocks), jnp.where(last, blocks // 2 - 2, blocks // 2))
    lax.fori_loop(0, early, block, 0)

    relays = pltpu.make_async_remote_copy(
        src_ref=lreq.at[pl.ds(0, 6)], dst_ref=rreq.at[pl.ds(0, 6)], send_sem=psem.at[0], recv_sem=rsem.at[0],
        device_id=device(LINE - 1, 0), device_id_type=MESH,
    )

    beside = jnp.logical_and(first, iy == ny - 1)

    @pl.when(beside)
    def _():
        to_side.wait_recv()
        from_side.start()

    @pl.when(jnp.logical_and(first, odd))
    def _():
        for k in (3, 5, 4, 1, 2, 0):
            c = k % 3
            if k in (3, 1):
                pl.semaphore_wait(open_.at[k // 3], 1)
            to_relay(c, k < 3).wait_recv()
            pltpu.make_async_remote_copy(
                src_ref=lreq.at[k], dst_ref=rreq.at[c], send_sem=psem.at[0], recv_sem=rsem.at[0],
                device_id=device(LINE - 1, 0 if k < 3 else -1), device_id_type=MESH,
            ).start()

    @pl.when(first)
    def _():
        for c in (6, 8, 7):
            pl.semaphore_wait(open_.at[c - 4], 1)
            request(c, device(*offsets[c])).start()
        for copy in halos_x[0]:
            copy.start()

    for c, known in ((6, last), (3, first), (0, second)):
        @pl.when(jnp.logical_and(wraps, jnp.logical_not(known)))
        def _(c=c):
            pl.semaphore_wait(open_.at[5 + c // 3], 1)
            request(c, device(*offsets[c])).start()

    middle = jnp.where(first, blocks, early)
    lax.fori_loop(early, middle, block, 0)

    lands = {}

    def answer(codes):
        for c in codes:
            ref = sreq if c == HERE else rreq
            for s in range(CAP):
                lands[c, s] = jnp.clip(ref[c, pl.ds(20 + s, 1), :].astype(jnp.int32), 0, COLS - 1)[0, 0]
        for c in codes:
            for s in range(CAP):
                for q, ref in enumerate((P_, D_, W_, O_)):
                    loc[c, pl.ds(4 * q + s, 1), :] = ref[pl.ds(lands[c, s], 1), :]
        for c in codes:
            ref = sreq if c == HERE else rreq
            a = [ref[c, pl.ds(4 * q, 4), :] for q in range(5)]
            b = [loc[c, pl.ds(4 * q, 4), :] for q in range(4)]
            flow = fluxes(a[0], a[1], mobility(a[2], a[3]), b[0], b[1], mobility(b[2], b[3]), a[4])
            for f in range(3):
                sresp[c, pl.ds(4 * f, 4), :] = flow[f]
                rows[f, pl.ds(SLOTS + 4 * c, 4), :] = -flow[f]
                if c == HERE:
                    rows[f, pl.ds(4 * c, 4), :] = flow[f]
            sresp[c, pl.ds(12, 4), :] = jnp.zeros((4, NZ), jnp.float32)
            if c == HERE:
                continue
            dx, dy = offsets[c]
            pltpu.make_async_remote_copy(
                src_ref=sresp.at[c], dst_ref=rresp.at[c], send_sem=ssem.at[1], recv_sem=rsem.at[1],
                device_id=device(-dx, -dy), device_id_type=MESH,
            ).start()

    for codes, n in (((0, 2, 1), 0), ((6, 8, 3, 5, 7, 4), 2)):
        part = pl.ds(0, 3) if n == 0 else pl.ds(3, 5)
        pltpu.make_async_remote_copy(
            src_ref=sreq.at[part], dst_ref=rreq.at[part], send_sem=ssem.at[0], recv_sem=rsem.at[n],
            device_id=device(0, 1), device_id_type=MESH,
        ).wait_recv()
        answer(codes)
    answers = pltpu.make_async_remote_copy(
        src_ref=sresp.at[eight], dst_ref=rresp.at[eight], send_sem=ssem.at[1], recv_sem=rsem.at[1],
        device_id=device(0, 1), device_id_type=MESH,
    )

    @pl.when(jnp.logical_and(first, goes[1]))
    def _():
        for copy in halos_x[1]:
            copy.start()

    for c in range(CODES):
        for s in range(CAP):
            idx0, idx1 = place(idx0, idx1, SLOTS + c * CAP + s, lands[c, s])

    lax.fori_loop(middle, blocks, block, 0)

    def face(axis, side):
        far = [(hy if axis else hx)[side, q] for q in range(5)]
        if axis:
            at = pl.ds((NY - 1) if side else 0, NX, NY)
        else:
            at = pl.ds((NX - 1) * NY if side else 0, NY)
        near = [ref[at, :] for ref in (P_, D_, W_, O_, KY if axis else KX)]
        lo, hi = (near, far) if side else (far, near)
        flow = fluxes(
            lo[0], lo[1], mobility(lo[2], lo[3]), hi[0], hi[1], mobility(hi[2], hi[3]), harmonic(lo[4], hi[4])
        )
        wt = wgt[at, :]
        for f in range(3):
            step = wt * flow[f]
            acc[f, at, :] = acc[f, at, :] + (-step if side else step)

    for axis in range(2):
        for side in range(2):
            @pl.when(comes[2 * axis + side])
            def _(axis=axis, side=side):
                if axis:
                    halos_y[side].wait_recv()
                else:
                    whole_x[side].wait_recv()
                face(axis, side)

    idx = jnp.concatenate([idx0, idx1], axis=1)
    cell = lax.broadcasted_iota(jnp.int32, (32, 2 * NZ), 0)

    def mark(b, carry):
        start = pl.multiple_of(b * 32, 32)
        hot[pl.ds(start, 32), :] = jnp.where(cell + start == idx, 1.0, 0.0).astype(jnp.bfloat16)
        return carry

    lax.fori_loop(0, COLS // 32, mark, 0)

    answers.wait_recv()
    for c in range(CODES):
        if c != HERE:
            for f in range(3):
                rows[f, pl.ds(4 * c, 4), :] = rresp[c, pl.ds(4 * f, 4), :]
    requests.wait_send()
    answers.wait_send()
    for side in range(2):
        @pl.when(goes[side])
        def _(side=side):
            whole_x[side].wait_send()

        @pl.when(goes[2 + side])
        def _(side=side):
            halos_y[side].wait_send()

    @pl.when(jnp.logical_and(first, odd))
    def _():
        relays.wait_send()

    @pl.when(beside)
    def _():
        from_side.wait_send()


def add_kernel(acc, wgt, hot, rows, out, parts, held, sem):
    for f in range(3):
        value = rows[f]
        for k in range(3):
            part = value.astype(jnp.bfloat16)
            parts[pl.ds(2 * SLOTS * k, 2 * SLOTS), pl.ds(NZ * f, NZ)] = part
            value = value - part.astype(jnp.float32)
        parts[pl.ds(240, 16), pl.ds(NZ * f, NZ)] = jnp.zeros((16, NZ), jnp.bfloat16)
    size = COLS // 8
    for n in range(8):
        at = pl.ds(n * size, size)
        delta = jnp.dot(hot[at, :], parts[...], preferred_element_type=jnp.float32)
        wt = wgt[at, :]
        for f in range(3):
            held[f, at, :] = acc[f, at, :] - wt * delta[:, NZ * f:NZ * (f + 1)]
            pltpu.make_async_copy(held.at[f, at], out.at[f, at], sem).start()
    pltpu.make_async_copy(held, out, sem).wait()


def body(pressure, depth, saturation, permeability, pore_volume, fault_pairs, fault_kind, fault_count, fault_table):
    f32, i32 = jnp.float32, jnp.int32
    hbm = pl.BlockSpec(memory_space=pltpu.HBM)
    vmem = pl.BlockSpec(memory_space=pltpu.VMEM)
    V = pltpu.VMEM
    acc, wgt, hot, rows = pl.pallas_call(
        grid_kernel,
        out_shape=(
            V((3, COLS, NZ), f32), V((COLS, NZ), f32), V((COLS, 2 * NZ), jnp.bfloat16), V((3, 2 * SLOTS, NZ), f32),
        ),
        in_specs=[hbm] * 8 + [pl.BlockSpec(memory_space=pltpu.SMEM)],
        out_specs=(vmem,) * 4,
        scratch_shapes=[
            V((4, COLS + TILE, NZ), f32), V((3, COLS + TILE, NZ), f32), V((COLS, NZ), f32), V((16, NZ), f32),
            pltpu.SMEM((3, 32), i32), pltpu.SMEM((32,), i32),
            V((CODES, 24, NZ), f32), V((CODES, 24, NZ), f32), V((7, 24, NZ), f32), V((CODES, 24, NZ), f32),
            V((CODES, 16, NZ), f32), V((CODES, 16, NZ), f32),
            V((2, 5, NX, NZ), f32), V((2, 5, NY, NZ), f32), V((2, 5, NX, NZ), f32),
            V((3, NY, NZ), f32), V((BLOCK, 3, TILE + NY, NZ), f32),
            pltpu.SemaphoreType.DMA((6,)), pltpu.SemaphoreType.DMA((2,)), pltpu.SemaphoreType.DMA((3,)),
            pltpu.SemaphoreType.DMA((7,)), pltpu.SemaphoreType.DMA((2,)),
            pltpu.SemaphoreType.DMA((4,)), pltpu.SemaphoreType.DMA((4,)), pltpu.SemaphoreType.REGULAR((8,)),
        ],
        compiler_params=pltpu.CompilerParams(collective_id=0, has_side_effects=True, vmem_limit_bytes=24 * 2**20),
        name="grid",
    )(
        *(
            pltpu.with_memory_space_constraint(x, pltpu.HBM)
            for x in (
                pressure.reshape(COLS, NZ), depth.reshape(COLS, NZ), saturation.reshape(2, COLS, NZ),
                permeability.reshape(3, COLS, NZ), pore_volume.reshape(COLS, NZ),
                fault_pairs.T, fault_kind, fault_table,
            )
        ),
        fault_count,
    )
    out = pl.pallas_call(
        add_kernel,
        out_shape=jax.ShapeDtypeStruct((3, COLS, NZ), f32),
        in_specs=[vmem] * 4,
        out_specs=hbm,
        scratch_shapes=[V((2 * NZ, 3 * NZ), jnp.bfloat16), V((3, COLS, NZ), f32), pltpu.SemaphoreType.DMA],
        compiler_params=pltpu.CompilerParams(vmem_limit_bytes=16 * 2**20),
        name="add",
    )(acc, wgt, hot, rows)
    return out.reshape(3, NX, NY, NZ)


def solution(mesh):
    in_specs = (
        P("gx", "gy", None),
        P("gx", "gy", None),
        P(None, "gx", "gy", None),
        P(None, "gx", "gy", None),
        P("gx", "gy", None),
        P(("gx", "gy"), None),
        P(("gx", "gy")),
        P(("gx", "gy")),
        P(),
    )
    out_specs = P(None, "gx", "gy", None)
    return jax.shard_map(body, mesh=mesh, in_specs=in_specs, out_specs=out_specs, check_vma=False)
```

```python
import jax
import jax.numpy as jnp
from jax import lax
from jax.experimental import pallas as pl
from jax.experimental.pallas import tpu as pltpu
from jax.sharding import PartitionSpec as P

CAP = 4
CODES = 9
HERE = 4
SLOTS = 40
RHO = (1.0, 0.8, 0.25)
STEP = 0.2
NX = 32
NY = 32
NZ = 128
COLS = NX * NY
TILE = 8
LINE = 4
BLOCK = 2
RELAY_AT = 6
MESH = pl.DeviceIdType.MESH


def mobility(sw, so):
    sg = 1.0 - sw - so
    return (sw * sw * 2.0, so * so, sg * sg * 4.0)


def harmonic(a, b):
    return 2.0 * a * b / (a + b)


def fluxes(pa, da, ma, pb, db, mb, trans):
    dp = pa - pb
    dd = da - db
    out = []
    for f in range(3):
        drive = dp - (dd if RHO[f] == 1.0 else RHO[f] * dd)
        out.append(trans * jnp.where(drive > 0.0, ma[f], mb[f]) * drive)
    return out


def grid_kernel(
    press, depth, sat, perm, pore, pairs, kind, table, CT,
    acc, wgt, hot, rows,
    X, K, TAB, PR, KD,
    sreq, rreq, lreq, loc, sresp, rresp,
    ysend, hx, hy, fxs, fys,
    lsem, ssem, rsem, qsem, psem, hsend, hrecv, open_,
):
    P_, D_, W_, O_ = (X.at[q] for q in range(4))
    KX, KY, KZ, PV = (K.at[q] for q in range(4))
    cols = pl.ds(0, COLS)
    ix = lax.axis_index("gx")
    iy = lax.axis_index("gy")
    nx = lax.axis_size("gx")
    ny = lax.axis_size("gy")

    def device(dx, dy):
        return (lax.rem(ix + (dx + nx), nx), lax.rem(iy + (dy + ny), ny))

    offsets = [(dx, dy) for dx in (-1, 0, 1) for dy in (-1, 0, 1)]
    barrier = pltpu.get_barrier_semaphore()
    iz = lax.rem(ix, LINE)
    first = iz == 0
    second = iz == 1
    last = iz == LINE - 1

    odd = lax.rem(iy, 2) == 1

    def greet(dx, dy):
        pl.semaphore_signal(barrier, inc=1, device_id=device(dx, dy), device_id_type=MESH)

    top = iy == ny - 1
    bottom = iy == 0
    @pl.when(jnp.logical_and(first, odd))
    def _():
        for dy in (-2, -1, 0):
            greet(LINE, dy)

    @pl.when(jnp.logical_and(jnp.logical_and(first, odd), iy < ny - 1))
    def _():
        greet(LINE, 1)

    for dx in (-1, 0, 1):
        ahead = (second, first, last)[dx + 1]
        for dy in (-1, 0, 1):
            if (dx, dy) == (0, 0):
                continue
            if dx:
                meets = jnp.logical_not(ahead)
                if dy == 1:
                    meets = jnp.logical_and(meets, jnp.logical_or(first, jnp.logical_not(top)))
            elif dy == 1:
                meets = jnp.logical_or(ahead, jnp.logical_not(top))
            else:
                meets = None
            if meets is None:
                greet(dx, dy)
            else:
                @pl.when(meets)
                def _(dx=dx, dy=dy):
                    greet(dx, dy)

    @pl.when(jnp.logical_and(first, odd))
    def _():
        for dy in (-1, 0):
            greet(LINE - 1, dy)

    loads = [
        pltpu.make_async_copy(src, dst, lsem.at[n])
        for n, src, dst in (
            (0, pairs, PR), (1, kind, KD),
            (2, press, X.at[0, cols]), (2, depth, X.at[1, cols]), (2, sat, X.at[pl.ds(2, 2), cols]),
            (3, table, TAB), (4, perm, K.at[pl.ds(0, 3), cols]), (4, pore, K.at[3, cols]),
        )
    ]
    for copy in loads:
        copy.start()
    state = pltpu.make_async_copy(X.at[:, cols], X.at[:, cols], lsem.at[2])

    zero = jnp.zeros((TILE, NZ), jnp.float32)
    for q in range(4):
        X[q, pl.ds(COLS, TILE), :] = zero
    K[1, pl.ds(COLS, TILE), :] = zero
    for f in range(3):
        for t in range(4):
            fxs[f, pl.ds(TILE * t, TILE), :] = zero
        for k in range(BLOCK):
            fys[k, f, pl.ds(0, TILE), :] = zero
        rows[f, pl.ds(32, TILE), :] = zero
        rows[f, pl.ds(SLOTS + 32, TILE), :] = zero

    @pl.when(last)
    def _():
        pl.semaphore_wait(barrier, jnp.where(bottom, 7, 9))

    for own_odd in (False, True):
        @pl.when(jnp.logical_and(last, odd if own_odd else jnp.logical_not(odd)))
        def _(own_odd=own_odd):
            pl.semaphore_signal(
                open_.at[0 if own_odd else 1], inc=1, device_id=device(1 - LINE, 0 if own_odd else 1),
                device_id_type=MESH,
            )

    for n in range(2):
        loads[n].wait()
    live = CT[0]
    log_y = ny.bit_length() - 1
    used = jnp.int32(0)
    words = [jnp.int32(0)] * CODES
    for r in range(32):
        target = PR[1, r]
        cx = ((target >> log_y) - ix + 1) & (nx - 1)
        cy = ((target & (ny - 1)) - iy + 1) & (ny - 1)
        code = cx * 3 + cy
        rank = (used >> (code * 3)) & 7
        on = jnp.where(r < live, 1, 0)
        used = used + (on << (code * 3))
        entry = ((r + 32) * on) << (rank * 6)
        for c in range(CODES):
            words[c] = words[c] + jnp.where(code == c, entry, 0)

    state.wait()
    loads[5].wait()
    lane = lax.broadcasted_iota(jnp.int32, (1, NZ), 1)
    idx0 = jnp.full((1, NZ), -1, jnp.int32)
    idx1 = jnp.full((1, NZ), -1, jnp.int32)

    def place(idx0, idx1, k, value):
        for copy in range(3):
            at = 2 * SLOTS * copy + k
            if at < NZ:
                idx0 = jnp.where(lane == at, value, idx0)
            else:
                idx1 = jnp.where(lane == at - NZ, value, idx1)
        return idx0, idx1

    for c in range(CODES):
        for s in range(CAP):
            entry = words[c] >> (6 * s)
            r = entry & 31
            full = jnp.where((entry & 32) > 0, 1.0, 0.0)
            src = PR[0, r]
            land = PR[2, r]
            kd = KD[r]
            for q, ref in enumerate((P_, D_, W_, O_)):
                sreq[c, pl.ds(4 * q + s, 1), :] = ref[pl.ds(src, 1), :]
            sreq[c, pl.ds(16 + s, 1), :] = TAB[pl.ds(kd, 1), :] * full
            sreq[c, pl.ds(20 + s, 1), :] = jnp.full((1, NZ), land, jnp.int32).astype(jnp.float32)
            idx0, idx1 = place(idx0, idx1, c * CAP + s, src)

    @pl.when(jnp.logical_not(last))
    def _():
        pl.semaphore_wait(barrier, jnp.where(first, jnp.where(bottom, 3, 4), jnp.where(bottom, jnp.where(second, 6, 5), 8)))

    def request(c, target):
        return pltpu.make_async_remote_copy(
            src_ref=sreq.at[c], dst_ref=rreq.at[c], send_sem=ssem.at[0], recv_sem=rsem.at[min(c, 3)],
            device_id=target, device_id_type=MESH,
        )

    def to_relay(c, to_odd):
        dx, dy = offsets[c]
        k = c if to_odd else 3 + c
        return pltpu.make_async_remote_copy(
            src_ref=sreq.at[c], dst_ref=lreq.at[k], send_sem=ssem.at[0], recv_sem=qsem.at[k],
            device_id=device(-LINE, dy if to_odd else dy + 1), device_id_type=MESH,
        )

    to_side = pltpu.make_async_remote_copy(
        src_ref=sreq.at[0], dst_ref=lreq.at[6], send_sem=ssem.at[0], recv_sem=qsem.at[6],
        device_id=device(0, -1), device_id_type=MESH,
    )
    from_side = pltpu.make_async_remote_copy(
        src_ref=lreq.at[6], dst_ref=lreq.at[0], send_sem=psem.at[0], recv_sem=qsem.at[0],
        device_id=device(-LINE, 0), device_id_type=MESH,
    )

    for own_odd in (False, True):
        @pl.when(jnp.logical_and(first, odd if own_odd else jnp.logical_not(odd)))
        def _(own_odd=own_odd):
            for c in (0, 2, 1):
                if c == 0 and not own_odd:
                    @pl.when(iy > 0)
                    def _():
                        to_relay(0, True).start()

                    @pl.when(iy == 0)
                    def _():
                        to_side.start()
                else:
                    to_relay(c, own_odd == (c == 1)).start()

    @pl.when(first)
    def _():
        for c in (3, 5):
            request(c, device(*offsets[c])).start()

    @pl.when(jnp.logical_and(jnp.logical_not(first), jnp.logical_not(bottom)))
    def _():
        for c in (6, 8, 0, 2, 3, 5, 7, 1):
            request(c, device(*offsets[c])).start()

    wraps = jnp.logical_and(jnp.logical_not(first), bottom)

    @pl.when(wraps)
    def _():
        for c in (8, 2, 5, 7, 1):
            request(c, device(*offsets[c])).start()

    for c, known in ((0, second), (6, last)):
        @pl.when(jnp.logical_and(bottom, known))
        def _(c=c):
            request(c, device(*offsets[c])).start()

    @pl.when(second)
    def _():
        for dy in (-1, 0, 1):
            pl.semaphore_signal(open_.at[2], inc=1, device_id=device(-1, dy), device_id_type=MESH)

    for dx in (-1, 0, 1):
        @pl.when(jnp.logical_and(jnp.logical_and(top, jnp.logical_not(first)), jnp.logical_not((second, first, last)[dx + 1])))
        def _(dx=dx):
            pl.semaphore_signal(open_.at[2], inc=1, device_id=device(dx, 1), device_id_type=MESH)

    eight = pl.ds(0, 8)
    requests = pltpu.make_async_remote_copy(
        src_ref=sreq.at[eight], dst_ref=rreq.at[eight], send_sem=ssem.at[0], recv_sem=rsem.at[0],
        device_id=device(0, 1), device_id_type=MESH,
    )

    for side, y in ((0, NY - 1), (1, 0)):
        for q, ref in enumerate((P_, D_, W_, O_)):
            ysend[side, q] = ref[pl.ds(y, NX, NY), :]
    pltpu.make_async_copy(K.at[:, cols], K.at[:, cols], lsem.at[4]).wait()
    for side, y in ((0, NY - 1), (1, 0)):
        ysend[side, 4] = KY[pl.ds(y, NX, NY), :]

    def halo(src, dst, n, dx, dy):
        return pltpu.make_async_remote_copy(
            src_ref=src, dst_ref=dst, send_sem=hsend.at[n], recv_sem=hrecv.at[n],
            device_id=device(dx, dy), device_id_type=MESH,
        )

    halos_x = []
    for side, (dx, x) in enumerate(((1, NX - 1), (-1, 0))):
        row = pl.ds(x * NY, NY)
        halos_x.append([
            halo(X.at[:, row], hx.at[side, pl.ds(0, 4)], side, dx, 0),
            halo(K.at[0, row], hx.at[side, 4], side, dx, 0),
        ])
    whole_x = [halo(hx.at[side], hx.at[side], side, dx, 0) for side, dx in enumerate((1, -1))]
    halos_y = [halo(ysend.at[side], hy.at[side], 2 + side, 0, dy) for side, dy in enumerate((1, -1))]
    goes = (ix < nx - 1, ix > 0, iy < ny - 1, iy > 0)
    comes = (goes[1], goes[0], goes[3], goes[2])

    @pl.when(jnp.logical_and(goes[0], jnp.logical_not(first)))
    def _():
        for copy in halos_x[0]:
            copy.start()

    @pl.when(jnp.logical_not(first))
    def _():
        for copy in halos_x[1]:
            copy.start()

    for side in range(2):
        @pl.when(goes[2 + side])
        def _(side=side):
            halos_y[side].start()

    lanes = lax.broadcasted_iota(jnp.int32, (TILE, NZ), 1)
    sublanes = lax.broadcasted_iota(jnp.int32, (TILE, NZ), 0)
    last_lane = lanes == NZ - 1
    last_sub = sublanes == TILE - 1

    def block(b, carry):
        for t in range(4):
            base = b * (BLOCK * NY) + TILE * t
            at = pl.ds(pl.multiple_of(base, TILE), TILE)
            p, d, w, o, kx = P_[at, :], D_[at, :], W_[at, :], O_[at, :], KX[at, :]
            m = mobility(w, o)
            fx = [fxs[f, pl.ds(TILE * t, TILE), :] for f in range(3)]
            for k in range(BLOCK):
                row = b * BLOCK + k
                at = pl.ds(pl.multiple_of(base + k * NY, TILE), TILE)
                nrow = jnp.minimum(row + 1, NX - 1)
                nat = pl.ds(pl.multiple_of(nrow * NY + TILE * t, TILE), TILE)
                pn, dn, wn, on, kn = P_[nat, :], D_[nat, :], W_[nat, :], O_[nat, :], KX[nat, :]
                mn = mobility(wn, on)
                inside = jnp.where(row < NX - 1, 2.0, 0.0)
                gx = fluxes(p, d, m, pn, dn, mn, inside * kx * kn / (kx + kn))
                net = [gx[f] - fx[f] for f in range(3)]
                uat = pl.ds(base + k * NY + 1, TILE)
                ky, ku = KY[at, :], KY[uat, :]
                gy = fluxes(p, d, m, P_[uat, :], D_[uat, :], mobility(W_[uat, :], O_[uat, :]), harmonic(ky, ku))
                for f in range(3):
                    g = jnp.where(last_sub, 0.0, gy[f]) if t == 3 else gy[f]
                    fys[k, f, pl.ds(TILE + TILE * t, TILE), :] = g
                    net[f] = net[f] + (g - fys[k, f, pl.ds(TILE + TILE * t - 1, TILE), :])
                kz = KZ[at, :]
                up = lambda v: pltpu.roll(v, NZ - 1, 1)
                tz = jnp.where(last_lane, 0.0, harmonic(kz, up(kz)))
                gz = fluxes(p, d, m, up(p), up(d), [up(v) for v in m], tz)
                wt = STEP / PV[at, :]
                wgt[at, :] = wt
                sats = (w, o, 1.0 - w - o)
                for f in range(3):
                    total = net[f] + (gz[f] - pltpu.roll(gz[f], 1, 1))
                    acc[f, at, :] = sats[f] - wt * total
                p, d, w, o, kx, m, fx = pn, dn, wn, on, kn, mn, gx
            for f in range(3):
                fxs[f, pl.ds(TILE * t, TILE), :] = fx[f]
        return carry

    blocks = NX // BLOCK
    early = jnp.where(first, jnp.where(odd, RELAY_AT, blocks), jnp.where(last, blocks // 2 - 2, blocks // 2))
    lax.fori_loop(0, early, block, 0)

    def relayed(n):
        part = pl.ds(0, n)
        return pltpu.make_async_remote_copy(
            src_ref=lreq.at[part], dst_ref=rreq.at[part], send_sem=psem.at[0], recv_sem=rsem.at[0],
            device_id=device(LINE - 1, 0), device_id_type=MESH,
        )

    beside = jnp.logical_and(first, iy == ny - 1)

    @pl.when(beside)
    def _():
        to_side.wait_recv()
        from_side.start()

    @pl.when(jnp.logical_and(first, odd))
    def _():
        for k in (3, 1, 5, 4, 2, 0):
            c = k % 3
            if k in (3, 1):
                pl.semaphore_wait(open_.at[k // 3], 1)
            to_relay(c, k < 3).wait_recv()
            pltpu.make_async_remote_copy(
                src_ref=lreq.at[k], dst_ref=rreq.at[c], send_sem=psem.at[0], recv_sem=rsem.at[c],
                device_id=device(LINE - 1, 0 if k < 3 else -1), device_id_type=MESH,
            ).start()

    @pl.when(first)
    def _():
        pl.semaphore_wait(open_.at[2], 3)
        for c in (6, 8, 7):
            request(c, device(*offsets[c])).start()
        for copy in halos_x[0]:
            copy.start()

    @pl.when(wraps)
    def _():
        pl.semaphore_wait(open_.at[2], jnp.where(jnp.logical_or(second, last), 2, 3))

    for c, known in ((6, last), (3, first), (0, second)):
        @pl.when(jnp.logical_and(wraps, jnp.logical_not(known)))
        def _(c=c):
            request(c, device(*offsets[c])).start()

    middle = jnp.where(first, blocks, early)
    lax.fori_loop(early, middle, block, 0)

    lands = {}

    def answer(codes):
        for n, c in codes:
            ref = sreq if n == HERE else rreq
            for s in range(CAP):
                lands[n, s] = jnp.clip(ref[c, pl.ds(20 + s, 1), :].astype(jnp.int32), 0, COLS - 1)[0, 0]
        for n, c in codes:
            for s in range(CAP):
                for q, ref in enumerate((P_, D_, W_, O_)):
                    loc[n, pl.ds(4 * q + s, 1), :] = ref[pl.ds(lands[n, s], 1), :]
        for n, c in codes:
            ref = sreq if n == HERE else rreq
            a = [ref[c, pl.ds(4 * q, 4), :] for q in range(5)]
            b = [loc[n, pl.ds(4 * q, 4), :] for q in range(4)]
            flow = fluxes(a[0], a[1], mobility(a[2], a[3]), b[0], b[1], mobility(b[2], b[3]), a[4])
            for f in range(3):
                sresp[c, pl.ds(4 * f, 4), :] = flow[f]
                rows[f, pl.ds(SLOTS + 4 * n, 4), :] = -flow[f]
                if n == HERE:
                    rows[f, pl.ds(4 * n, 4), :] = flow[f]
            sresp[c, pl.ds(12, 4), :] = jnp.zeros((4, NZ), jnp.float32)
            if n == HERE:
                continue
            pltpu.make_async_remote_copy(
                src_ref=sresp.at[c], dst_ref=rresp.at[c], send_sem=ssem.at[1], recv_sem=rsem.at[4],
                device_id=device(1, 1 - c) if n < 3 else device(-offsets[c][0], -offsets[c][1]),
                device_id_type=MESH,
            ).start()

    for n, c in ((0, jnp.where(odd, 1, 0)), (1, 2), (2, jnp.where(odd, 0, 1))):
        pltpu.make_async_remote_copy(
            src_ref=sreq.at[c], dst_ref=rreq.at[c], send_sem=ssem.at[0], recv_sem=rsem.at[c],
            device_id=device(0, 1), device_id_type=MESH,
        ).wait_recv()
        answer([(n, c)])
    five = pl.ds(3, 5)
    pltpu.make_async_remote_copy(
        src_ref=sreq.at[five], dst_ref=rreq.at[five], send_sem=ssem.at[0], recv_sem=rsem.at[3],
        device_id=device(0, 1), device_id_type=MESH,
    ).wait_recv()
    answer([(c, c) for c in (6, 8, 3, 5, 7, HERE)])
    answers = pltpu.make_async_remote_copy(
        src_ref=sresp.at[eight], dst_ref=rresp.at[eight], send_sem=ssem.at[1], recv_sem=rsem.at[4],
        device_id=device(0, 1), device_id_type=MESH,
    )

    @pl.when(jnp.logical_and(first, goes[1]))
    def _():
        for copy in halos_x[1]:
            copy.start()

    for c in range(CODES):
        for s in range(CAP):
            idx0, idx1 = place(idx0, idx1, SLOTS + c * CAP + s, lands[c, s])

    lax.fori_loop(middle, blocks, block, 0)

    def face(axis, side):
        far = [(hy if axis else hx)[side, q] for q in range(5)]
        if axis:
            at = pl.ds((NY - 1) if side else 0, NX, NY)
        else:
            at = pl.ds((NX - 1) * NY if side else 0, NY)
        near = [ref[at, :] for ref in (P_, D_, W_, O_, KY if axis else KX)]
        lo, hi = (near, far) if side else (far, near)
        flow = fluxes(
            lo[0], lo[1], mobility(lo[2], lo[3]), hi[0], hi[1], mobility(hi[2], hi[3]), harmonic(lo[4], hi[4])
        )
        wt = wgt[at, :]
        for f in range(3):
            step = wt * flow[f]
            acc[f, at, :] = acc[f, at, :] + (-step if side else step)

    for axis in range(2):
        for side in range(2):
            @pl.when(comes[2 * axis + side])
            def _(axis=axis, side=side):
                if axis:
                    halos_y[side].wait_recv()
                else:
                    whole_x[side].wait_recv()
                face(axis, side)

    idx = jnp.concatenate([idx0, idx1], axis=1)
    cell = lax.broadcasted_iota(jnp.int32, (32, 2 * NZ), 0)

    def mark(b, carry):
        start = pl.multiple_of(b * 32, 32)
        hot[pl.ds(start, 32), :] = jnp.where(cell + start == idx, 1.0, 0.0).astype(jnp.bfloat16)
        return carry

    lax.fori_loop(0, COLS // 32, mark, 0)

    answers.wait_recv()
    for c in range(CODES):
        if c != HERE:
            for f in range(3):
                rows[f, pl.ds(4 * c, 4), :] = rresp[c, pl.ds(4 * f, 4), :]
    requests.wait_send()
    answers.wait_send()
    for side in range(2):
        @pl.when(goes[side])
        def _(side=side):
            whole_x[side].wait_send()

        @pl.when(goes[2 + side])
        def _(side=side):
            halos_y[side].wait_send()

    @pl.when(jnp.logical_and(jnp.logical_and(first, odd), jnp.logical_not(top)))
    def _():
        relayed(6).wait_send()

    @pl.when(beside)
    def _():
        relayed(7).wait_send()


def add_kernel(acc, wgt, hot, rows, out, parts, held, sem):
    for f in range(3):
        value = rows[f]
        for k in range(3):
            part = value.astype(jnp.bfloat16)
            parts[pl.ds(2 * SLOTS * k, 2 * SLOTS), pl.ds(NZ * f, NZ)] = part
            value = value - part.astype(jnp.float32)
        parts[pl.ds(240, 16), pl.ds(NZ * f, NZ)] = jnp.zeros((16, NZ), jnp.bfloat16)
    size = COLS // 8
    for n in range(8):
        at = pl.ds(n * size, size)
        delta = jnp.dot(hot[at, :], parts[...], preferred_element_type=jnp.float32)
        wt = wgt[at, :]
        for f in range(3):
            held[f, at, :] = acc[f, at, :] - wt * delta[:, NZ * f:NZ * (f + 1)]
            pltpu.make_async_copy(held.at[f, at], out.at[f, at], sem).start()
    pltpu.make_async_copy(held, out, sem).wait()


def body(pressure, depth, saturation, permeability, pore_volume, fault_pairs, fault_kind, fault_count, fault_table):
    f32, i32 = jnp.float32, jnp.int32
    hbm = pl.BlockSpec(memory_space=pltpu.HBM)
    vmem = pl.BlockSpec(memory_space=pltpu.VMEM)
    V = pltpu.VMEM
    acc, wgt, hot, rows = pl.pallas_call(
        grid_kernel,
        out_shape=(
            V((3, COLS, NZ), f32), V((COLS, NZ), f32), V((COLS, 2 * NZ), jnp.bfloat16), V((3, 2 * SLOTS, NZ), f32),
        ),
        in_specs=[hbm] * 8 + [pl.BlockSpec(memory_space=pltpu.SMEM)],
        out_specs=(vmem,) * 4,
        scratch_shapes=[
            V((4, COLS + TILE, NZ), f32), V((4, COLS + TILE, NZ), f32), V((16, NZ), f32),
            pltpu.SMEM((3, 32), i32), pltpu.SMEM((32,), i32),
            V((CODES, 24, NZ), f32), V((CODES, 24, NZ), f32), V((7, 24, NZ), f32), V((CODES, 24, NZ), f32),
            V((CODES, 16, NZ), f32), V((CODES, 16, NZ), f32),
            V((2, 5, NX, NZ), f32), V((2, 5, NY, NZ), f32), V((2, 5, NX, NZ), f32),
            V((3, NY, NZ), f32), V((BLOCK, 3, TILE + NY, NZ), f32),
            pltpu.SemaphoreType.DMA((5,)), pltpu.SemaphoreType.DMA((2,)), pltpu.SemaphoreType.DMA((5,)),
            pltpu.SemaphoreType.DMA((7,)), pltpu.SemaphoreType.DMA((1,)),
            pltpu.SemaphoreType.DMA((4,)), pltpu.SemaphoreType.DMA((4,)), pltpu.SemaphoreType.REGULAR((3,)),
        ],
        compiler_params=pltpu.CompilerParams(collective_id=0, has_side_effects=True, vmem_limit_bytes=24 * 2**20),
        name="grid",
    )(
        *(
            pltpu.with_memory_space_constraint(x, pltpu.HBM)
            for x in (
                pressure.reshape(COLS, NZ), depth.reshape(COLS, NZ), saturation.reshape(2, COLS, NZ),
                permeability.reshape(3, COLS, NZ), pore_volume.reshape(COLS, NZ),
                fault_pairs.T, fault_kind, fault_table,
            )
        ),
        fault_count,
    )
    out = pl.pallas_call(
        add_kernel,
        out_shape=jax.ShapeDtypeStruct((3, COLS, NZ), f32),
        in_specs=[vmem] * 4,
        out_specs=hbm,
        scratch_shapes=[V((2 * NZ, 3 * NZ), jnp.bfloat16), V((3, COLS, NZ), f32), pltpu.SemaphoreType.DMA],
        compiler_params=pltpu.CompilerParams(vmem_limit_bytes=16 * 2**20),
        name="add",
    )(acc, wgt, hot, rows)
    return out.reshape(3, NX, NY, NZ)


def solution(mesh):
    in_specs = (
        P("gx", "gy", None),
        P("gx", "gy", None),
        P(None, "gx", "gy", None),
        P(None, "gx", "gy", None),
        P("gx", "gy", None),
        P(("gx", "gy"), None),
        P(("gx", "gy")),
        P(("gx", "gy")),
        P(),
    )
    out_specs = P(None, "gx", "gy", None)
    return jax.shard_map(body, mesh=mesh, in_specs=in_specs, out_specs=out_specs, check_vma=False)
```

```python
import jax
import jax.numpy as jnp
from jax import lax
from jax.experimental import pallas as pl
from jax.experimental.pallas import tpu as pltpu
from jax.sharding import PartitionSpec as P

CAP = 4
CODES = 9
HERE = 4
SLOTS = 40
RHO = (1.0, 0.8, 0.25)
STEP = 0.2
NX = 32
NY = 32
NZ = 128
COLS = NX * NY
TILE = 8
LINE = 4
BLOCK = 2
RELAY_AT = 6
MESH = pl.DeviceIdType.MESH


def mobility(sw, so):
    sg = 1.0 - sw - so
    return (sw * sw * 2.0, so * so, sg * sg * 4.0)


def harmonic(a, b):
    return 2.0 * a * b / (a + b)


def fluxes(pa, da, ma, pb, db, mb, trans):
    dp = pa - pb
    dd = da - db
    out = []
    for f in range(3):
        drive = dp - (dd if RHO[f] == 1.0 else RHO[f] * dd)
        out.append(trans * jnp.where(drive > 0.0, ma[f], mb[f]) * drive)
    return out


def grid_kernel(
    press, depth, sat, perm, pore, pairs, kind, table, CT,
    acc, wgt, hot, rows,
    X, K, TAB, PR, KD,
    sreq, rreq, lreq, loc, sresp, rresp,
    ysend, hx, hy, fxs, fys,
    lsem, ssem, rsem, qsem, psem, hsend, hrecv, open_,
):
    P_, D_, W_, O_ = (X.at[q] for q in range(4))
    KX, KY, KZ, PV = (K.at[q] for q in range(4))
    cols = pl.ds(0, COLS)
    ix = lax.axis_index("gx")
    iy = lax.axis_index("gy")
    nx = lax.axis_size("gx")
    ny = lax.axis_size("gy")

    def device(dx, dy):
        return (lax.rem(ix + (dx + nx), nx), lax.rem(iy + (dy + ny), ny))

    offsets = [(dx, dy) for dx in (-1, 0, 1) for dy in (-1, 0, 1)]
    barrier = pltpu.get_barrier_semaphore()
    iz = lax.rem(ix, LINE)
    first = iz == 0
    second = iz == 1
    last = iz == LINE - 1

    odd = lax.rem(iy, 2) == 1

    def greet(dx, dy):
        pl.semaphore_signal(barrier, inc=1, device_id=device(dx, dy), device_id_type=MESH)

    top = iy == ny - 1
    bottom = iy == 0
    @pl.when(jnp.logical_and(first, odd))
    def _():
        for dy in (-2, -1, 0):
            greet(LINE, dy)

    @pl.when(jnp.logical_and(jnp.logical_and(first, odd), iy < ny - 1))
    def _():
        greet(LINE, 1)

    for dx in (-1, 0, 1):
        ahead = (second, first, last)[dx + 1]
        for dy in (-1, 0, 1):
            if (dx, dy) == (0, 0):
                continue
            if dx:
                meets = jnp.logical_not(ahead)
                if dy == 1:
                    meets = jnp.logical_and(meets, jnp.logical_or(first, jnp.logical_not(top)))
            elif dy == 1:
                meets = jnp.logical_or(ahead, jnp.logical_not(top))
            else:
                meets = None
            if meets is None:
                greet(dx, dy)
            else:
                @pl.when(meets)
                def _(dx=dx, dy=dy):
                    greet(dx, dy)

    @pl.when(jnp.logical_and(first, odd))
    def _():
        for dy in (-1, 0):
            greet(LINE - 1, dy)

    loads = [
        pltpu.make_async_copy(src, dst, lsem.at[n])
        for n, src, dst in (
            (0, pairs, PR), (1, kind, KD),
            (2, press, X.at[0, cols]), (2, depth, X.at[1, cols]), (2, sat, X.at[pl.ds(2, 2), cols]),
            (3, table, TAB), (4, perm, K.at[pl.ds(0, 3), cols]), (4, pore, K.at[3, cols]),
        )
    ]
    for copy in loads:
        copy.start()
    state = pltpu.make_async_copy(X.at[:, cols], X.at[:, cols], lsem.at[2])

    zero = jnp.zeros((TILE, NZ), jnp.float32)
    for q in range(4):
        X[q, pl.ds(COLS, TILE), :] = zero
    K[1, pl.ds(COLS, TILE), :] = zero
    for f in range(3):
        for t in range(4):
            fxs[f, pl.ds(TILE * t, TILE), :] = zero
        for k in range(BLOCK):
            fys[k, f, pl.ds(0, TILE), :] = zero
        rows[f, pl.ds(32, TILE), :] = zero
        rows[f, pl.ds(SLOTS + 32, TILE), :] = zero

    @pl.when(last)
    def _():
        pl.semaphore_wait(barrier, jnp.where(bottom, 7, 9))

    for own_odd in (False, True):
        @pl.when(jnp.logical_and(last, odd if own_odd else jnp.logical_not(odd)))
        def _(own_odd=own_odd):
            pl.semaphore_signal(
                open_.at[0 if own_odd else 1], inc=1, device_id=device(1 - LINE, 0 if own_odd else 1),
                device_id_type=MESH,
            )

    for n in range(2):
        loads[n].wait()
    live = CT[0]
    log_y = ny.bit_length() - 1
    used = jnp.int32(0)
    words = [jnp.int32(0)] * CODES
    for r in range(32):
        target = PR[1, r]
        cx = ((target >> log_y) - ix + 1) & (nx - 1)
        cy = ((target & (ny - 1)) - iy + 1) & (ny - 1)
        code = cx * 3 + cy
        rank = (used >> (code * 3)) & 7
        on = jnp.where(r < live, 1, 0)
        used = used + (on << (code * 3))
        entry = ((r + 32) * on) << (rank * 6)
        for c in range(CODES):
            words[c] = words[c] + jnp.where(code == c, entry, 0)

    state.wait()
    loads[5].wait()
    lane = lax.broadcasted_iota(jnp.int32, (1, NZ), 1)
    idx0 = jnp.full((1, NZ), -1, jnp.int32)
    idx1 = jnp.full((1, NZ), -1, jnp.int32)

    def place(idx0, idx1, k, value):
        for copy in range(3):
            at = 2 * SLOTS * copy + k
            if at < NZ:
                idx0 = jnp.where(lane == at, value, idx0)
            else:
                idx1 = jnp.where(lane == at - NZ, value, idx1)
        return idx0, idx1

    for c in range(CODES):
        for s in range(CAP):
            entry = words[c] >> (6 * s)
            r = entry & 31
            full = jnp.where((entry & 32) > 0, 1.0, 0.0)
            src = PR[0, r]
            land = PR[2, r]
            kd = KD[r]
            for q, ref in enumerate((P_, D_, W_, O_)):
                sreq[c, pl.ds(4 * q + s, 1), :] = ref[pl.ds(src, 1), :]
            sreq[c, pl.ds(16 + s, 1), :] = TAB[pl.ds(kd, 1), :] * full
            sreq[c, pl.ds(20 + s, 1), :] = jnp.full((1, NZ), land, jnp.int32).astype(jnp.float32)
            idx0, idx1 = place(idx0, idx1, c * CAP + s, src)

    @pl.when(jnp.logical_not(last))
    def _():
        pl.semaphore_wait(barrier, jnp.where(first, jnp.where(bottom, 3, 4), jnp.where(bottom, jnp.where(second, 6, 5), 8)))

    def request(c, target):
        return pltpu.make_async_remote_copy(
            src_ref=sreq.at[c], dst_ref=rreq.at[c], send_sem=ssem.at[0], recv_sem=rsem.at[min(c, 3)],
            device_id=target, device_id_type=MESH,
        )

    def to_relay(c, to_odd):
        dx, dy = offsets[c]
        k = c if to_odd else 3 + c
        return pltpu.make_async_remote_copy(
            src_ref=sreq.at[c], dst_ref=lreq.at[k], send_sem=ssem.at[0], recv_sem=qsem.at[k],
            device_id=device(-LINE, dy if to_odd else dy + 1), device_id_type=MESH,
        )

    to_side = pltpu.make_async_remote_copy(
        src_ref=sreq.at[0], dst_ref=lreq.at[6], send_sem=ssem.at[0], recv_sem=qsem.at[6],
        device_id=device(0, -1), device_id_type=MESH,
    )
    from_side = pltpu.make_async_remote_copy(
        src_ref=lreq.at[6], dst_ref=lreq.at[0], send_sem=psem.at[0], recv_sem=qsem.at[0],
        device_id=device(-LINE, 0), device_id_type=MESH,
    )

    for own_odd in (False, True):
        @pl.when(jnp.logical_and(first, odd if own_odd else jnp.logical_not(odd)))
        def _(own_odd=own_odd):
            for c in (0, 2, 1):
                if c == 0 and not own_odd:
                    @pl.when(iy > 0)
                    def _():
                        to_relay(0, True).start()

                    @pl.when(iy == 0)
                    def _():
                        to_side.start()
                else:
                    to_relay(c, own_odd == (c == 1)).start()

    @pl.when(first)
    def _():
        for c in (3, 5):
            request(c, device(*offsets[c])).start()

    @pl.when(jnp.logical_and(jnp.logical_not(first), jnp.logical_not(bottom)))
    def _():
        for c in (6, 8, 0, 2, 3, 5, 7, 1):
            request(c, device(*offsets[c])).start()

    wraps = jnp.logical_and(jnp.logical_not(first), bottom)

    @pl.when(wraps)
    def _():
        for c in (8, 2, 5, 7, 1):
            request(c, device(*offsets[c])).start()

    for c, known in ((0, second), (6, last)):
        @pl.when(jnp.logical_and(bottom, known))
        def _(c=c):
            request(c, device(*offsets[c])).start()

    @pl.when(second)
    def _():
        for dy in (-1, 0, 1):
            pl.semaphore_signal(open_.at[2], inc=1, device_id=device(-1, dy), device_id_type=MESH)

    for dx in (-1, 0, 1):
        @pl.when(jnp.logical_and(jnp.logical_and(top, jnp.logical_not(first)), jnp.logical_not((second, first, last)[dx + 1])))
        def _(dx=dx):
            pl.semaphore_signal(open_.at[2], inc=1, device_id=device(dx, 1), device_id_type=MESH)

    eight = pl.ds(0, 8)
    requests = pltpu.make_async_remote_copy(
        src_ref=sreq.at[eight], dst_ref=rreq.at[eight], send_sem=ssem.at[0], recv_sem=rsem.at[0],
        device_id=device(0, 1), device_id_type=MESH,
    )

    for side, y in ((0, NY - 1), (1, 0)):
        for q, ref in enumerate((P_, D_, W_, O_)):
            ysend[side, q] = ref[pl.ds(y, NX, NY), :]
    pltpu.make_async_copy(K.at[:, cols], K.at[:, cols], lsem.at[4]).wait()
    for side, y in ((0, NY - 1), (1, 0)):
        ysend[side, 4] = KY[pl.ds(y, NX, NY), :]

    def halo(src, dst, n, dx, dy):
        return pltpu.make_async_remote_copy(
            src_ref=src, dst_ref=dst, send_sem=hsend.at[n], recv_sem=hrecv.at[n],
            device_id=device(dx, dy), device_id_type=MESH,
        )

    halos_x = []
    for side, (dx, x) in enumerate(((1, NX - 1), (-1, 0))):
        row = pl.ds(x * NY, NY)
        halos_x.append([
            halo(X.at[:, row], hx.at[side, pl.ds(0, 4)], side, dx, 0),
            halo(K.at[0, row], hx.at[side, 4], side, dx, 0),
        ])
    whole_x = [halo(hx.at[side], hx.at[side], side, dx, 0) for side, dx in enumerate((1, -1))]
    halos_y = [halo(ysend.at[side], hy.at[side], 2 + side, 0, dy) for side, dy in enumerate((1, -1))]
    goes = (ix < nx - 1, ix > 0, iy < ny - 1, iy > 0)
    comes = (goes[1], goes[0], goes[3], goes[2])

    @pl.when(jnp.logical_and(goes[0], jnp.logical_not(first)))
    def _():
        for copy in halos_x[0]:
            copy.start()

    @pl.when(jnp.logical_not(first))
    def _():
        for copy in halos_x[1]:
            copy.start()

    for side in range(2):
        @pl.when(goes[2 + side])
        def _(side=side):
            halos_y[side].start()

    lanes = lax.broadcasted_iota(jnp.int32, (TILE, NZ), 1)
    sublanes = lax.broadcasted_iota(jnp.int32, (TILE, NZ), 0)
    last_lane = lanes == NZ - 1
    last_sub = sublanes == TILE - 1

    def block(b, carry):
        for t in range(4):
            base = b * (BLOCK * NY) + TILE * t
            at = pl.ds(pl.multiple_of(base, TILE), TILE)
            p, d, w, o, kx = P_[at, :], D_[at, :], W_[at, :], O_[at, :], KX[at, :]
            m = mobility(w, o)
            fx = [fxs[f, pl.ds(TILE * t, TILE), :] for f in range(3)]
            for k in range(BLOCK):
                row = b * BLOCK + k
                at = pl.ds(pl.multiple_of(base + k * NY, TILE), TILE)
                nrow = jnp.minimum(row + 1, NX - 1)
                nat = pl.ds(pl.multiple_of(nrow * NY + TILE * t, TILE), TILE)
                pn, dn, wn, on, kn = P_[nat, :], D_[nat, :], W_[nat, :], O_[nat, :], KX[nat, :]
                mn = mobility(wn, on)
                inside = jnp.where(row < NX - 1, 2.0, 0.0)
                gx = fluxes(p, d, m, pn, dn, mn, inside * kx * kn / (kx + kn))
                net = [gx[f] - fx[f] for f in range(3)]
                uat = pl.ds(base + k * NY + 1, TILE)
                ky, ku = KY[at, :], KY[uat, :]
                gy = fluxes(p, d, m, P_[uat, :], D_[uat, :], mobility(W_[uat, :], O_[uat, :]), harmonic(ky, ku))
                for f in range(3):
                    g = jnp.where(last_sub, 0.0, gy[f]) if t == 3 else gy[f]
                    fys[k, f, pl.ds(TILE + TILE * t, TILE), :] = g
                    net[f] = net[f] + (g - fys[k, f, pl.ds(TILE + TILE * t - 1, TILE), :])
                kz = KZ[at, :]
                up = lambda v: pltpu.roll(v, NZ - 1, 1)
                tz = jnp.where(last_lane, 0.0, harmonic(kz, up(kz)))
                gz = fluxes(p, d, m, up(p), up(d), [up(v) for v in m], tz)
                wt = STEP / PV[at, :]
                wgt[at, :] = wt
                sats = (w, o, 1.0 - w - o)
                for f in range(3):
                    total = net[f] + (gz[f] - pltpu.roll(gz[f], 1, 1))
                    acc[f, at, :] = sats[f] - wt * total
                p, d, w, o, kx, m, fx = pn, dn, wn, on, kn, mn, gx
            for f in range(3):
                fxs[f, pl.ds(TILE * t, TILE), :] = fx[f]
        return carry

    blocks = NX // BLOCK
    early = jnp.where(first, jnp.where(odd, RELAY_AT, blocks), jnp.where(last, blocks // 2 - 2, blocks // 2))
    lax.fori_loop(0, early, block, 0)

    def relayed(n):
        part = pl.ds(0, n)
        return pltpu.make_async_remote_copy(
            src_ref=lreq.at[part], dst_ref=rreq.at[part], send_sem=psem.at[0], recv_sem=rsem.at[0],
            device_id=device(LINE - 1, 0), device_id_type=MESH,
        )

    beside = jnp.logical_and(first, iy == ny - 1)

    @pl.when(beside)
    def _():
        to_side.wait_recv()
        from_side.start()

    @pl.when(jnp.logical_and(first, odd))
    def _():
        for k in (3, 5, 1, 4, 2, 0):
            c = k % 3
            if k in (3, 1):
                pl.semaphore_wait(open_.at[k // 3], 1)
            to_relay(c, k < 3).wait_recv()
            pltpu.make_async_remote_copy(
                src_ref=lreq.at[k], dst_ref=rreq.at[c], send_sem=psem.at[0], recv_sem=rsem.at[c],
                device_id=device(LINE - 1, 0 if k < 3 else -1), device_id_type=MESH,
            ).start()

    @pl.when(first)
    def _():
        pl.semaphore_wait(open_.at[2], 3)
        for c in (6, 8, 7):
            request(c, device(*offsets[c])).start()
        for copy in halos_x[0]:
            copy.start()

    @pl.when(wraps)
    def _():
        pl.semaphore_wait(open_.at[2], jnp.where(jnp.logical_or(second, last), 2, 3))

    for c, known in ((6, last), (3, first), (0, second)):
        @pl.when(jnp.logical_and(wraps, jnp.logical_not(known)))
        def _(c=c):
            request(c, device(*offsets[c])).start()

    middle = jnp.where(first, blocks, early)
    lax.fori_loop(early, middle, block, 0)

    lands = {}

    def answer(codes):
        for n, c in codes:
            ref = sreq if n == HERE else rreq
            for s in range(CAP):
                lands[n, s] = jnp.clip(ref[c, pl.ds(20 + s, 1), :].astype(jnp.int32), 0, COLS - 1)[0, 0]
        for n, c in codes:
            for s in range(CAP):
                for q, ref in enumerate((P_, D_, W_, O_)):
                    loc[n, pl.ds(4 * q + s, 1), :] = ref[pl.ds(lands[n, s], 1), :]
        for n, c in codes:
            ref = sreq if n == HERE else rreq
            a = [ref[c, pl.ds(4 * q, 4), :] for q in range(5)]
            b = [loc[n, pl.ds(4 * q, 4), :] for q in range(4)]
            flow = fluxes(a[0], a[1], mobility(a[2], a[3]), b[0], b[1], mobility(b[2], b[3]), a[4])
            for f in range(3):
                sresp[c, pl.ds(4 * f, 4), :] = flow[f]
                rows[f, pl.ds(SLOTS + 4 * n, 4), :] = -flow[f]
                if n == HERE:
                    rows[f, pl.ds(4 * n, 4), :] = flow[f]
            sresp[c, pl.ds(12, 4), :] = jnp.zeros((4, NZ), jnp.float32)
            if n == HERE:
                continue
            pltpu.make_async_remote_copy(
                src_ref=sresp.at[c], dst_ref=rresp.at[c], send_sem=ssem.at[1], recv_sem=rsem.at[4],
                device_id=device(1, 1 - c) if n < 3 else device(-offsets[c][0], -offsets[c][1]),
                device_id_type=MESH,
            ).start()

    for n, c in ((0, jnp.where(odd, 1, 0)), (1, 2), (2, jnp.where(odd, 0, 1))):
        pltpu.make_async_remote_copy(
            src_ref=sreq.at[c], dst_ref=rreq.at[c], send_sem=ssem.at[0], recv_sem=rsem.at[c],
            device_id=device(0, 1), device_id_type=MESH,
        ).wait_recv()
        answer([(n, c)])
    five = pl.ds(3, 5)
    pltpu.make_async_remote_copy(
        src_ref=sreq.at[five], dst_ref=rreq.at[five], send_sem=ssem.at[0], recv_sem=rsem.at[3],
        device_id=device(0, 1), device_id_type=MESH,
    ).wait_recv()
    answer([(c, c) for c in (6, 8, 3, 5, 7, HERE)])
    answers = pltpu.make_async_remote_copy(
        src_ref=sresp.at[eight], dst_ref=rresp.at[eight], send_sem=ssem.at[1], recv_sem=rsem.at[4],
        device_id=device(0, 1), device_id_type=MESH,
    )

    @pl.when(jnp.logical_and(first, goes[1]))
    def _():
        for copy in halos_x[1]:
            copy.start()

    for c in range(CODES):
        for s in range(CAP):
            idx0, idx1 = place(idx0, idx1, SLOTS + c * CAP + s, lands[c, s])

    lax.fori_loop(middle, blocks, block, 0)

    def face(axis, side):
        far = [(hy if axis else hx)[side, q] for q in range(5)]
        if axis:
            at = pl.ds((NY - 1) if side else 0, NX, NY)
        else:
            at = pl.ds((NX - 1) * NY if side else 0, NY)
        near = [ref[at, :] for ref in (P_, D_, W_, O_, KY if axis else KX)]
        lo, hi = (near, far) if side else (far, near)
        flow = fluxes(
            lo[0], lo[1], mobility(lo[2], lo[3]), hi[0], hi[1], mobility(hi[2], hi[3]), harmonic(lo[4], hi[4])
        )
        wt = wgt[at, :]
        for f in range(3):
            step = wt * flow[f]
            acc[f, at, :] = acc[f, at, :] + (-step if side else step)

    for axis in range(2):
        for side in range(2):
            @pl.when(comes[2 * axis + side])
            def _(axis=axis, side=side):
                if axis:
                    halos_y[side].wait_recv()
                else:
                    whole_x[side].wait_recv()
                face(axis, side)

    idx = jnp.concatenate([idx0, idx1], axis=1)
    cell = lax.broadcasted_iota(jnp.int32, (32, 2 * NZ), 0)

    def mark(b, carry):
        start = pl.multiple_of(b * 32, 32)
        hot[pl.ds(start, 32), :] = jnp.where(cell + start == idx, 1.0, 0.0).astype(jnp.bfloat16)
        return carry

    lax.fori_loop(0, COLS // 32, mark, 0)

    answers.wait_recv()
    for c in range(CODES):
        if c != HERE:
            for f in range(3):
                rows[f, pl.ds(4 * c, 4), :] = rresp[c, pl.ds(4 * f, 4), :]
    requests.wait_send()
    answers.wait_send()
    for side in range(2):
        @pl.when(goes[side])
        def _(side=side):
            whole_x[side].wait_send()

        @pl.when(goes[2 + side])
        def _(side=side):
            halos_y[side].wait_send()

    @pl.when(jnp.logical_and(jnp.logical_and(first, odd), jnp.logical_not(top)))
    def _():
        relayed(6).wait_send()

    @pl.when(beside)
    def _():
        relayed(7).wait_send()


def add_kernel(acc, wgt, hot, rows, out, parts, held, sem):
    for f in range(3):
        value = rows[f]
        for k in range(3):
            part = value.astype(jnp.bfloat16)
            parts[pl.ds(2 * SLOTS * k, 2 * SLOTS), pl.ds(NZ * f, NZ)] = part
            value = value - part.astype(jnp.float32)
        parts[pl.ds(240, 16), pl.ds(NZ * f, NZ)] = jnp.zeros((16, NZ), jnp.bfloat16)
    size = COLS // 8
    for n in range(8):
        at = pl.ds(n * size, size)
        delta = jnp.dot(hot[at, :], parts[...], preferred_element_type=jnp.float32)
        wt = wgt[at, :]
        for f in range(3):
            held[f, at, :] = acc[f, at, :] - wt * delta[:, NZ * f:NZ * (f + 1)]
            pltpu.make_async_copy(held.at[f, at], out.at[f, at], sem).start()
    pltpu.make_async_copy(held, out, sem).wait()


def body(pressure, depth, saturation, permeability, pore_volume, fault_pairs, fault_kind, fault_count, fault_table):
    f32, i32 = jnp.float32, jnp.int32
    hbm = pl.BlockSpec(memory_space=pltpu.HBM)
    vmem = pl.BlockSpec(memory_space=pltpu.VMEM)
    V = pltpu.VMEM
    acc, wgt, hot, rows = pl.pallas_call(
        grid_kernel,
        out_shape=(
            V((3, COLS, NZ), f32), V((COLS, NZ), f32), V((COLS, 2 * NZ), jnp.bfloat16), V((3, 2 * SLOTS, NZ), f32),
        ),
        in_specs=[hbm] * 8 + [pl.BlockSpec(memory_space=pltpu.SMEM)],
        out_specs=(vmem,) * 4,
        scratch_shapes=[
            V((4, COLS + TILE, NZ), f32), V((4, COLS + TILE, NZ), f32), V((16, NZ), f32),
            pltpu.SMEM((3, 32), i32), pltpu.SMEM((32,), i32),
            V((CODES, 24, NZ), f32), V((CODES, 24, NZ), f32), V((7, 24, NZ), f32), V((CODES, 24, NZ), f32),
            V((CODES, 16, NZ), f32), V((CODES, 16, NZ), f32),
            V((2, 5, NX, NZ), f32), V((2, 5, NY, NZ), f32), V((2, 5, NX, NZ), f32),
            V((3, NY, NZ), f32), V((BLOCK, 3, TILE + NY, NZ), f32),
            pltpu.SemaphoreType.DMA((5,)), pltpu.SemaphoreType.DMA((2,)), pltpu.SemaphoreType.DMA((5,)),
            pltpu.SemaphoreType.DMA((7,)), pltpu.SemaphoreType.DMA((1,)),
            pltpu.SemaphoreType.DMA((4,)), pltpu.SemaphoreType.DMA((4,)), pltpu.SemaphoreType.REGULAR((3,)),
        ],
        compiler_params=pltpu.CompilerParams(collective_id=0, has_side_effects=True, vmem_limit_bytes=24 * 2**20),
        name="grid",
    )(
        *(
            pltpu.with_memory_space_constraint(x, pltpu.HBM)
            for x in (
                pressure.reshape(COLS, NZ), depth.reshape(COLS, NZ), saturation.reshape(2, COLS, NZ),
                permeability.reshape(3, COLS, NZ), pore_volume.reshape(COLS, NZ),
                fault_pairs.T, fault_kind, fault_table,
            )
        ),
        fault_count,
    )
    out = pl.pallas_call(
        add_kernel,
        out_shape=jax.ShapeDtypeStruct((3, COLS, NZ), f32),
        in_specs=[vmem] * 4,
        out_specs=hbm,
        scratch_shapes=[V((2 * NZ, 3 * NZ), jnp.bfloat16), V((3, COLS, NZ), f32), pltpu.SemaphoreType.DMA],
        compiler_params=pltpu.CompilerParams(vmem_limit_bytes=16 * 2**20),
        name="add",
    )(acc, wgt, hot, rows)
    return out.reshape(3, NX, NY, NZ)


def solution(mesh):
    in_specs = (
        P("gx", "gy", None),
        P("gx", "gy", None),
        P(None, "gx", "gy", None),
        P(None, "gx", "gy", None),
        P("gx", "gy", None),
        P(("gx", "gy"), None),
        P(("gx", "gy")),
        P(("gx", "gy")),
        P(),
    )
    out_specs = P(None, "gx", "gy", None)
    return jax.shard_map(body, mesh=mesh, in_specs=in_specs, out_specs=out_specs, check_vma=False)
```

```python
import jax
import jax.numpy as jnp
from jax import lax
from jax.experimental import pallas as pl
from jax.experimental.pallas import tpu as pltpu
from jax.sharding import PartitionSpec as P

CAP = 4
CODES = 9
HERE = 4
SLOTS = 40
RHO = (1.0, 0.8, 0.25)
STEP = 0.2
NX = 32
NY = 32
NZ = 128
COLS = NX * NY
TILE = 8
LINE = 4
BLOCK = 2
RELAY_AT = 6
MESH = pl.DeviceIdType.MESH


def mobility(sw, so):
    sg = 1.0 - sw - so
    return (sw * sw * 2.0, so * so, sg * sg * 4.0)


def harmonic(a, b):
    return 2.0 * a * b / (a + b)


def fluxes(pa, da, ma, pb, db, mb, trans):
    dp = pa - pb
    dd = da - db
    out = []
    for f in range(3):
        drive = dp - (dd if RHO[f] == 1.0 else RHO[f] * dd)
        out.append(trans * jnp.where(drive > 0.0, ma[f], mb[f]) * drive)
    return out


def grid_kernel(
    press, depth, sat, perm, pore, pairs, kind, table, CT,
    acc, wgt, hot, rows,
    X, K, TAB, PR, KD,
    sreq, rreq, lreq, loc, sresp, rresp,
    ysend, hx, hy, fxs, fys,
    lsem, ssem, rsem, qsem, psem, hsend, hrecv, open_,
):
    P_, D_, W_, O_ = (X.at[q] for q in range(4))
    KX, KY, KZ, PV = (K.at[q] for q in range(4))
    cols = pl.ds(0, COLS)
    ix = lax.axis_index("gx")
    iy = lax.axis_index("gy")
    nx = lax.axis_size("gx")
    ny = lax.axis_size("gy")

    def device(dx, dy):
        return (lax.rem(ix + (dx + nx), nx), lax.rem(iy + (dy + ny), ny))

    offsets = [(dx, dy) for dx in (-1, 0, 1) for dy in (-1, 0, 1)]
    barrier = pltpu.get_barrier_semaphore()
    iz = lax.rem(ix, LINE)
    first = iz == 0
    second = iz == 1
    last = iz == LINE - 1

    odd = lax.rem(iy, 2) == 1

    def greet(dx, dy):
        pl.semaphore_signal(barrier, inc=1, device_id=device(dx, dy), device_id_type=MESH)

    top = iy == ny - 1
    bottom = iy == 0
    @pl.when(jnp.logical_and(first, odd))
    def _():
        for dy in (-2, -1, 0):
            greet(LINE, dy)

    @pl.when(jnp.logical_and(jnp.logical_and(first, odd), iy < ny - 1))
    def _():
        greet(LINE, 1)

    for dx in (-1, 0, 1):
        ahead = (second, first, last)[dx + 1]
        for dy in (-1, 0, 1):
            if (dx, dy) == (0, 0):
                continue
            if dx:
                meets = jnp.logical_not(ahead)
                if dy == 1:
                    meets = jnp.logical_and(meets, jnp.logical_or(first, jnp.logical_not(top)))
            elif dy == 1:
                meets = jnp.logical_or(ahead, jnp.logical_not(top))
            else:
                meets = None
            if meets is None:
                greet(dx, dy)
            else:
                @pl.when(meets)
                def _(dx=dx, dy=dy):
                    greet(dx, dy)

    @pl.when(jnp.logical_and(first, odd))
    def _():
        for dy in (-1, 0):
            greet(LINE - 1, dy)

    loads = [
        pltpu.make_async_copy(src, dst, lsem.at[n])
        for n, src, dst in (
            (0, pairs, PR), (1, kind, KD),
            (2, press, X.at[0, cols]), (2, depth, X.at[1, cols]), (2, sat, X.at[pl.ds(2, 2), cols]),
            (3, table, TAB.at[pl.ds(0, 16)]), (4, perm, K.at[pl.ds(0, 3), cols]), (4, pore, K.at[3, cols]),
        )
    ]
    for copy in loads:
        copy.start()
    state = pltpu.make_async_copy(X.at[:, cols], X.at[:, cols], lsem.at[2])

    zero = jnp.zeros((TILE, NZ), jnp.float32)
    for q in range(4):
        X[q, pl.ds(COLS, TILE), :] = zero
    K[1, pl.ds(COLS, TILE), :] = zero
    for f in range(3):
        for t in range(4):
            fxs[f, pl.ds(TILE * t, TILE), :] = zero
        for k in range(BLOCK):
            fys[k, f, pl.ds(0, TILE), :] = zero
        rows[f, pl.ds(32, TILE), :] = zero
        rows[f, pl.ds(SLOTS + 32, TILE), :] = zero

    @pl.when(last)
    def _():
        pl.semaphore_wait(barrier, jnp.where(bottom, 7, 9))

    for own_odd in (False, True):
        @pl.when(jnp.logical_and(last, odd if own_odd else jnp.logical_not(odd)))
        def _(own_odd=own_odd):
            pl.semaphore_signal(
                open_.at[0 if own_odd else 1], inc=1, device_id=device(1 - LINE, 0 if own_odd else 1),
                device_id_type=MESH,
            )

    for n in range(2):
        loads[n].wait()
    live = CT[0]
    log_y = ny.bit_length() - 1
    used = jnp.int32(0)
    words = [jnp.int32(0)] * CODES
    for r in range(32):
        target = PR[1, r]
        cx = ((target >> log_y) - ix + 1) & (nx - 1)
        cy = ((target & (ny - 1)) - iy + 1) & (ny - 1)
        code = cx * 3 + cy
        rank = (used >> (code * 3)) & 7
        on = jnp.where(r < live, 1, 0)
        used = used + (on << (code * 3))
        entry = ((r + 32) * on) << (rank * 6)
        for c in range(CODES):
            words[c] = words[c] + jnp.where(code == c, entry, 0)

    state.wait()
    loads[5].wait()
    lane = lax.broadcasted_iota(jnp.int32, (1, NZ), 1)
    idx0 = jnp.full((1, NZ), -1, jnp.int32)
    idx1 = jnp.full((1, NZ), -1, jnp.int32)

    def place(idx0, idx1, k, value):
        for copy in range(3):
            at = 2 * SLOTS * copy + k
            if at < NZ:
                idx0 = jnp.where(lane == at, value, idx0)
            else:
                idx1 = jnp.where(lane == at - NZ, value, idx1)
        return idx0, idx1

    for c in range(CODES):
        for s in range(CAP):
            entry = words[c] >> (6 * s)
            r = entry & 31
            full = jnp.where((entry & 32) > 0, 1.0, 0.0)
            src = PR[0, r]
            land = PR[2, r]
            kd = KD[r]
            for q, ref in enumerate((P_, D_, W_, O_)):
                sreq[c, pl.ds(4 * q + s, 1), :] = ref[pl.ds(src, 1), :]
            sreq[c, pl.ds(16 + s, 1), :] = TAB[pl.ds(kd, 1), :] * full
            sreq[c, pl.ds(20 + s, 1), :] = jnp.full((1, NZ), land, jnp.int32).astype(jnp.float32)
            idx0, idx1 = place(idx0, idx1, c * CAP + s, src)

    @pl.when(jnp.logical_not(last))
    def _():
        pl.semaphore_wait(barrier, jnp.where(first, jnp.where(bottom, 3, 4), jnp.where(bottom, jnp.where(second, 6, 5), 8)))

    def request(c, target):
        return pltpu.make_async_remote_copy(
            src_ref=sreq.at[c], dst_ref=rreq.at[c], send_sem=ssem.at[0], recv_sem=rsem.at[min(c, 3)],
            device_id=target, device_id_type=MESH,
        )

    def to_relay(c, to_odd):
        dx, dy = offsets[c]
        k = c if to_odd else 3 + c
        return pltpu.make_async_remote_copy(
            src_ref=sreq.at[c], dst_ref=lreq.at[k], send_sem=ssem.at[0], recv_sem=qsem.at[k],
            device_id=device(-LINE, dy if to_odd else dy + 1), device_id_type=MESH,
        )

    to_side = pltpu.make_async_remote_copy(
        src_ref=sreq.at[0], dst_ref=lreq.at[6], send_sem=ssem.at[0], recv_sem=qsem.at[6],
        device_id=device(0, -1), device_id_type=MESH,
    )
    from_side = pltpu.make_async_remote_copy(
        src_ref=lreq.at[6], dst_ref=lreq.at[0], send_sem=psem.at[0], recv_sem=qsem.at[0],
        device_id=device(-LINE, 0), device_id_type=MESH,
    )

    for own_odd in (False, True):
        @pl.when(jnp.logical_and(first, odd if own_odd else jnp.logical_not(odd)))
        def _(own_odd=own_odd):
            for c in (0, 2, 1):
                if c == 0 and not own_odd:
                    @pl.when(iy > 0)
                    def _():
                        to_relay(0, True).start()

                    @pl.when(iy == 0)
                    def _():
                        to_side.start()
                else:
                    to_relay(c, own_odd == (c == 1)).start()

    @pl.when(first)
    def _():
        for c in (3, 5):
            request(c, device(*offsets[c])).start()

    @pl.when(jnp.logical_and(jnp.logical_not(first), jnp.logical_not(bottom)))
    def _():
        for c in (6, 8, 0, 2, 3, 5, 7, 1):
            request(c, device(*offsets[c])).start()

    wraps = jnp.logical_and(jnp.logical_not(first), bottom)

    @pl.when(wraps)
    def _():
        for c in (8, 2, 5, 7, 1):
            request(c, device(*offsets[c])).start()

    for c, known in ((0, second), (6, last)):
        @pl.when(jnp.logical_and(bottom, known))
        def _(c=c):
            request(c, device(*offsets[c])).start()

    @pl.when(second)
    def _():
        for dy in (-1, 0, 1):
            pl.semaphore_signal(open_.at[2], inc=1, device_id=device(-1, dy), device_id_type=MESH)

    for dx in (-1, 0, 1):
        @pl.when(jnp.logical_and(jnp.logical_and(top, jnp.logical_not(first)), jnp.logical_not((second, first, last)[dx + 1])))
        def _(dx=dx):
            pl.semaphore_signal(open_.at[2], inc=1, device_id=device(dx, 1), device_id_type=MESH)

    eight = pl.ds(0, 8)
    requests = pltpu.make_async_remote_copy(
        src_ref=sreq.at[eight], dst_ref=rreq.at[eight], send_sem=ssem.at[0], recv_sem=rsem.at[0],
        device_id=device(0, 1), device_id_type=MESH,
    )

    for side, y in ((0, NY - 1), (1, 0)):
        for q, ref in enumerate((P_, D_, W_, O_)):
            ysend[side, q] = ref[pl.ds(y, NX, NY), :]
    pltpu.make_async_copy(K.at[:, cols], K.at[:, cols], lsem.at[4]).wait()
    for side, y in ((0, NY - 1), (1, 0)):
        ysend[side, 4] = KY[pl.ds(y, NX, NY), :]

    def halo(src, dst, n, dx, dy):
        return pltpu.make_async_remote_copy(
            src_ref=src, dst_ref=dst, send_sem=hsend.at[n], recv_sem=hrecv.at[n],
            device_id=device(dx, dy), device_id_type=MESH,
        )

    halos_x = []
    for side, (dx, x) in enumerate(((1, NX - 1), (-1, 0))):
        row = pl.ds(x * NY, NY)
        halos_x.append([
            halo(X.at[:, row], hx.at[side, pl.ds(0, 4)], side, dx, 0),
            halo(K.at[0, row], hx.at[side, 4], side, dx, 0),
        ])
    whole_x = [halo(hx.at[side], hx.at[side], side, dx, 0) for side, dx in enumerate((1, -1))]
    halos_y = [halo(ysend.at[side], hy.at[side], 2 + side, 0, dy) for side, dy in enumerate((1, -1))]
    goes = (ix < nx - 1, ix > 0, iy < ny - 1, iy > 0)
    comes = (goes[1], goes[0], goes[3], goes[2])

    @pl.when(jnp.logical_and(goes[0], jnp.logical_not(first)))
    def _():
        for copy in halos_x[0]:
            copy.start()

    @pl.when(jnp.logical_not(first))
    def _():
        for copy in halos_x[1]:
            copy.start()

    for side in range(2):
        @pl.when(goes[2 + side])
        def _(side=side):
            halos_y[side].start()

    lanes = lax.broadcasted_iota(jnp.int32, (TILE, NZ), 1)
    sublanes = lax.broadcasted_iota(jnp.int32, (TILE, NZ), 0)
    last_lane = lanes == NZ - 1
    last_sub = sublanes == TILE - 1

    def block(b, carry):
        for t in range(4):
            base = b * (BLOCK * NY) + TILE * t
            at = pl.ds(pl.multiple_of(base, TILE), TILE)
            p, d, w, o, kx = P_[at, :], D_[at, :], W_[at, :], O_[at, :], KX[at, :]
            m = mobility(w, o)
            fx = [fxs[f, pl.ds(TILE * t, TILE), :] for f in range(3)]
            for k in range(BLOCK):
                row = b * BLOCK + k
                at = pl.ds(pl.multiple_of(base + k * NY, TILE), TILE)
                nrow = jnp.minimum(row + 1, NX - 1)
                nat = pl.ds(pl.multiple_of(nrow * NY + TILE * t, TILE), TILE)
                pn, dn, wn, on, kn = P_[nat, :], D_[nat, :], W_[nat, :], O_[nat, :], KX[nat, :]
                mn = mobility(wn, on)
                inside = jnp.where(row < NX - 1, 2.0, 0.0)
                gx = fluxes(p, d, m, pn, dn, mn, inside * kx * kn / (kx + kn))
                net = [gx[f] - fx[f] for f in range(3)]
                uat = pl.ds(base + k * NY + 1, TILE)
                ky, ku = KY[at, :], KY[uat, :]
                gy = fluxes(p, d, m, P_[uat, :], D_[uat, :], mobility(W_[uat, :], O_[uat, :]), harmonic(ky, ku))
                for f in range(3):
                    g = jnp.where(last_sub, 0.0, gy[f]) if t == 3 else gy[f]
                    fys[k, f, pl.ds(TILE + TILE * t, TILE), :] = g
                    net[f] = net[f] + (g - fys[k, f, pl.ds(TILE + TILE * t - 1, TILE), :])
                kz = KZ[at, :]
                up = lambda v: pltpu.roll(v, NZ - 1, 1)
                tz = jnp.where(last_lane, 0.0, harmonic(kz, up(kz)))
                gz = fluxes(p, d, m, up(p), up(d), [up(v) for v in m], tz)
                wt = STEP / PV[at, :]
                wgt[at, :] = wt
                sats = (w, o, 1.0 - w - o)
                for f in range(3):
                    total = net[f] + (gz[f] - pltpu.roll(gz[f], 1, 1))
                    acc[f, at, :] = sats[f] - wt * total
                p, d, w, o, kx, m, fx = pn, dn, wn, on, kn, mn, gx
            for f in range(3):
                fxs[f, pl.ds(TILE * t, TILE), :] = fx[f]
        return carry

    blocks = NX // BLOCK
    early = jnp.where(first, jnp.where(odd, RELAY_AT, blocks), jnp.where(last, blocks // 2 - 2, blocks // 2))
    lax.fori_loop(0, early, block, 0)

    def relayed(n):
        part = pl.ds(0, n)
        return pltpu.make_async_remote_copy(
            src_ref=lreq.at[part], dst_ref=rreq.at[part], send_sem=psem.at[0], recv_sem=rsem.at[0],
            device_id=device(LINE - 1, 0), device_id_type=MESH,
        )

    beside = jnp.logical_and(first, iy == ny - 1)

    @pl.when(beside)
    def _():
        to_side.wait_recv()
        from_side.start()

    @pl.when(jnp.logical_and(first, odd))
    def _():
        for k in (3, 5, 1, 4, 2, 0):
            c = k % 3
            if k in (3, 1):
                pl.semaphore_wait(open_.at[k // 3], 1)
            to_relay(c, k < 3).wait_recv()
            pltpu.make_async_remote_copy(
                src_ref=lreq.at[k], dst_ref=rreq.at[c], send_sem=psem.at[0], recv_sem=rsem.at[c],
                device_id=device(LINE - 1, 0 if k < 3 else -1), device_id_type=MESH,
            ).start()

    @pl.when(first)
    def _():
        pl.semaphore_wait(open_.at[2], 3)
        for c in (6, 8, 7):
            request(c, device(*offsets[c])).start()
        for copy in halos_x[0]:
            copy.start()

    @pl.when(wraps)
    def _():
        pl.semaphore_wait(open_.at[2], jnp.where(jnp.logical_or(second, last), 2, 3))

    for c, known in ((6, last), (3, first), (0, second)):
        @pl.when(jnp.logical_and(wraps, jnp.logical_not(known)))
        def _(c=c):
            request(c, device(*offsets[c])).start()

    middle = jnp.where(first, blocks, early)
    lax.fori_loop(early, middle, block, 0)

    lands = {}

    def answer(codes):
        for n, c in codes:
            ref = sreq if n == HERE else rreq
            for s in range(CAP):
                lands[n, s] = jnp.clip(ref[c, pl.ds(20 + s, 1), :].astype(jnp.int32), 0, COLS - 1)[0, 0]
        for n, c in codes:
            for s in range(CAP):
                for q, ref in enumerate((P_, D_, W_, O_)):
                    loc[n, pl.ds(4 * q + s, 1), :] = ref[pl.ds(lands[n, s], 1), :]
        for n, c in codes:
            ref = sreq if n == HERE else rreq
            a = [ref[c, pl.ds(4 * q, 4), :] for q in range(5)]
            b = [loc[n, pl.ds(4 * q, 4), :] for q in range(4)]
            flow = fluxes(a[0], a[1], mobility(a[2], a[3]), b[0], b[1], mobility(b[2], b[3]), a[4])
            for f in range(3):
                sresp[c, pl.ds(4 * f, 4), :] = flow[f]
                rows[f, pl.ds(SLOTS + 4 * n, 4), :] = -flow[f]
                if n == HERE:
                    rows[f, pl.ds(4 * n, 4), :] = flow[f]
            sresp[c, pl.ds(12, 4), :] = jnp.zeros((4, NZ), jnp.float32)
            if n == HERE:
                continue
            pltpu.make_async_remote_copy(
                src_ref=sresp.at[c], dst_ref=rresp.at[c], send_sem=ssem.at[1], recv_sem=rsem.at[4],
                device_id=device(1, 1 - c) if n < 3 else device(-offsets[c][0], -offsets[c][1]),
                device_id_type=MESH,
            ).start()

    for n, c in ((0, jnp.where(odd, 1, 0)), (1, 2), (2, jnp.where(odd, 0, 1))):
        pltpu.make_async_remote_copy(
            src_ref=sreq.at[c], dst_ref=rreq.at[c], send_sem=ssem.at[0], recv_sem=rsem.at[c],
            device_id=device(0, 1), device_id_type=MESH,
        ).wait_recv()
        answer([(n, c)])
    five = pl.ds(3, 5)
    pltpu.make_async_remote_copy(
        src_ref=sreq.at[five], dst_ref=rreq.at[five], send_sem=ssem.at[0], recv_sem=rsem.at[3],
        device_id=device(0, 1), device_id_type=MESH,
    ).wait_recv()
    answer([(c, c) for c in (6, 8, 3, 5, 7, HERE)])
    answers = pltpu.make_async_remote_copy(
        src_ref=sresp.at[eight], dst_ref=rresp.at[eight], send_sem=ssem.at[1], recv_sem=rsem.at[4],
        device_id=device(0, 1), device_id_type=MESH,
    )

    @pl.when(jnp.logical_and(first, goes[1]))
    def _():
        for copy in halos_x[1]:
            copy.start()

    for c in range(CODES):
        for s in range(CAP):
            idx0, idx1 = place(idx0, idx1, SLOTS + c * CAP + s, lands[c, s])

    lax.fori_loop(middle, blocks, block, 0)

    def face(axis, side):
        far = [(hy if axis else hx)[side, q] for q in range(5)]
        if axis:
            at = pl.ds((NY - 1) if side else 0, NX, NY)
        else:
            at = pl.ds((NX - 1) * NY if side else 0, NY)
        near = [ref[at, :] for ref in (P_, D_, W_, O_, KY if axis else KX)]
        lo, hi = (near, far) if side else (far, near)
        flow = fluxes(
            lo[0], lo[1], mobility(lo[2], lo[3]), hi[0], hi[1], mobility(hi[2], hi[3]), harmonic(lo[4], hi[4])
        )
        wt = wgt[at, :]
        for f in range(3):
            step = wt * flow[f]
            acc[f, at, :] = acc[f, at, :] + (-step if side else step)

    for axis in range(2):
        for side in range(2):
            @pl.when(comes[2 * axis + side])
            def _(axis=axis, side=side):
                if axis:
                    halos_y[side].wait_recv()
                else:
                    whole_x[side].wait_recv()
                face(axis, side)

    idx = jnp.concatenate([idx0, idx1], axis=1)
    cell = lax.broadcasted_iota(jnp.int32, (32, 2 * NZ), 0)

    def mark(b, carry):
        start = pl.multiple_of(b * 32, 32)
        hot[pl.ds(start, 32), :] = jnp.where(cell + start == idx, 1.0, 0.0).astype(jnp.bfloat16)
        return carry

    lax.fori_loop(0, COLS // 32, mark, 0)

    answers.wait_recv()
    for c in range(CODES):
        if c != HERE:
            for f in range(3):
                rows[f, pl.ds(4 * c, 4), :] = rresp[c, pl.ds(4 * f, 4), :]
    requests.wait_send()
    answers.wait_send()
    for side in range(2):
        @pl.when(goes[side])
        def _(side=side):
            whole_x[side].wait_send()

        @pl.when(goes[2 + side])
        def _(side=side):
            halos_y[side].wait_send()

    @pl.when(jnp.logical_and(jnp.logical_and(first, odd), jnp.logical_not(top)))
    def _():
        relayed(6).wait_send()

    @pl.when(beside)
    def _():
        relayed(7).wait_send()


def add_kernel(acc, wgt, hot, rows, out, parts, held, sem):
    for f in range(3):
        value = rows[f]
        for k in range(3):
            part = value.astype(jnp.bfloat16)
            parts[pl.ds(2 * SLOTS * k, 2 * SLOTS), pl.ds(NZ * f, NZ)] = part
            value = value - part.astype(jnp.float32)
        parts[pl.ds(240, 16), pl.ds(NZ * f, NZ)] = jnp.zeros((16, NZ), jnp.bfloat16)
    size = COLS // 8
    for n in range(8):
        at = pl.ds(n * size, size)
        delta = jnp.dot(hot[at, :], parts[...], preferred_element_type=jnp.float32)
        wt = wgt[at, :]
        for f in range(3):
            held[f, at, :] = acc[f, at, :] - wt * delta[:, NZ * f:NZ * (f + 1)]
            pltpu.make_async_copy(held.at[f, at], out.at[f, at], sem).start()
    pltpu.make_async_copy(held, out, sem).wait()


def body(pressure, depth, saturation, permeability, pore_volume, fault_pairs, fault_kind, fault_count, fault_table):
    f32, i32 = jnp.float32, jnp.int32
    hbm = pl.BlockSpec(memory_space=pltpu.HBM)
    vmem = pl.BlockSpec(memory_space=pltpu.VMEM)
    V = pltpu.VMEM
    acc, wgt, hot, rows = pl.pallas_call(
        grid_kernel,
        out_shape=(
            V((3, COLS, NZ), f32), V((COLS, NZ), f32), V((COLS, 2 * NZ), jnp.bfloat16), V((3, 2 * SLOTS, NZ), f32),
        ),
        in_specs=[hbm] * 8 + [pl.BlockSpec(memory_space=pltpu.SMEM)],
        out_specs=(vmem,) * 4,
        scratch_shapes=[
            V((4, COLS + TILE, NZ), f32), V((4, COLS + TILE, NZ), f32), V((16 + TILE, NZ), f32),
            pltpu.SMEM((3, 32), i32), pltpu.SMEM((32,), i32),
            V((CODES, 24, NZ), f32), V((CODES, 24, NZ), f32), V((7, 24, NZ), f32), V((CODES, 24, NZ), f32),
            V((CODES, 16, NZ), f32), V((CODES, 16, NZ), f32),
            V((2, 5, NX, NZ), f32), V((2, 5, NY, NZ), f32), V((2, 5, NX, NZ), f32),
            V((3, NY, NZ), f32), V((BLOCK, 3, TILE + NY, NZ), f32),
            pltpu.SemaphoreType.DMA((5,)), pltpu.SemaphoreType.DMA((2,)), pltpu.SemaphoreType.DMA((5,)),
            pltpu.SemaphoreType.DMA((7,)), pltpu.SemaphoreType.DMA((1,)),
            pltpu.SemaphoreType.DMA((4,)), pltpu.SemaphoreType.DMA((4,)), pltpu.SemaphoreType.REGULAR((3,)),
        ],
        compiler_params=pltpu.CompilerParams(collective_id=0, has_side_effects=True, vmem_limit_bytes=24 * 2**20),
        name="grid",
    )(
        *(
            pltpu.with_memory_space_constraint(x, pltpu.HBM)
            for x in (
                pressure.reshape(COLS, NZ), depth.reshape(COLS, NZ), saturation.reshape(2, COLS, NZ),
                permeability.reshape(3, COLS, NZ), pore_volume.reshape(COLS, NZ),
                fault_pairs.T, fault_kind, fault_table,
            )
        ),
        fault_count,
    )
    out = pl.pallas_call(
        add_kernel,
        out_shape=jax.ShapeDtypeStruct((3, COLS, NZ), f32),
        in_specs=[vmem] * 4,
        out_specs=hbm,
        scratch_shapes=[V((2 * NZ, 3 * NZ), jnp.bfloat16), V((3, COLS, NZ), f32), pltpu.SemaphoreType.DMA],
        compiler_params=pltpu.CompilerParams(vmem_limit_bytes=16 * 2**20),
        name="add",
    )(acc, wgt, hot, rows)
    return out.reshape(3, NX, NY, NZ)


def solution(mesh):
    in_specs = (
        P("gx", "gy", None),
        P("gx", "gy", None),
        P(None, "gx", "gy", None),
        P(None, "gx", "gy", None),
        P("gx", "gy", None),
        P(("gx", "gy"), None),
        P(("gx", "gy")),
        P(("gx", "gy")),
        P(),
    )
    out_specs = P(None, "gx", "gy", None)
    return jax.shard_map(body, mesh=mesh, in_specs=in_specs, out_specs=out_specs, check_vma=False)
```

```python
import jax
import jax.numpy as jnp
from jax import lax
from jax.experimental import pallas as pl
from jax.experimental.pallas import tpu as pltpu
from jax.sharding import PartitionSpec as P

CAP = 4
CODES = 9
HERE = 4
SLOTS = 40
RHO = (1.0, 0.8, 0.25)
STEP = 0.2
NX = 32
NY = 32
NZ = 128
COLS = NX * NY
TILE = 8
LINE = 4
BLOCK = 2
RELAY_AT = 6
MESH = pl.DeviceIdType.MESH


def mobility(sw, so):
    sg = 1.0 - sw - so
    return (sw * sw * 2.0, so * so, sg * sg * 4.0)


def harmonic(a, b):
    return 2.0 * a * b / (a + b)


def fluxes(pa, da, ma, pb, db, mb, trans):
    dp = pa - pb
    dd = da - db
    out = []
    for f in range(3):
        drive = dp - (dd if RHO[f] == 1.0 else RHO[f] * dd)
        out.append(trans * jnp.where(drive > 0.0, ma[f], mb[f]) * drive)
    return out


def grid_kernel(
    press, depth, sat, perm, pore, pairs, kind, table, CT,
    acc, wgt, hot, rows,
    X, K, TAB, PR, KD,
    sreq, rreq, lreq, loc, sresp, rresp,
    ysend, hx, hy, fxs, fys,
    lsem, ssem, rsem, qsem, psem, hsend, hrecv, open_,
):
    P_, D_, W_, O_ = (X.at[q] for q in range(4))
    KX, KY, KZ, PV = (K.at[q] for q in range(4))
    cols = pl.ds(0, COLS)
    ix = lax.axis_index("gx")
    iy = lax.axis_index("gy")
    nx = lax.axis_size("gx")
    ny = lax.axis_size("gy")

    def device(dx, dy):
        return (lax.rem(ix + (dx + nx), nx), lax.rem(iy + (dy + ny), ny))

    offsets = [(dx, dy) for dx in (-1, 0, 1) for dy in (-1, 0, 1)]
    barrier = pltpu.get_barrier_semaphore()
    iz = lax.rem(ix, LINE)
    first = iz == 0
    second = iz == 1
    last = iz == LINE - 1

    odd = lax.rem(iy, 2) == 1

    def greet(dx, dy):
        pl.semaphore_signal(barrier, inc=1, device_id=device(dx, dy), device_id_type=MESH)

    top = iy == ny - 1
    bottom = iy == 0
    @pl.when(jnp.logical_and(first, odd))
    def _():
        for dy in (-2, -1, 0):
            greet(LINE, dy)

    @pl.when(jnp.logical_and(jnp.logical_and(first, odd), iy < ny - 1))
    def _():
        greet(LINE, 1)

    for dx in (-1, 0, 1):
        ahead = (second, first, last)[dx + 1]
        for dy in (-1, 0, 1):
            if (dx, dy) == (0, 0):
                continue
            if dx:
                meets = jnp.logical_not(ahead)
                if dy == 1:
                    meets = jnp.logical_and(meets, jnp.logical_or(first, jnp.logical_not(top)))
            elif dy == 1:
                meets = jnp.logical_or(ahead, jnp.logical_not(top))
            else:
                meets = None
            if meets is None:
                greet(dx, dy)
            else:
                @pl.when(meets)
                def _(dx=dx, dy=dy):
                    greet(dx, dy)

    @pl.when(jnp.logical_and(first, odd))
    def _():
        for dy in (-1, 0):
            greet(LINE - 1, dy)

    loads = [
        pltpu.make_async_copy(src, dst, lsem.at[n])
        for n, src, dst in (
            (0, pairs, PR), (1, kind, KD),
            (2, press, X.at[0, cols]), (2, depth, X.at[1, cols]), (2, sat, X.at[pl.ds(2, 2), cols]),
            (3, table, TAB.at[pl.ds(0, 16)]), (4, perm, K.at[pl.ds(0, 3), cols]), (4, pore, K.at[3, cols]),
        )
    ]
    for copy in loads:
        copy.start()
    state = pltpu.make_async_copy(X.at[:, cols], X.at[:, cols], lsem.at[2])

    zero = jnp.zeros((TILE, NZ), jnp.float32)
    for q in range(4):
        X[q, pl.ds(COLS, TILE), :] = zero
    K[1, pl.ds(COLS, TILE), :] = zero
    for f in range(3):
        for t in range(4):
            fxs[f, pl.ds(TILE * t, TILE), :] = zero
        for k in range(BLOCK):
            fys[k, f, pl.ds(0, TILE), :] = zero
        rows[f, pl.ds(32, TILE), :] = zero
        rows[f, pl.ds(SLOTS + 32, TILE), :] = zero

    @pl.when(last)
    def _():
        pl.semaphore_wait(barrier, jnp.where(bottom, 7, 9))

    for own_odd in (False, True):
        @pl.when(jnp.logical_and(last, odd if own_odd else jnp.logical_not(odd)))
        def _(own_odd=own_odd):
            pl.semaphore_signal(
                open_.at[0 if own_odd else 1], inc=1, device_id=device(1 - LINE, 0 if own_odd else 1),
                device_id_type=MESH,
            )

    for n in range(2):
        loads[n].wait()
    live = CT[0]
    log_y = ny.bit_length() - 1
    used = jnp.int32(0)
    words = [jnp.int32(0)] * CODES
    for r in range(32):
        target = PR[1, r]
        cx = ((target >> log_y) - ix + 1) & (nx - 1)
        cy = ((target & (ny - 1)) - iy + 1) & (ny - 1)
        code = cx * 3 + cy
        rank = (used >> (code * 3)) & 7
        on = jnp.where(r < live, 1, 0)
        used = used + (on << (code * 3))
        entry = ((r + 32) * on) << (rank * 6)
        for c in range(CODES):
            words[c] = words[c] + jnp.where(code == c, entry, 0)

    state.wait()
    loads[5].wait()
    lane = lax.broadcasted_iota(jnp.int32, (1, NZ), 1)
    idx0 = jnp.full((1, NZ), -1, jnp.int32)
    idx1 = jnp.full((1, NZ), -1, jnp.int32)

    def place(idx0, idx1, k, value):
        for copy in range(3):
            at = 2 * SLOTS * copy + k
            if at < NZ:
                idx0 = jnp.where(lane == at, value, idx0)
            else:
                idx1 = jnp.where(lane == at - NZ, value, idx1)
        return idx0, idx1

    for c in range(CODES):
        for s in range(CAP):
            entry = words[c] >> (6 * s)
            r = entry & 31
            full = jnp.where((entry & 32) > 0, 1.0, 0.0)
            src = PR[0, r]
            land = PR[2, r]
            kd = KD[r]
            for q, ref in enumerate((P_, D_, W_, O_)):
                sreq[c, pl.ds(4 * q + s, 1), :] = ref[pl.ds(src, 1), :]
            sreq[c, pl.ds(16 + s, 1), :] = TAB[pl.ds(kd, 1), :] * full
            sreq[c, pl.ds(20 + s, 1), :] = jnp.full((1, NZ), land, jnp.int32).astype(jnp.float32)
            idx0, idx1 = place(idx0, idx1, c * CAP + s, src)

    @pl.when(jnp.logical_not(last))
    def _():
        pl.semaphore_wait(barrier, jnp.where(first, jnp.where(bottom, 3, 4), jnp.where(bottom, jnp.where(second, 6, 5), 8)))

    def request(c, target):
        return pltpu.make_async_remote_copy(
            src_ref=sreq.at[c], dst_ref=rreq.at[c], send_sem=ssem.at[0], recv_sem=rsem.at[min(c, 3)],
            device_id=target, device_id_type=MESH,
        )

    def to_relay(c, to_odd):
        dx, dy = offsets[c]
        k = c if to_odd else 3 + c
        return pltpu.make_async_remote_copy(
            src_ref=sreq.at[c], dst_ref=lreq.at[k], send_sem=ssem.at[0], recv_sem=qsem.at[k],
            device_id=device(-LINE, dy if to_odd else dy + 1), device_id_type=MESH,
        )

    to_side = pltpu.make_async_remote_copy(
        src_ref=sreq.at[0], dst_ref=lreq.at[6], send_sem=ssem.at[0], recv_sem=qsem.at[6],
        device_id=device(0, -1), device_id_type=MESH,
    )
    from_side = pltpu.make_async_remote_copy(
        src_ref=lreq.at[6], dst_ref=lreq.at[0], send_sem=psem.at[0], recv_sem=qsem.at[0],
        device_id=device(-LINE, 0), device_id_type=MESH,
    )

    for own_odd in (False, True):
        @pl.when(jnp.logical_and(first, odd if own_odd else jnp.logical_not(odd)))
        def _(own_odd=own_odd):
            for c in (0, 2, 1):
                if c == 0 and not own_odd:
                    @pl.when(iy > 0)
                    def _():
                        to_relay(0, True).start()

                    @pl.when(iy == 0)
                    def _():
                        to_side.start()
                else:
                    to_relay(c, own_odd == (c == 1)).start()

    @pl.when(first)
    def _():
        for c in (3, 5):
            request(c, device(*offsets[c])).start()

    @pl.when(jnp.logical_and(jnp.logical_not(first), jnp.logical_not(bottom)))
    def _():
        for c in (6, 8, 0, 2, 3, 5, 7, 1):
            request(c, device(*offsets[c])).start()

    wraps = jnp.logical_and(jnp.logical_not(first), bottom)

    @pl.when(wraps)
    def _():
        for c in (8, 2, 5, 7, 1):
            request(c, device(*offsets[c])).start()

    for c, known in ((0, second), (6, last)):
        @pl.when(jnp.logical_and(bottom, known))
        def _(c=c):
            request(c, device(*offsets[c])).start()

    @pl.when(second)
    def _():
        for dy in (-1, 0, 1):
            pl.semaphore_signal(open_.at[2], inc=1, device_id=device(-1, dy), device_id_type=MESH)

    for dx in (-1, 0, 1):
        @pl.when(jnp.logical_and(jnp.logical_and(top, jnp.logical_not(first)), jnp.logical_not((second, first, last)[dx + 1])))
        def _(dx=dx):
            pl.semaphore_signal(open_.at[2], inc=1, device_id=device(dx, 1), device_id_type=MESH)

    eight = pl.ds(0, 8)
    requests = pltpu.make_async_remote_copy(
        src_ref=sreq.at[eight], dst_ref=rreq.at[eight], send_sem=ssem.at[0], recv_sem=rsem.at[0],
        device_id=device(0, 1), device_id_type=MESH,
    )

    for side, y in ((0, NY - 1), (1, 0)):
        for q, ref in enumerate((P_, D_, W_, O_)):
            ysend[side, q] = ref[pl.ds(y, NX, NY), :]
    pltpu.make_async_copy(K.at[:, cols], K.at[:, cols], lsem.at[4]).wait()
    for side, y in ((0, NY - 1), (1, 0)):
        ysend[side, 4] = KY[pl.ds(y, NX, NY), :]

    def halo(src, dst, n, dx, dy):
        return pltpu.make_async_remote_copy(
            src_ref=src, dst_ref=dst, send_sem=hsend.at[0], recv_sem=hrecv.at[n],
            device_id=device(dx, dy), device_id_type=MESH,
        )

    halos_x = []
    for side, (dx, x) in enumerate(((1, NX - 1), (-1, 0))):
        row = pl.ds(x * NY, NY)
        halos_x.append([
            halo(X.at[:, row], hx.at[side, pl.ds(0, 4)], side, dx, 0),
            halo(K.at[0, row], hx.at[side, 4], side, dx, 0),
        ])
    whole_x = [halo(hx.at[side], hx.at[side], side, dx, 0) for side, dx in enumerate((1, -1))]
    halos_y = [halo(ysend.at[side], hy.at[side], 2 + side, 0, dy) for side, dy in enumerate((1, -1))]
    goes = (ix < nx - 1, ix > 0, iy < ny - 1, iy > 0)
    comes = (goes[1], goes[0], goes[3], goes[2])

    @pl.when(jnp.logical_and(goes[0], jnp.logical_not(first)))
    def _():
        for copy in halos_x[0]:
            copy.start()

    @pl.when(jnp.logical_not(first))
    def _():
        for copy in halos_x[1]:
            copy.start()

    for side in range(2):
        @pl.when(goes[2 + side])
        def _(side=side):
            halos_y[side].start()

    lanes = lax.broadcasted_iota(jnp.int32, (TILE, NZ), 1)
    sublanes = lax.broadcasted_iota(jnp.int32, (TILE, NZ), 0)
    last_lane = lanes == NZ - 1
    last_sub = sublanes == TILE - 1

    def block(b, carry):
        for t in range(4):
            base = b * (BLOCK * NY) + TILE * t
            at = pl.ds(pl.multiple_of(base, TILE), TILE)
            p, d, w, o, kx = P_[at, :], D_[at, :], W_[at, :], O_[at, :], KX[at, :]
            m = mobility(w, o)
            fx = [fxs[f, pl.ds(TILE * t, TILE), :] for f in range(3)]
            for k in range(BLOCK):
                row = b * BLOCK + k
                at = pl.ds(pl.multiple_of(base + k * NY, TILE), TILE)
                nrow = jnp.minimum(row + 1, NX - 1)
                nat = pl.ds(pl.multiple_of(nrow * NY + TILE * t, TILE), TILE)
                pn, dn, wn, on, kn = P_[nat, :], D_[nat, :], W_[nat, :], O_[nat, :], KX[nat, :]
                mn = mobility(wn, on)
                inside = jnp.where(row < NX - 1, 2.0, 0.0)
                gx = fluxes(p, d, m, pn, dn, mn, inside * kx * kn / (kx + kn))
                net = [gx[f] - fx[f] for f in range(3)]
                uat = pl.ds(base + k * NY + 1, TILE)
                ky, ku = KY[at, :], KY[uat, :]
                gy = fluxes(p, d, m, P_[uat, :], D_[uat, :], mobility(W_[uat, :], O_[uat, :]), harmonic(ky, ku))
                for f in range(3):
                    g = jnp.where(last_sub, 0.0, gy[f]) if t == 3 else gy[f]
                    fys[k, f, pl.ds(TILE + TILE * t, TILE), :] = g
                    net[f] = net[f] + (g - fys[k, f, pl.ds(TILE + TILE * t - 1, TILE), :])
                kz = KZ[at, :]
                up = lambda v: pltpu.roll(v, NZ - 1, 1)
                tz = jnp.where(last_lane, 0.0, harmonic(kz, up(kz)))
                gz = fluxes(p, d, m, up(p), up(d), [up(v) for v in m], tz)
                wt = STEP / PV[at, :]
                wgt[at, :] = wt
                sats = (w, o, 1.0 - w - o)
                for f in range(3):
                    total = net[f] + (gz[f] - pltpu.roll(gz[f], 1, 1))
                    acc[f, at, :] = sats[f] - wt * total
                p, d, w, o, kx, m, fx = pn, dn, wn, on, kn, mn, gx
            for f in range(3):
                fxs[f, pl.ds(TILE * t, TILE), :] = fx[f]
        return carry

    blocks = NX // BLOCK
    early = jnp.where(first, jnp.where(odd, RELAY_AT, blocks), jnp.where(last, blocks // 2 - 2, blocks // 2))
    lax.fori_loop(0, early, block, 0)

    def relayed(n):
        part = pl.ds(0, n)
        return pltpu.make_async_remote_copy(
            src_ref=lreq.at[part], dst_ref=rreq.at[part], send_sem=psem.at[0], recv_sem=rsem.at[0],
            device_id=device(LINE - 1, 0), device_id_type=MESH,
        )

    beside = jnp.logical_and(first, iy == ny - 1)

    @pl.when(beside)
    def _():
        to_side.wait_recv()
        from_side.start()

    @pl.when(jnp.logical_and(first, odd))
    def _():
        for k in (3, 5, 1, 4, 2, 0):
            c = k % 3
            if k in (3, 1):
                pl.semaphore_wait(open_.at[k // 3], 1)
            to_relay(c, k < 3).wait_recv()
            pltpu.make_async_remote_copy(
                src_ref=lreq.at[k], dst_ref=rreq.at[c], send_sem=psem.at[0], recv_sem=rsem.at[c],
                device_id=device(LINE - 1, 0 if k < 3 else -1), device_id_type=MESH,
            ).start()

    @pl.when(first)
    def _():
        pl.semaphore_wait(open_.at[2], 3)
        for c in (6, 8, 7):
            request(c, device(*offsets[c])).start()
        for copy in halos_x[0]:
            copy.start()

    @pl.when(wraps)
    def _():
        pl.semaphore_wait(open_.at[2], jnp.where(jnp.logical_or(second, last), 2, 3))

    for c, known in ((6, last), (3, first), (0, second)):
        @pl.when(jnp.logical_and(wraps, jnp.logical_not(known)))
        def _(c=c):
            request(c, device(*offsets[c])).start()

    middle = jnp.where(first, blocks, early)
    lax.fori_loop(early, middle, block, 0)

    lands = {}

    def answer(codes):
        for n, c in codes:
            ref = sreq if n == HERE else rreq
            for s in range(CAP):
                lands[n, s] = jnp.clip(ref[c, pl.ds(20 + s, 1), :].astype(jnp.int32), 0, COLS - 1)[0, 0]
        for n, c in codes:
            for s in range(CAP):
                for q, ref in enumerate((P_, D_, W_, O_)):
                    loc[n, pl.ds(4 * q + s, 1), :] = ref[pl.ds(lands[n, s], 1), :]
        for n, c in codes:
            ref = sreq if n == HERE else rreq
            a = [ref[c, pl.ds(4 * q, 4), :] for q in range(5)]
            b = [loc[n, pl.ds(4 * q, 4), :] for q in range(4)]
            flow = fluxes(a[0], a[1], mobility(a[2], a[3]), b[0], b[1], mobility(b[2], b[3]), a[4])
            for f in range(3):
                sresp[c, pl.ds(4 * f, 4), :] = flow[f]
                rows[f, pl.ds(SLOTS + 4 * n, 4), :] = -flow[f]
                if n == HERE:
                    rows[f, pl.ds(4 * n, 4), :] = flow[f]
            sresp[c, pl.ds(12, 4), :] = jnp.zeros((4, NZ), jnp.float32)
            if n == HERE:
                continue
            pltpu.make_async_remote_copy(
                src_ref=sresp.at[c], dst_ref=rresp.at[c], send_sem=ssem.at[1], recv_sem=rsem.at[4],
                device_id=device(1, 1 - c) if n < 3 else device(-offsets[c][0], -offsets[c][1]),
                device_id_type=MESH,
            ).start()

    for n, c in ((0, jnp.where(odd, 1, 0)), (1, 2), (2, jnp.where(odd, 0, 1))):
        pltpu.make_async_remote_copy(
            src_ref=sreq.at[c], dst_ref=rreq.at[c], send_sem=ssem.at[0], recv_sem=rsem.at[c],
            device_id=device(0, 1), device_id_type=MESH,
        ).wait_recv()
        answer([(n, c)])
    five = pl.ds(3, 5)
    pltpu.make_async_remote_copy(
        src_ref=sreq.at[five], dst_ref=rreq.at[five], send_sem=ssem.at[0], recv_sem=rsem.at[3],
        device_id=device(0, 1), device_id_type=MESH,
    ).wait_recv()
    answer([(c, c) for c in (6, 8, 3, 5, 7, HERE)])
    answers = pltpu.make_async_remote_copy(
        src_ref=sresp.at[eight], dst_ref=rresp.at[eight], send_sem=ssem.at[1], recv_sem=rsem.at[4],
        device_id=device(0, 1), device_id_type=MESH,
    )

    @pl.when(jnp.logical_and(first, goes[1]))
    def _():
        for copy in halos_x[1]:
            copy.start()

    for c in range(CODES):
        for s in range(CAP):
            idx0, idx1 = place(idx0, idx1, SLOTS + c * CAP + s, lands[c, s])

    lax.fori_loop(middle, blocks, block, 0)

    def face(axis, side):
        far = [(hy if axis else hx)[side, q] for q in range(5)]
        if axis:
            at = pl.ds((NY - 1) if side else 0, NX, NY)
        else:
            at = pl.ds((NX - 1) * NY if side else 0, NY)
        near = [ref[at, :] for ref in (P_, D_, W_, O_, KY if axis else KX)]
        lo, hi = (near, far) if side else (far, near)
        flow = fluxes(
            lo[0], lo[1], mobility(lo[2], lo[3]), hi[0], hi[1], mobility(hi[2], hi[3]), harmonic(lo[4], hi[4])
        )
        wt = wgt[at, :]
        for f in range(3):
            step = wt * flow[f]
            acc[f, at, :] = acc[f, at, :] + (-step if side else step)

    for axis in range(2):
        for side in range(2):
            @pl.when(comes[2 * axis + side])
            def _(axis=axis, side=side):
                if axis:
                    halos_y[side].wait_recv()
                else:
                    whole_x[side].wait_recv()
                face(axis, side)

    idx = jnp.concatenate([idx0, idx1], axis=1)
    cell = lax.broadcasted_iota(jnp.int32, (32, 2 * NZ), 0)

    def mark(b, carry):
        start = pl.multiple_of(b * 32, 32)
        hot[pl.ds(start, 32), :] = jnp.where(cell + start == idx, 1.0, 0.0).astype(jnp.bfloat16)
        return carry

    lax.fori_loop(0, COLS // 32, mark, 0)

    answers.wait_recv()
    for c in range(CODES):
        if c != HERE:
            for f in range(3):
                rows[f, pl.ds(4 * c, 4), :] = rresp[c, pl.ds(4 * f, 4), :]
    requests.wait_send()
    answers.wait_send()
    for side in range(2):
        @pl.when(goes[side])
        def _(side=side):
            whole_x[side].wait_send()

        @pl.when(goes[2 + side])
        def _(side=side):
            halos_y[side].wait_send()

    @pl.when(jnp.logical_and(jnp.logical_and(first, odd), jnp.logical_not(top)))
    def _():
        relayed(6).wait_send()

    @pl.when(beside)
    def _():
        relayed(7).wait_send()


def add_kernel(acc, wgt, hot, rows, out, parts, held, sem):
    for f in range(3):
        value = rows[f]
        for k in range(3):
            part = value.astype(jnp.bfloat16)
            parts[pl.ds(2 * SLOTS * k, 2 * SLOTS), pl.ds(NZ * f, NZ)] = part
            value = value - part.astype(jnp.float32)
        parts[pl.ds(240, 16), pl.ds(NZ * f, NZ)] = jnp.zeros((16, NZ), jnp.bfloat16)
    size = COLS // 8
    for n in range(8):
        at = pl.ds(n * size, size)
        delta = jnp.dot(hot[at, :], parts[...], preferred_element_type=jnp.float32)
        wt = wgt[at, :]
        for f in range(3):
            held[f, at, :] = acc[f, at, :] - wt * delta[:, NZ * f:NZ * (f + 1)]
            pltpu.make_async_copy(held.at[f, at], out.at[f, at], sem).start()
    pltpu.make_async_copy(held, out, sem).wait()


def body(pressure, depth, saturation, permeability, pore_volume, fault_pairs, fault_kind, fault_count, fault_table):
    f32, i32 = jnp.float32, jnp.int32
    hbm = pl.BlockSpec(memory_space=pltpu.HBM)
    vmem = pl.BlockSpec(memory_space=pltpu.VMEM)
    V = pltpu.VMEM
    acc, wgt, hot, rows = pl.pallas_call(
        grid_kernel,
        out_shape=(
            V((3, COLS, NZ), f32), V((COLS, NZ), f32), V((COLS, 2 * NZ), jnp.bfloat16), V((3, 2 * SLOTS, NZ), f32),
        ),
        in_specs=[hbm] * 8 + [pl.BlockSpec(memory_space=pltpu.SMEM)],
        out_specs=(vmem,) * 4,
        scratch_shapes=[
            V((4, COLS + TILE, NZ), f32), V((4, COLS + TILE, NZ), f32), V((16 + TILE, NZ), f32),
            pltpu.SMEM((3, 32), i32), pltpu.SMEM((32,), i32),
            V((CODES, 24, NZ), f32), V((CODES, 24, NZ), f32), V((7, 24, NZ), f32), V((CODES, 24, NZ), f32),
            V((CODES, 16, NZ), f32), V((CODES, 16, NZ), f32),
            V((2, 5, NX, NZ), f32), V((2, 5, NY, NZ), f32), V((2, 5, NX, NZ), f32),
            V((3, NY, NZ), f32), V((BLOCK, 3, TILE + NY, NZ), f32),
            pltpu.SemaphoreType.DMA((5,)), pltpu.SemaphoreType.DMA((2,)), pltpu.SemaphoreType.DMA((5,)),
            pltpu.SemaphoreType.DMA((7,)), pltpu.SemaphoreType.DMA((1,)),
            pltpu.SemaphoreType.DMA((1,)), pltpu.SemaphoreType.DMA((4,)), pltpu.SemaphoreType.REGULAR((3,)),
        ],
        compiler_params=pltpu.CompilerParams(collective_id=0, has_side_effects=True, vmem_limit_bytes=24 * 2**20),
        name="grid",
    )(
        *(
            pltpu.with_memory_space_constraint(x, pltpu.HBM)
            for x in (
                pressure.reshape(COLS, NZ), depth.reshape(COLS, NZ), saturation.reshape(2, COLS, NZ),
                permeability.reshape(3, COLS, NZ), pore_volume.reshape(COLS, NZ),
                fault_pairs.T, fault_kind, fault_table,
            )
        ),
        fault_count,
    )
    out = pl.pallas_call(
        add_kernel,
        out_shape=jax.ShapeDtypeStruct((3, COLS, NZ), f32),
        in_specs=[vmem] * 4,
        out_specs=hbm,
        scratch_shapes=[V((2 * NZ, 3 * NZ), jnp.bfloat16), V((3, COLS, NZ), f32), pltpu.SemaphoreType.DMA],
        compiler_params=pltpu.CompilerParams(vmem_limit_bytes=16 * 2**20),
        name="add",
    )(acc, wgt, hot, rows)
    return out.reshape(3, NX, NY, NZ)


def solution(mesh):
    in_specs = (
        P("gx", "gy", None),
        P("gx", "gy", None),
        P(None, "gx", "gy", None),
        P(None, "gx", "gy", None),
        P("gx", "gy", None),
        P(("gx", "gy"), None),
        P(("gx", "gy")),
        P(("gx", "gy")),
        P(),
    )
    out_specs = P(None, "gx", "gy", None)
    return jax.shard_map(body, mesh=mesh, in_specs=in_specs, out_specs=out_specs, check_vma=False)
```

```python
import jax
import jax.numpy as jnp
from jax import lax
from jax.experimental import pallas as pl
from jax.experimental.pallas import tpu as pltpu
from jax.sharding import PartitionSpec as P

CAP = 4
CODES = 9
HERE = 4
SLOTS = 40
RHO = (1.0, 0.8, 0.25)
STEP = 0.2
NX = 32
NY = 32
NZ = 128
COLS = NX * NY
TILE = 8
LINE = 4
BLOCK = 2
RELAY_AT = 6
MESH = pl.DeviceIdType.MESH


def mobility(sw, so):
    sg = 1.0 - sw - so
    return (sw * sw * 2.0, so * so, sg * sg * 4.0)


def harmonic(a, b):
    return 2.0 * a * b / (a + b)


def fluxes(pa, da, ma, pb, db, mb, trans):
    dp = pa - pb
    dd = da - db
    out = []
    for f in range(3):
        drive = dp - (dd if RHO[f] == 1.0 else RHO[f] * dd)
        out.append(trans * jnp.where(drive > 0.0, ma[f], mb[f]) * drive)
    return out


def grid_kernel(
    press, depth, sat, perm, pore, pairs, kind, table, CT,
    acc, wgt, hot, rows,
    X, K, TAB, PR, KD,
    sreq, rreq, lreq, loc, sresp, rresp,
    ysend, hx, hy, fxs, fys,
    lsem, ssem, rsem, qsem, psem, hsend, hrecv, open_,
):
    P_, D_, W_, O_ = (X.at[q] for q in range(4))
    KX, KY, KZ, PV = (K.at[q] for q in range(4))
    cols = pl.ds(0, COLS)
    ix = lax.axis_index("gx")
    iy = lax.axis_index("gy")
    nx = lax.axis_size("gx")
    ny = lax.axis_size("gy")

    def device(dx, dy):
        return (lax.rem(ix + (dx + nx), nx), lax.rem(iy + (dy + ny), ny))

    offsets = [(dx, dy) for dx in (-1, 0, 1) for dy in (-1, 0, 1)]
    barrier = pltpu.get_barrier_semaphore()
    iz = lax.rem(ix, LINE)
    first = iz == 0
    second = iz == 1
    last = iz == LINE - 1

    odd = lax.rem(iy, 2) == 1

    def greet(dx, dy):
        pl.semaphore_signal(barrier, inc=1, device_id=device(dx, dy), device_id_type=MESH)

    top = iy == ny - 1
    bottom = iy == 0
    @pl.when(jnp.logical_and(first, odd))
    def _():
        for dy in (-2, -1, 0):
            greet(LINE, dy)

    @pl.when(jnp.logical_and(jnp.logical_and(first, odd), iy < ny - 1))
    def _():
        greet(LINE, 1)

    for dx in (-1, 0, 1):
        ahead = (second, first, last)[dx + 1]
        for dy in (-1, 0, 1):
            if (dx, dy) == (0, 0):
                continue
            if dx:
                meets = jnp.logical_not(ahead)
                if dy == 1:
                    meets = jnp.logical_and(meets, jnp.logical_or(first, jnp.logical_not(top)))
            elif dy == 1:
                meets = jnp.logical_or(ahead, jnp.logical_not(top))
            else:
                meets = None
            if meets is None:
                greet(dx, dy)
            else:
                @pl.when(meets)
                def _(dx=dx, dy=dy):
                    greet(dx, dy)

    @pl.when(jnp.logical_and(first, odd))
    def _():
        for dy in (-1, 0):
            greet(LINE - 1, dy)

    loads = [
        pltpu.make_async_copy(src, dst, lsem.at[n])
        for n, src, dst in (
            (0, pairs, PR), (1, kind, KD),
            (2, press, X.at[0, cols]), (2, depth, X.at[1, cols]), (2, sat, X.at[pl.ds(2, 2), cols]),
            (3, table, TAB.at[pl.ds(0, 16)]), (4, perm, K.at[pl.ds(0, 3), cols]), (4, pore, K.at[3, cols]),
        )
    ]
    for copy in loads:
        copy.start()
    state = pltpu.make_async_copy(X.at[:, cols], X.at[:, cols], lsem.at[2])

    zero = jnp.zeros((TILE, NZ), jnp.float32)
    for q in range(4):
        X[q, pl.ds(COLS, TILE), :] = zero
    K[1, pl.ds(COLS, TILE), :] = zero
    for f in range(3):
        for t in range(4):
            fxs[f, pl.ds(TILE * t, TILE), :] = zero
        for k in range(BLOCK):
            fys[k, f, pl.ds(0, TILE), :] = zero
        rows[f, pl.ds(32, TILE), :] = zero
        rows[f, pl.ds(SLOTS + 32, TILE), :] = zero

    @pl.when(last)
    def _():
        pl.semaphore_wait(barrier, jnp.where(bottom, 7, 9))

    for own_odd in (False, True):
        @pl.when(jnp.logical_and(last, odd if own_odd else jnp.logical_not(odd)))
        def _(own_odd=own_odd):
            pl.semaphore_signal(
                open_.at[0 if own_odd else 1], inc=1, device_id=device(1 - LINE, 0 if own_odd else 1),
                device_id_type=MESH,
            )

    for n in range(2):
        loads[n].wait()
    live = CT[0]
    log_y = ny.bit_length() - 1
    used = jnp.int32(0)
    words = [jnp.int32(0)] * CODES
    for r in range(32):
        target = PR[1, r]
        cx = ((target >> log_y) - ix + 1) & (nx - 1)
        cy = ((target & (ny - 1)) - iy + 1) & (ny - 1)
        code = cx * 3 + cy
        rank = (used >> (code * 3)) & 7
        on = jnp.where(r < live, 1, 0)
        used = used + (on << (code * 3))
        entry = ((r + 32) * on) << (rank * 6)
        for c in range(CODES):
            words[c] = words[c] + jnp.where(code == c, entry, 0)

    state.wait()
    loads[5].wait()
    lane = lax.broadcasted_iota(jnp.int32, (1, NZ), 1)
    idx0 = jnp.full((1, NZ), -1, jnp.int32)
    idx1 = jnp.full((1, NZ), -1, jnp.int32)

    def place(idx0, idx1, k, value):
        for copy in range(3):
            at = 2 * SLOTS * copy + k
            if at < NZ:
                idx0 = jnp.where(lane == at, value, idx0)
            else:
                idx1 = jnp.where(lane == at - NZ, value, idx1)
        return idx0, idx1

    for c in range(CODES):
        for s in range(CAP):
            entry = words[c] >> (6 * s)
            r = entry & 31
            full = jnp.where((entry & 32) > 0, 1.0, 0.0)
            src = PR[0, r]
            land = PR[2, r]
            kd = KD[r]
            for q, ref in enumerate((P_, D_, W_, O_)):
                sreq[c, pl.ds(4 * q + s, 1), :] = ref[pl.ds(src, 1), :]
            sreq[c, pl.ds(16 + s, 1), :] = TAB[pl.ds(kd, 1), :] * full
            sreq[c, pl.ds(20 + s, 1), :] = jnp.full((1, NZ), land, jnp.int32).astype(jnp.float32)
            idx0, idx1 = place(idx0, idx1, c * CAP + s, src)

    @pl.when(jnp.logical_not(last))
    def _():
        pl.semaphore_wait(barrier, jnp.where(first, jnp.where(bottom, 3, 4), jnp.where(bottom, jnp.where(second, 6, 5), 8)))

    def request(c, target):
        return pltpu.make_async_remote_copy(
            src_ref=sreq.at[c], dst_ref=rreq.at[c], send_sem=ssem.at[0], recv_sem=rsem.at[min(c, 3)],
            device_id=target, device_id_type=MESH,
        )

    def to_relay(c, to_odd):
        dx, dy = offsets[c]
        k = c if to_odd else 3 + c
        return pltpu.make_async_remote_copy(
            src_ref=sreq.at[c], dst_ref=lreq.at[k], send_sem=ssem.at[0], recv_sem=qsem.at[k],
            device_id=device(-LINE, dy if to_odd else dy + 1), device_id_type=MESH,
        )

    to_side = pltpu.make_async_remote_copy(
        src_ref=sreq.at[0], dst_ref=lreq.at[6], send_sem=ssem.at[0], recv_sem=qsem.at[6],
        device_id=device(0, -1), device_id_type=MESH,
    )
    from_side = pltpu.make_async_remote_copy(
        src_ref=lreq.at[6], dst_ref=lreq.at[0], send_sem=psem.at[0], recv_sem=qsem.at[0],
        device_id=device(-LINE, 0), device_id_type=MESH,
    )

    for own_odd in (False, True):
        @pl.when(jnp.logical_and(first, odd if own_odd else jnp.logical_not(odd)))
        def _(own_odd=own_odd):
            for c in (0, 2, 1):
                if c == 0 and not own_odd:
                    @pl.when(iy > 0)
                    def _():
                        to_relay(0, True).start()

                    @pl.when(iy == 0)
                    def _():
                        to_side.start()
                else:
                    to_relay(c, own_odd == (c == 1)).start()

    @pl.when(first)
    def _():
        for c in (3, 5):
            request(c, device(*offsets[c])).start()

    @pl.when(jnp.logical_and(jnp.logical_not(first), jnp.logical_not(bottom)))
    def _():
        for c in (6, 8, 0, 2, 3, 5, 7, 1):
            request(c, device(*offsets[c])).start()

    wraps = jnp.logical_and(jnp.logical_not(first), bottom)

    @pl.when(wraps)
    def _():
        for c in (8, 2, 5, 7, 1):
            request(c, device(*offsets[c])).start()

    for c, known in ((0, second), (6, last)):
        @pl.when(jnp.logical_and(bottom, known))
        def _(c=c):
            request(c, device(*offsets[c])).start()

    @pl.when(second)
    def _():
        for dy in (-1, 0, 1):
            pl.semaphore_signal(open_.at[2], inc=1, device_id=device(-1, dy), device_id_type=MESH)

    for dx in (-1, 0, 1):
        @pl.when(jnp.logical_and(jnp.logical_and(top, jnp.logical_not(first)), jnp.logical_not((second, first, last)[dx + 1])))
        def _(dx=dx):
            pl.semaphore_signal(open_.at[2], inc=1, device_id=device(dx, 1), device_id_type=MESH)

    eight = pl.ds(0, 8)
    requests = pltpu.make_async_remote_copy(
        src_ref=sreq.at[eight], dst_ref=rreq.at[eight], send_sem=ssem.at[0], recv_sem=rsem.at[0],
        device_id=device(0, 1), device_id_type=MESH,
    )

    for side, y in ((0, NY - 1), (1, 0)):
        for q, ref in enumerate((P_, D_, W_, O_)):
            ysend[side, q] = ref[pl.ds(y, NX, NY), :]
    pltpu.make_async_copy(K.at[:, cols], K.at[:, cols], lsem.at[4]).wait()
    for side, y in ((0, NY - 1), (1, 0)):
        ysend[side, 4] = KY[pl.ds(y, NX, NY), :]

    def halo(src, dst, n, dx, dy):
        return pltpu.make_async_remote_copy(
            src_ref=src, dst_ref=dst, send_sem=hsend.at[n], recv_sem=hrecv.at[n],
            device_id=device(dx, dy), device_id_type=MESH,
        )

    halos_x = []
    for side, (dx, x) in enumerate(((1, NX - 1), (-1, 0))):
        row = pl.ds(x * NY, NY)
        halos_x.append([
            halo(X.at[:, row], hx.at[side, pl.ds(0, 4)], side, dx, 0),
            halo(K.at[0, row], hx.at[side, 4], side, dx, 0),
        ])
    whole_x = [halo(hx.at[side], hx.at[side], side, dx, 0) for side, dx in enumerate((1, -1))]
    halos_y = [halo(ysend.at[side], hy.at[side], 2 + side, 0, dy) for side, dy in enumerate((1, -1))]
    goes = (ix < nx - 1, ix > 0, iy < ny - 1, iy > 0)
    comes = (goes[1], goes[0], goes[3], goes[2])

    @pl.when(jnp.logical_and(goes[0], jnp.logical_not(first)))
    def _():
        for copy in halos_x[0]:
            copy.start()

    @pl.when(jnp.logical_not(first))
    def _():
        for copy in halos_x[1]:
            copy.start()

    for side in range(2):
        @pl.when(goes[2 + side])
        def _(side=side):
            halos_y[side].start()

    lanes = lax.broadcasted_iota(jnp.int32, (TILE, NZ), 1)
    sublanes = lax.broadcasted_iota(jnp.int32, (TILE, NZ), 0)
    last_lane = lanes == NZ - 1
    last_sub = sublanes == TILE - 1

    def block(b, carry):
        for t in range(4):
            base = b * (BLOCK * NY) + TILE * t
            at = pl.ds(pl.multiple_of(base, TILE), TILE)
            p, d, w, o, kx = P_[at, :], D_[at, :], W_[at, :], O_[at, :], KX[at, :]
            m = mobility(w, o)
            fx = [fxs[f, pl.ds(TILE * t, TILE), :] for f in range(3)]
            for k in range(BLOCK):
                row = b * BLOCK + k
                at = pl.ds(pl.multiple_of(base + k * NY, TILE), TILE)
                nrow = jnp.minimum(row + 1, NX - 1)
                nat = pl.ds(pl.multiple_of(nrow * NY + TILE * t, TILE), TILE)
                pn, dn, wn, on, kn = P_[nat, :], D_[nat, :], W_[nat, :], O_[nat, :], KX[nat, :]
                mn = mobility(wn, on)
                inside = jnp.where(row < NX - 1, 2.0, 0.0)
                gx = fluxes(p, d, m, pn, dn, mn, inside * kx * kn / (kx + kn))
                net = [gx[f] - fx[f] for f in range(3)]
                uat = pl.ds(base + k * NY + 1, TILE)
                ky, ku = KY[at, :], KY[uat, :]
                gy = fluxes(p, d, m, P_[uat, :], D_[uat, :], mobility(W_[uat, :], O_[uat, :]), harmonic(ky, ku))
                for f in range(3):
                    g = jnp.where(last_sub, 0.0, gy[f]) if t == 3 else gy[f]
                    fys[k, f, pl.ds(TILE + TILE * t, TILE), :] = g
                    net[f] = net[f] + (g - fys[k, f, pl.ds(TILE + TILE * t - 1, TILE), :])
                kz = KZ[at, :]
                up = lambda v: pltpu.roll(v, NZ - 1, 1)
                tz = jnp.where(last_lane, 0.0, harmonic(kz, up(kz)))
                gz = fluxes(p, d, m, up(p), up(d), [up(v) for v in m], tz)
                wt = STEP / PV[at, :]
                wgt[at, :] = wt
                sats = (w, o, 1.0 - w - o)
                for f in range(3):
                    total = net[f] + (gz[f] - pltpu.roll(gz[f], 1, 1))
                    acc[f, at, :] = sats[f] - wt * total
                p, d, w, o, kx, m, fx = pn, dn, wn, on, kn, mn, gx
            for f in range(3):
                fxs[f, pl.ds(TILE * t, TILE), :] = fx[f]
        return carry

    blocks = NX // BLOCK
    early = jnp.where(first, jnp.where(odd, RELAY_AT, blocks), jnp.where(last, blocks // 2 - 2, blocks // 2))
    lax.fori_loop(0, early, block, 0)

    def relayed(n):
        part = pl.ds(0, n)
        return pltpu.make_async_remote_copy(
            src_ref=lreq.at[part], dst_ref=rreq.at[part], send_sem=psem.at[0], recv_sem=rsem.at[0],
            device_id=device(LINE - 1, 0), device_id_type=MESH,
        )

    beside = jnp.logical_and(first, iy == ny - 1)

    @pl.when(beside)
    def _():
        to_side.wait_recv()
        from_side.start()

    for order, here in (((3, 5, 1, 4, 2, 0), iy != 1), ((3, 4, 1, 2, 5, 0), iy == 1)):
        @pl.when(jnp.logical_and(jnp.logical_and(first, odd), here))
        def _(order=order):
            for k in order:
                c = k % 3
                if k in (3, 1):
                    pl.semaphore_wait(open_.at[k // 3], 1)
                to_relay(c, k < 3).wait_recv()
                pltpu.make_async_remote_copy(
                    src_ref=lreq.at[k], dst_ref=rreq.at[c], send_sem=psem.at[0], recv_sem=rsem.at[c],
                    device_id=device(LINE - 1, 0 if k < 3 else -1), device_id_type=MESH,
                ).start()

    @pl.when(first)
    def _():
        pl.semaphore_wait(open_.at[2], 3)
        for c in (6, 8, 7):
            request(c, device(*offsets[c])).start()
        for copy in halos_x[0]:
            copy.start()

    @pl.when(wraps)
    def _():
        pl.semaphore_wait(open_.at[2], jnp.where(jnp.logical_or(second, last), 2, 3))

    for c, known in ((6, last), (3, first), (0, second)):
        @pl.when(jnp.logical_and(wraps, jnp.logical_not(known)))
        def _(c=c):
            request(c, device(*offsets[c])).start()

    middle = jnp.where(first, blocks, early)
    lax.fori_loop(early, middle, block, 0)

    lands = {}

    def answer(codes):
        for n, c in codes:
            ref = sreq if n == HERE else rreq
            for s in range(CAP):
                lands[n, s] = jnp.clip(ref[c, pl.ds(20 + s, 1), :].astype(jnp.int32), 0, COLS - 1)[0, 0]
        for n, c in codes:
            for s in range(CAP):
                for q, ref in enumerate((P_, D_, W_, O_)):
                    loc[n, pl.ds(4 * q + s, 1), :] = ref[pl.ds(lands[n, s], 1), :]
        for n, c in codes:
            ref = sreq if n == HERE else rreq
            a = [ref[c, pl.ds(4 * q, 4), :] for q in range(5)]
            b = [loc[n, pl.ds(4 * q, 4), :] for q in range(4)]
            flow = fluxes(a[0], a[1], mobility(a[2], a[3]), b[0], b[1], mobility(b[2], b[3]), a[4])
            for f in range(3):
                sresp[c, pl.ds(4 * f, 4), :] = flow[f]
                rows[f, pl.ds(SLOTS + 4 * n, 4), :] = -flow[f]
                if n == HERE:
                    rows[f, pl.ds(4 * n, 4), :] = flow[f]
            sresp[c, pl.ds(12, 4), :] = jnp.zeros((4, NZ), jnp.float32)
            if n == HERE:
                continue
            pltpu.make_async_remote_copy(
                src_ref=sresp.at[c], dst_ref=rresp.at[c], send_sem=ssem.at[1], recv_sem=rsem.at[4],
                device_id=device(1, 1 - c) if n < 3 else device(-offsets[c][0], -offsets[c][1]),
                device_id_type=MESH,
            ).start()

    for n, c in ((0, jnp.where(odd, 1, 0)), (1, 2), (2, jnp.where(odd, 0, 1))):
        pltpu.make_async_remote_copy(
            src_ref=sreq.at[c], dst_ref=rreq.at[c], send_sem=ssem.at[0], recv_sem=rsem.at[c],
            device_id=device(0, 1), device_id_type=MESH,
        ).wait_recv()
        answer([(n, c)])
    five = pl.ds(3, 5)
    pltpu.make_async_remote_copy(
        src_ref=sreq.at[five], dst_ref=rreq.at[five], send_sem=ssem.at[0], recv_sem=rsem.at[3],
        device_id=device(0, 1), device_id_type=MESH,
    ).wait_recv()
    answer([(c, c) for c in (6, 8, 3, 5, 7, HERE)])
    answers = pltpu.make_async_remote_copy(
        src_ref=sresp.at[eight], dst_ref=rresp.at[eight], send_sem=ssem.at[1], recv_sem=rsem.at[4],
        device_id=device(0, 1), device_id_type=MESH,
    )

    @pl.when(jnp.logical_and(first, goes[1]))
    def _():
        for copy in halos_x[1]:
            copy.start()

    for c in range(CODES):
        for s in range(CAP):
            idx0, idx1 = place(idx0, idx1, SLOTS + c * CAP + s, lands[c, s])

    lax.fori_loop(middle, blocks, block, 0)

    def face(axis, side):
        far = [(hy if axis else hx)[side, q] for q in range(5)]
        if axis:
            at = pl.ds((NY - 1) if side else 0, NX, NY)
        else:
            at = pl.ds((NX - 1) * NY if side else 0, NY)
        near = [ref[at, :] for ref in (P_, D_, W_, O_, KY if axis else KX)]
        lo, hi = (near, far) if side else (far, near)
        flow = fluxes(
            lo[0], lo[1], mobility(lo[2], lo[3]), hi[0], hi[1], mobility(hi[2], hi[3]), harmonic(lo[4], hi[4])
        )
        wt = wgt[at, :]
        for f in range(3):
            step = wt * flow[f]
            acc[f, at, :] = acc[f, at, :] + (-step if side else step)

    for axis in range(2):
        for side in range(2):
            @pl.when(comes[2 * axis + side])
            def _(axis=axis, side=side):
                if axis:
                    halos_y[side].wait_recv()
                else:
                    whole_x[side].wait_recv()
                face(axis, side)

    idx = jnp.concatenate([idx0, idx1], axis=1)
    cell = lax.broadcasted_iota(jnp.int32, (32, 2 * NZ), 0)

    def mark(b, carry):
        start = pl.multiple_of(b * 32, 32)
        hot[pl.ds(start, 32), :] = jnp.where(cell + start == idx, 1.0, 0.0).astype(jnp.bfloat16)
        return carry

    lax.fori_loop(0, COLS // 32, mark, 0)

    answers.wait_recv()
    for c in range(CODES):
        if c != HERE:
            for f in range(3):
                rows[f, pl.ds(4 * c, 4), :] = rresp[c, pl.ds(4 * f, 4), :]
    requests.wait_send()
    answers.wait_send()
    for side in range(2):
        @pl.when(goes[side])
        def _(side=side):
            whole_x[side].wait_send()

        @pl.when(goes[2 + side])
        def _(side=side):
            halos_y[side].wait_send()

    @pl.when(jnp.logical_and(jnp.logical_and(first, odd), jnp.logical_not(top)))
    def _():
        relayed(6).wait_send()

    @pl.when(beside)
    def _():
        relayed(7).wait_send()


def add_kernel(acc, wgt, hot, rows, out, parts, held, sem):
    for f in range(3):
        value = rows[f]
        for k in range(3):
            part = value.astype(jnp.bfloat16)
            parts[pl.ds(2 * SLOTS * k, 2 * SLOTS), pl.ds(NZ * f, NZ)] = part
            value = value - part.astype(jnp.float32)
        parts[pl.ds(240, 16), pl.ds(NZ * f, NZ)] = jnp.zeros((16, NZ), jnp.bfloat16)
    size = COLS // 8
    for n in range(8):
        at = pl.ds(n * size, size)
        delta = jnp.dot(hot[at, :], parts[...], preferred_element_type=jnp.float32)
        wt = wgt[at, :]
        for f in range(3):
            held[f, at, :] = acc[f, at, :] - wt * delta[:, NZ * f:NZ * (f + 1)]
            pltpu.make_async_copy(held.at[f, at], out.at[f, at], sem).start()
    pltpu.make_async_copy(held, out, sem).wait()


def body(pressure, depth, saturation, permeability, pore_volume, fault_pairs, fault_kind, fault_count, fault_table):
    f32, i32 = jnp.float32, jnp.int32
    hbm = pl.BlockSpec(memory_space=pltpu.HBM)
    vmem = pl.BlockSpec(memory_space=pltpu.VMEM)
    V = pltpu.VMEM
    acc, wgt, hot, rows = pl.pallas_call(
        grid_kernel,
        out_shape=(
            V((3, COLS, NZ), f32), V((COLS, NZ), f32), V((COLS, 2 * NZ), jnp.bfloat16), V((3, 2 * SLOTS, NZ), f32),
        ),
        in_specs=[hbm] * 8 + [pl.BlockSpec(memory_space=pltpu.SMEM)],
        out_specs=(vmem,) * 4,
        scratch_shapes=[
            V((4, COLS + TILE, NZ), f32), V((4, COLS + TILE, NZ), f32), V((16 + TILE, NZ), f32),
            pltpu.SMEM((3, 32), i32), pltpu.SMEM((32,), i32),
            V((CODES, 24, NZ), f32), V((CODES, 24, NZ), f32), V((7, 24, NZ), f32), V((CODES, 24, NZ), f32),
            V((CODES, 16, NZ), f32), V((CODES, 16, NZ), f32),
            V((2, 5, NX, NZ), f32), V((2, 5, NY, NZ), f32), V((2, 5, NX, NZ), f32),
            V((3, NY, NZ), f32), V((BLOCK, 3, TILE + NY, NZ), f32),
            pltpu.SemaphoreType.DMA((5,)), pltpu.SemaphoreType.DMA((2,)), pltpu.SemaphoreType.DMA((5,)),
            pltpu.SemaphoreType.DMA((7,)), pltpu.SemaphoreType.DMA((1,)),
            pltpu.SemaphoreType.DMA((4,)), pltpu.SemaphoreType.DMA((4,)), pltpu.SemaphoreType.REGULAR((3,)),
        ],
        compiler_params=pltpu.CompilerParams(collective_id=0, has_side_effects=True, vmem_limit_bytes=24 * 2**20),
        name="grid",
    )(
        *(
            pltpu.with_memory_space_constraint(x, pltpu.HBM)
            for x in (
                pressure.reshape(COLS, NZ), depth.reshape(COLS, NZ), saturation.reshape(2, COLS, NZ),
                permeability.reshape(3, COLS, NZ), pore_volume.reshape(COLS, NZ),
                fault_pairs.T, fault_kind, fault_table,
            )
        ),
        fault_count,
    )
    out = pl.pallas_call(
        add_kernel,
        out_shape=jax.ShapeDtypeStruct((3, COLS, NZ), f32),
        in_specs=[vmem] * 4,
        out_specs=hbm,
        scratch_shapes=[V((2 * NZ, 3 * NZ), jnp.bfloat16), V((3, COLS, NZ), f32), pltpu.SemaphoreType.DMA],
        compiler_params=pltpu.CompilerParams(vmem_limit_bytes=16 * 2**20),
        name="add",
    )(acc, wgt, hot, rows)
    return out.reshape(3, NX, NY, NZ)


def solution(mesh):
    in_specs = (
        P("gx", "gy", None),
        P("gx", "gy", None),
        P(None, "gx", "gy", None),
        P(None, "gx", "gy", None),
        P("gx", "gy", None),
        P(("gx", "gy"), None),
        P(("gx", "gy")),
        P(("gx", "gy")),
        P(),
    )
    out_specs = P(None, "gx", "gy", None)
    return jax.shard_map(body, mesh=mesh, in_specs=in_specs, out_specs=out_specs, check_vma=False)
```
